128 devices in a mesh: rep: 16 (over y, x_hi, core), tp: 8 (over x_lo, z).
Axes of the slice: x: 4 (x_hi: 2, x_lo: 2; x = x_hi * 2 + x_lo), y: 4, z: 4, core: 2. Of those that a mesh axis runs over, the one named last changes fastest.
Arguments:
- hidden: bfloat16 [1024, 8192], P('rep'), may hold values from -6 to 6
- norm_gain: bfloat16 [8192], replicated, may hold values from 0.5 to 1.5
- query_weight_matrix: bfloat16 [8192, 4096], P(None, 'tp'), may hold values from -0.0625 to 0.0625
- key_value_weight: bfloat16 [2, 8192, 1024], P(None, None, 'tp'), may hold values from -0.0625 to 0.0625
- output_weight_matrix: bfloat16 [4096, 8192], P('tp'), may hold values from -0.375 to 0.375
- input_down_factors: bfloat16 [3, 8192, 64], P(None, ('rep', 'tp')), may hold values from -0.0625 to 0.0625
- query_up_factor: bfloat16 [64, 4096], P(None, ('rep', 'tp')), may hold values from -0.75 to 0.75
- key_value_up_factors: bfloat16 [2, 64, 1024], P(None, None, ('rep', 'tp')), may hold values from -0.75 to 0.75
- output_down_factor: bfloat16 [4096, 64], P(('rep', 'tp')), may hold values from -0.375 to 0.375
- output_up_factor: bfloat16 [64, 8192], P(None, ('rep', 'tp')), may hold values from -0.75 to 0.75
- cache_keys: bfloat16 [1024, 8, 128, 128], P('rep', 'tp'), may hold values from -360 to 360
- cache_values: bfloat16 [1024, 8, 128, 128], P('rep', 'tp'), may hold values from -6 to 6
- lengths: int32 [1024], P('rep'), may hold values from 1 to 127
Outputs:
- attn_out: bfloat16 [1024, 8192], P('rep', 'tp')
The draws below stay inside these ranges and needn't reach their ends.
All inputs are finite; a program needn't handle non-finite values.
Results may differ from the reference program's by a relative error of at most 0.03.
Values may be sent and summed in bfloat16 or wider, within the bound.
A program may use at most 128 MiB of HBM per device.

```python
import math
import jax
import jax.numpy as jnp
from jax import lax

D = 8192
HEADS = 32
KV_HEADS = 8
HEAD_DIM = 128
RANK = 64
CACHE = 128
BATCH = 1024


def draw_cache_keys(key, part):
    base_key = jax.random.fold_in(key, 11)
    values = jax.random.normal(base_key, (BATCH, KV_HEADS, CACHE, HEAD_DIM), jnp.float32)
    values = jnp.clip(values, -6.0, 6.0)
    return values.astype(jnp.bfloat16)


def set_ends(array, key, least, largest):
    spot = [jax.random.randint(jax.random.fold_in(key, axis), (), 0, length) for axis, length in enumerate(array.shape)]
    widest = array.shape.index(max(array.shape))
    next_to = spot[:widest] + [(spot[widest] + 1) % array.shape[widest]] + spot[widest + 1:]
    return array.at[tuple(spot)].set(least).at[tuple(next_to)].set(largest)


def levels(stream_key, dims, shards, least, largest):
    factor_of, own = 1.0, jax.random.fold_in(stream_key, 6)
    for axis_at, blocks in shards:
        heights = jnp.exp(jax.random.uniform(jax.random.fold_in(own, axis_at), (blocks,), jnp.float32, least / len(shards), largest / len(shards)))
        factor_of = factor_of * jnp.repeat(heights, dims[axis_at] // blocks).reshape([-1 if axis == axis_at else 1 for axis in range(len(dims))])
    return factor_of


def normal_values(rng, extent, scale, most, pieces=(), held_as=jnp.bfloat16):
    entries = jax.random.normal(rng, extent, jnp.float32) * scale
    if len(pieces) > 0:
        entries = levels(rng, extent, pieces, -0.22, 0.18) * entries
    return jnp.clip(entries, min=-most, max=most).astype(held_as)


def setup_inputs(seed: int = 0) -> dict:
    key_list = jax.random.split(jax.random.key(seed), 14)
    hidden = normal_values(key_list[0], (BATCH, D), 1.0, 6.0, ((0, 16),))
    norm_gain = jnp.clip(1.0 + 0.1 * jax.random.normal(key_list[1], (D,), jnp.float32), 0.5, 1.5).astype(jnp.bfloat16)
    query_weight_matrix = normal_values(key_list[2], (D, HEADS * HEAD_DIM), D ** -0.5, 0.0625, ((1, 8),))
    key_value_weight = normal_values(key_list[3], (2, D, KV_HEADS * HEAD_DIM), D ** -0.5, 0.0625, ((2, 8),))
    output_weight_matrix = normal_values(key_list[4], (HEADS * HEAD_DIM, D), (HEADS * HEAD_DIM // 16) ** -0.5, 0.375, ((0, 8),))
    input_down_factors = normal_values(key_list[5], (3, D, RANK), D ** -0.5, 0.0625, ((1, 128),))
    query_up_factor = normal_values(key_list[6], (RANK, HEADS * HEAD_DIM), RANK ** -0.5, 0.75, ((1, 128),))
    key_value_up_factors = normal_values(key_list[7], (2, RANK, KV_HEADS * HEAD_DIM), RANK ** -0.5, 0.75, ((2, 128),))
    output_down_factor = normal_values(key_list[8], (HEADS * HEAD_DIM, RANK), (HEADS * HEAD_DIM // 16) ** -0.5, 0.375, ((0, 128),))
    output_up_factor = normal_values(key_list[9], (RANK, D), RANK ** -0.5, 0.75, ((1, 128),))
    cache_keys = draw_cache_keys(jax.random.fold_in(key_list[13], 71), 0)
    cache_values = normal_values(key_list[11], (BATCH, KV_HEADS, CACHE, HEAD_DIM), 1.0, 6.0, ((0, 16), (1, 8)))
    lengths = set_ends(jax.random.randint(key_list[12], (BATCH,), 1, CACHE), jax.random.fold_in(key_list[12], 1), 1, CACHE - 1).astype(jnp.int32)
    return dict(hidden=hidden, norm_gain=norm_gain, query_weight_matrix=query_weight_matrix, key_value_weight=key_value_weight, output_weight_matrix=output_weight_matrix, input_down_factors=input_down_factors, query_up_factor=query_up_factor, key_value_up_factors=key_value_up_factors, output_down_factor=output_down_factor, output_up_factor=output_up_factor, cache_keys=cache_keys, cache_values=cache_values, lengths=lengths)


epsilon = 1e-06
rope_base = 1000000.0
adapter_scale = 0.5

def rope_angles(lengths, head_dim):
    half_dim = head_dim // 2
    frequency = rope_base ** (-(jnp.arange(half_dim, dtype=jnp.float32) * 2.0) / head_dim)
    return lengths.astype(jnp.float32)[:, None] * frequency[None, :]

def rotate(vectors, angles):
    half_dim = vectors.shape[-1] // 2
    cosine = jnp.cos(angles)[:, None, :]
    sine_part = jnp.sin(angles)[:, None, :]
    low_half = vectors[..., :half_dim]
    high_half = vectors[..., half_dim:]
    return jnp.concatenate([low_half * cosine - high_half * sine_part, high_half * cosine + low_half * sine_part], axis=-1)

def adapted(normed, frozen_matrix, inner_part, up_factor):
    base_part = jnp.dot(normed, frozen_matrix, preferred_element_type=jnp.float32)
    return base_part + adapter_scale * jnp.dot(inner_part, up_factor, preferred_element_type=jnp.float32)

def attend(query, new_key, new_value, keys, values, lengths):
    score_scale = 1.0 / math.sqrt(keys.shape[-1])
    scores = jnp.einsum('bkgd,bkld->bkgl', query, keys.astype(jnp.float32), precision=lax.Precision.HIGHEST) * score_scale
    own_score = lax.optimization_barrier(jnp.sum(query * new_key.astype(jnp.float32)[:, :, None, :], axis=-1)) * score_scale
    live_mask = jnp.arange(keys.shape[2], dtype=jnp.int32)[None, None, None, :] < lengths[:, None, None, None]
    row_max = jnp.maximum(lax.optimization_barrier(jnp.max(jnp.where(live_mask, scores, -1e+30), axis=-1)), own_score)
    weights = jnp.where(live_mask, jnp.exp(scores - row_max[..., None]), 0.0)
    own_weight = jnp.exp(own_score - row_max)
    denom_sum = lax.optimization_barrier(jnp.sum(weights, axis=-1)) + own_weight
    probs = (weights / denom_sum[..., None]).astype(jnp.bfloat16)
    own_prob = (own_weight / denom_sum).astype(jnp.bfloat16)
    context = jnp.einsum('bkgl,bkld->bkgd', probs.astype(jnp.float32), values.astype(jnp.float32))
    context = context + own_prob.astype(jnp.float32)[..., None] * new_value.astype(jnp.float32)[:, :, None, :]
    return context.astype(jnp.bfloat16)

def reference(hidden, norm_gain, query_weight_matrix, key_value_weight, output_weight_matrix, input_down_factors, query_up_factor, key_value_up_factors, output_down_factor, output_up_factor, cache_keys, cache_values, lengths):
    states = hidden.astype(jnp.float32)
    square = lax.optimization_barrier(jnp.mean(states * states, axis=-1, keepdims=True))
    normed = (states * lax.rsqrt(square + epsilon) * norm_gain.astype(jnp.float32)).astype(jnp.bfloat16)
    inner_query = jnp.dot(normed, input_down_factors[0], preferred_element_type=jnp.float32).astype(jnp.bfloat16)
    inner_key = jnp.dot(normed, input_down_factors[1], preferred_element_type=jnp.float32).astype(jnp.bfloat16)
    inner_value = jnp.dot(normed, input_down_factors[2], preferred_element_type=jnp.float32).astype(jnp.bfloat16)
    batch = hidden.shape[0]
    kv_count = cache_keys.shape[1]
    head_dim = cache_keys.shape[3]
    angles = rope_angles(lengths, head_dim)
    query = adapted(normed, query_weight_matrix, inner_query, query_up_factor).reshape(batch, -1, head_dim)
    query = rotate(query, angles).reshape(batch, kv_count, -1, head_dim)
    new_key = adapted(normed, key_value_weight[0], inner_key, key_value_up_factors[0]).reshape(batch, kv_count, head_dim)
    new_key = rotate(new_key, angles).astype(jnp.bfloat16)
    new_value = adapted(normed, key_value_weight[1], inner_value, key_value_up_factors[1]).reshape(batch, kv_count, head_dim).astype(jnp.bfloat16)
    context = attend(query, new_key, new_value, cache_keys, cache_values, lengths).reshape(batch, -1)
    middle = jnp.dot(context, output_down_factor, preferred_element_type=jnp.float32).astype(jnp.bfloat16)
    return adapted(context, output_weight_matrix, middle, output_up_factor).astype(jnp.bfloat16)
```

```python
import math

import jax
import jax.numpy as jnp
from jax import lax
from jax.experimental import pallas as pl
from jax.experimental.pallas import tpu as pltpu
from jax.sharding import PartitionSpec as P

MESH = pl.DeviceIdType.MESH
bf16, f32 = jnp.bfloat16, jnp.float32

epsilon = 1e-06
rope_base = 1000000.0
adapter_scale = 0.5

FEATURES = 8192
SEQS = 64
RANK = 64
HEAD = 128
QCOLS = 512
OUTC = 1024
TP = 8
CHIPS = 8
CHUNKS = 8
CHUNK = FEATURES // CHUNKS
DROWS = 96
UROWS = 80
GROUP = 8


def dot(a, b):
    return jnp.dot(a, b, preferred_element_type=f32)


def dot_nt(a, b):
    return lax.dot_general(a, b, (((1,), (1,)), ((), ())), preferred_element_type=f32)


def dot_tn(a, b):
    return lax.dot_general(a, b, (((0,), (0,)), ((), ())), preferred_element_type=f32)


def at_lanes(offset, rows):
    row = lax.broadcasted_iota(jnp.int32, (rows, 128), 0)
    lane = lax.broadcasted_iota(jnp.int32, (rows, 128), 1)
    return jnp.where(lane == row + offset, 1.0, 0.0).astype(bf16)


def kernel(
    hidden, gain, wq, wkv, wo, down, qup, kvup, odown, oup, keys, values, lengths,
    out,
    hid_v, nrm_v, wq_v, wkv_v, wo_v, k_v, v_v,
    down_v, qup_v, kvup_v, odown_v, oup_v,
    dg, w2, ug, ut, inner_p, ou_v, mid_p, rs_send, rs_recv,
    qacc, kacc, vacc, q_s, own_s, ctx_s, len_s, ctx_b, out_v,
    load_sem, wq_sem, wkv_sem, small_sem,
    d_send, d_recv, dd_sem, u_send, u_recv, t_send, t_recv, tt_sem,
    i_send, i_recv, m_send, m_recv, r_send, r_recv,
):
    rep = lax.axis_index("rep")
    t = lax.axis_index("tp")
    chip = rep // 2
    core = rep % 2
    partner = chip * 2 + (1 - core)

    def chip_at(j):
        return lax.rem(chip + j, CHIPS)

    def tp_at(j):
        return lax.rem(t + j, TP)

    barrier = pltpu.get_barrier_semaphore()
    pl.semaphore_signal(barrier, inc=1, device_id=(partner, t), device_id_type=MESH)
    for j in range(1, CHIPS):
        pl.semaphore_signal(barrier, inc=1, device_id=(chip_at(j) * 2 + core, t), device_id_type=MESH)
    for j in range(1, TP):
        pl.semaphore_signal(barrier, inc=1, device_id=(rep, tp_at(j)), device_id_type=MESH)

    small = [
        pltpu.make_async_copy(src, dst, small_sem.at[i])
        for i, (src, dst) in enumerate(
            ((down, down_v), (qup, qup_v), (kvup, kvup_v), (odown, odown_v), (oup, oup_v))
        )
    ]
    for copy in small:
        copy.start()
    hid_copy = pltpu.make_async_copy(hidden, hid_v, load_sem.at[0])
    hid_copy.start()

    def wq_copy(i):
        rows = pl.ds(pl.multiple_of(i * CHUNK, CHUNK), CHUNK)
        return pltpu.make_async_copy(wq.at[rows, :], wq_v.at[rows, :], wq_sem.at[i])

    def wkv_copy(i):
        rows = pl.ds(pl.multiple_of(i * CHUNK, CHUNK), CHUNK)
        return pltpu.make_async_copy(wkv.at[:, rows, :], wkv_v.at[:, rows, :], wkv_sem.at[i])

    def start_chunk(i, carry):
        wq_copy(i).start()
        wkv_copy(i).start()
        return carry

    lax.fori_loop(0, CHUNKS, start_chunk, 0)
    key_copy = pltpu.make_async_copy(keys, k_v, load_sem.at[1])
    value_copy = pltpu.make_async_copy(values, v_v, load_sem.at[2])
    wo_copy = pltpu.make_async_copy(wo, wo_v, load_sem.at[3])
    key_copy.start()
    value_copy.start()
    wo_copy.start()

    for copy in small:
        copy.wait()
    low, high = at_lanes(0, RANK), at_lanes(64, RANK)
    dg[core, chip, 0:64, :] = (dot(down_v[0], low) + dot(down_v[1], high)).astype(bf16)
    dg[core, chip, 64:96, :] = (dot(down_v[2, 0:32, :], low) + dot(down_v[2, 32:64, :], high)).astype(bf16)
    ug[chip, 0:32, :] = (dot_tn(qup_v[...], low) + dot(odown_v[...], high)).astype(bf16)
    ug[chip, 32:64, :] = (dot(oup_v[0:32, :], low) + dot(oup_v[32:64, :], high)).astype(bf16)
    last = dot_tn(kvup_v[1], low) + dot_tn(kvup_v[0], high)
    ug[chip, 64:80, :] = jnp.concatenate([last, jnp.zeros_like(last)], axis=0).astype(bf16)

    pl.semaphore_wait(barrier, CHIPS + TP - 1)

    def d_copy(j):
        return pltpu.make_async_remote_copy(
            src_ref=dg.at[core, chip], dst_ref=dg.at[core, chip],
            send_sem=d_send.at[j], recv_sem=d_recv.at[j],
            device_id=(chip_at(j) * 2 + core, t), device_id_type=MESH)

    def u_copy(j):
        return pltpu.make_async_remote_copy(
            src_ref=ug.at[chip], dst_ref=ug.at[chip],
            send_sem=u_send.at[j], recv_sem=u_recv.at[j],
            device_id=(chip_at(j) * 2 + core, t), device_id_type=MESH)

    for j in range(1, CHIPS):
        d_copy(j).start()
    for j in range(1, CHIPS):
        u_copy(j).start()

    hid_copy.wait()

    def squares(i, total):
        cols = pl.ds(pl.multiple_of(i * CHUNK, CHUNK), CHUNK)
        x = hid_v[:, cols].astype(f32)
        x = x * x
        for k in range(CHUNK // 128):
            total = total + x[:, k * 128 : (k + 1) * 128]
        return total

    total = lax.fori_loop(0, CHUNKS, squares, jnp.zeros((SEQS, 128), f32))
    square = jnp.sum(total, axis=-1, keepdims=True) * (1.0 / FEATURES)
    scale = lax.rsqrt(square + epsilon)

    def normalise(i, carry):
        cols = pl.ds(pl.multiple_of(i * CHUNK, CHUNK), CHUNK)
        x = hid_v[:, cols].astype(f32)
        nrm_v[:, cols] = (x * scale * gain[:, cols].astype(f32)).astype(bf16)
        return carry

    lax.fori_loop(0, CHUNKS, normalise, 0)

    qacc[...] = jnp.zeros_like(qacc)
    kacc[...] = jnp.zeros_like(kacc)
    vacc[...] = jnp.zeros_like(vacc)

    def project(i, carry):
        wq_copy(i).wait()
        wkv_copy(i).wait()
        cols = pl.ds(pl.multiple_of(i * CHUNK, CHUNK), CHUNK)
        x = nrm_v[:, cols]
        qacc[...] += dot(x, wq_v[cols, :])
        kacc[...] += dot(x, wkv_v[0, cols, :])
        vacc[...] += dot(x, wkv_v[1, cols, :])
        return carry

    lax.fori_loop(0, CHUNKS, project, 0)

    w2[...] = jnp.zeros_like(w2)
    for j in range(1, CHIPS):
        d_copy(j).wait_recv()
    across = pltpu.make_async_remote_copy(
        src_ref=dg.at[core], dst_ref=dg.at[core],
        send_sem=dd_sem.at[0], recv_sem=dd_sem.at[1],
        device_id=(partner, t), device_id_type=MESH)
    across.start()

    for j in range(1, CHIPS):
        u_copy(j).wait_recv()

    def t_copy(j):
        return pltpu.make_async_remote_copy(
            src_ref=ug.at[tp_at(j)], dst_ref=ut.at[core, t],
            send_sem=t_send.at[j], recv_sem=t_recv.at[j],
            device_id=(rep, tp_at(j)), device_id_type=MESH)

    lane = lax.broadcasted_iota(jnp.int32, (SEQS, 128), 1)
    half = pl.multiple_of((t % 2) * 64, 64)

    across.wait_recv()
    partial = jnp.zeros((SEQS, 256), f32)
    for r in range(2 * CHIPS):
        c, q = r % 2, r // 2
        w2[r, pl.ds(half, 64), 0:128] = dg[c, q, 0:64, :]
        tail = dg[c, q, 64:96, :].astype(f32)
        both = jnp.concatenate([tail, pltpu.roll(tail, 64, axis=1)], axis=0)
        w2[r, pl.ds(half, 64), 128:256] = both.astype(bf16)
    for r in range(2 * CHIPS):
        cols = pl.ds(pl.multiple_of(r * QCOLS + (t // 2) * 128, 128), 128)
        partial = partial + dot(nrm_v[:, cols], w2[r])
    inner_p[t, 0:64, :] = partial[:, 0:128].astype(bf16)
    tail = partial[:, 128:256]
    tail = jnp.where(lane[0:32] < 64, tail[0:32], pltpu.roll(tail[32:64], 64, axis=1))
    inner_p[t, 64:96, :] = tail.astype(bf16)

    def i_copy(j):
        return pltpu.make_async_remote_copy(
            src_ref=inner_p.at[t], dst_ref=inner_p.at[t],
            send_sem=i_send.at[j], recv_sem=i_recv.at[j],
            device_id=(rep, tp_at(j)), device_id_type=MESH)

    for j in range(1, TP):
        i_copy(j).start()
    for j in range(1, TP):
        t_copy(j).start()
    ut[core, t] = ug[t]

    lens = lengths[...].reshape(1, SEQS)
    square_rows = lax.broadcasted_iota(jnp.int32, (SEQS, SEQS), 0)
    square_lanes = lax.broadcasted_iota(jnp.int32, (SEQS, SEQS), 1)
    len_col = jnp.sum(
        jnp.where(square_rows == square_lanes, jnp.broadcast_to(lens, (SEQS, SEQS)), 0).astype(f32),
        axis=-1, keepdims=True)
    len_b = jnp.broadcast_to(len_col, (SEQS, 128))
    for h in range(8):
        len_s[pl.ds(h, SEQS, stride=8), :] = len_b
    index = (lane % 64).astype(f32)
    frequency = jnp.exp(index * (-2.0 / HEAD * math.log(rope_base)))
    angles = len_b * frequency
    cosine = jnp.cos(angles)
    sine = jnp.where(lane < 64, -jnp.sin(angles), jnp.sin(angles))

    def rotate(x):
        return x * cosine + pltpu.roll(x, 64, axis=1) * sine

    for j in range(1, TP):
        t_copy(j).wait_recv()
    up_across = pltpu.make_async_remote_copy(
        src_ref=ut.at[core], dst_ref=ut.at[core],
        send_sem=tt_sem.at[0], recv_sem=tt_sem.at[1],
        device_id=(partner, t), device_id_type=MESH)
    up_across.start()

    for j in range(1, TP):
        i_copy(j).wait_recv()
    inner = inner_p[0].astype(f32)
    for k in range(1, TP):
        inner = inner + inner_p[k].astype(f32)
    first = inner[0:64]
    tail = inner[64:96]
    tail = jnp.concatenate([tail, pltpu.roll(tail, 64, axis=1)], axis=0)
    inner_q = jnp.where(lane < 64, first, 0.0).astype(bf16)
    inner_k = jnp.where(lane < 64, 0.0, first).astype(bf16)
    inner_v = jnp.where(lane < 64, tail, 0.0).astype(bf16)
    up_across.wait_recv()

    up_rows = ut[:, :, 0:32, :].reshape(QCOLS, 128)
    kv_rows = jnp.concatenate(
        [ut[n // TP, n % TP, 64:80, :].astype(f32)[0:8] for n in range(2 * TP)], axis=0).astype(bf16)
    new_key = rotate(kacc[...] + adapter_scale * dot_nt(inner_k, kv_rows)).astype(bf16).astype(f32)
    new_value = (vacc[...] + adapter_scale * dot_nt(inner_v, kv_rows)).astype(bf16).astype(f32)
    query = qacc[...] + adapter_scale * dot_nt(inner_q, up_rows)
    score_scale = 1.0 / math.sqrt(HEAD)
    for h in range(4):
        x = rotate(query[:, h * HEAD : (h + 1) * HEAD])
        main = x.astype(bf16).astype(f32)
        own = jnp.sum(x * new_key, axis=-1, keepdims=True) * score_scale
        own = jnp.broadcast_to(own, (SEQS, 128))
        q_s[pl.ds(h, SEQS, stride=8), :] = main
        q_s[pl.ds(h + 4, SEQS, stride=8), :] = x - main
        own_s[pl.ds(h, SEQS, stride=8), :] = own
        own_s[pl.ds(h + 4, SEQS, stride=8), :] = own

    key_copy.wait()
    value_copy.wait()
    wide = 8 * GROUP
    position = lax.broadcasted_iota(jnp.int32, (wide, 128), 1).astype(f32)

    def attend(g, carry):
        rows = pl.ds(pl.multiple_of(g * wide, wide), wide)
        q_rows = q_s[rows, :].astype(bf16)
        scores = []
        for s in range(GROUP):
            sc = dot_nt(q_rows[s * 8 : (s + 1) * 8], k_v[g * GROUP + s, 0])
            scores.append(sc + pltpu.roll(sc, 4, axis=0))
        scores = jnp.concatenate(scores, axis=0) * score_scale
        own = own_s[rows, :]
        live = position < len_s[rows, :]
        row_max = jnp.maximum(
            jnp.max(jnp.where(live, scores, -1e30), axis=-1, keepdims=True), own)
        weights = jnp.where(live, jnp.exp(scores - row_max), 0.0)
        own_weight = jnp.exp(own - row_max)
        denom = jnp.sum(weights, axis=-1, keepdims=True) + own_weight
        probs = (weights / denom).astype(bf16)
        own_s[rows, :] = (own_weight / denom).astype(bf16).astype(f32)
        parts = [
            dot(probs[s * 8 : (s + 1) * 8], v_v[g * GROUP + s, 0]) for s in range(GROUP)
        ]
        ctx_s[rows, :] = jnp.concatenate(parts, axis=0)
        return carry

    lax.fori_loop(0, SEQS // GROUP, attend, 0)

    for h in range(4):
        x = ctx_s[pl.ds(h, SEQS, stride=8), :] + own_s[pl.ds(h, SEQS, stride=8), :] * new_value
        ctx_b[:, h * HEAD : (h + 1) * HEAD] = x.astype(bf16)
    context = ctx_b[...]

    middle = dot(context, up_rows)
    middle = jnp.where(lane[0:32] < 64, pltpu.roll(middle[0:32], 64, axis=1), middle[32:64])
    mid_p[t] = middle

    def m_copy(j):
        return pltpu.make_async_remote_copy(
            src_ref=mid_p.at[t], dst_ref=mid_p.at[t],
            send_sem=m_send.at[j], recv_sem=m_recv.at[j],
            device_id=(rep, tp_at(j)), device_id_type=MESH)

    for j in range(1, TP):
        m_copy(j).start()
    wo_copy.wait()

    def r_copy(j):
        return pltpu.make_async_remote_copy(
            src_ref=rs_send.at[tp_at(j)], dst_ref=rs_recv.at[t],
            send_sem=r_send.at[j], recv_sem=r_recv.at[j],
            device_id=(rep, tp_at(j)), device_id_type=MESH)

    def send_block(j, carry):
        cols = pl.ds(pl.multiple_of(tp_at(j) * OUTC, OUTC), OUTC)
        rs_send[tp_at(j)] = dot(ctx_b[...], wo_v[:, cols]).astype(bf16)
        r_copy(j).start()
        return carry

    lax.fori_loop(1, TP, send_block, 0)

    for k in range(TP):
        a = ut[(2 * k) // TP, (2 * k) % TP, 32:64, :].astype(f32)
        b = ut[(2 * k) // TP, (2 * k + 1) % TP, 32:64, :].astype(f32)
        a_r, b_r = pltpu.roll(a, 64, axis=1), pltpu.roll(b, 64, axis=1)
        left = lane[0:32] < 64
        ou_v[0:32, k * 128 : (k + 1) * 128] = jnp.where(left, a, b_r).astype(bf16)
        ou_v[32:64, k * 128 : (k + 1) * 128] = jnp.where(left, a_r, b).astype(bf16)

    mine = pl.ds(pl.multiple_of(t * OUTC, OUTC), OUTC)
    own_block = dot(ctx_b[...], wo_v[:, mine])

    for j in range(1, TP):
        m_copy(j).wait_recv()
    middle = mid_p[0]
    for k in range(1, TP):
        middle = middle + mid_p[k]
    middle = jnp.concatenate([middle, pltpu.roll(middle, 64, axis=1)], axis=0)[:, 0:64].astype(bf16)
    out_v[...] = own_block + adapter_scale * dot(middle, ou_v[...])

    def add_block(j, carry):
        r_copy(j).wait_recv()
        out_v[...] += rs_recv[lax.rem(t + TP - j, TP)].astype(f32)
        return carry

    lax.fori_loop(1, TP, add_block, 0)
    out[...] = out_v[...].astype(bf16)

    for j in range(1, CHIPS):
        d_copy(j).wait_send()
        u_copy(j).wait_send()
    across.wait_send()
    up_across.wait_send()
    for j in range(1, TP):
        i_copy(j).wait_send()
        t_copy(j).wait_send()
        m_copy(j).wait_send()
        r_copy(j).wait_send()


def local(
    hidden, norm_gain, query_weight_matrix, key_value_weight, output_weight_matrix,
    input_down_factors, query_up_factor, key_value_up_factors, output_down_factor,
    output_up_factor, cache_keys, cache_values, lengths,
):
    anywhere = pl.BlockSpec(memory_space=pl.ANY)
    vmem = pl.BlockSpec(memory_space=pltpu.VMEM)
    dma = pltpu.SemaphoreType.DMA
    return pl.pallas_call(
        kernel,
        out_shape=jax.ShapeDtypeStruct((SEQS, OUTC), bf16),
        in_specs=[anywhere, vmem] + [anywhere] * 10 + [vmem],
        out_specs=vmem,
        scratch_shapes=[
            pltpu.VMEM((SEQS, FEATURES), bf16),
            pltpu.VMEM((SEQS, FEATURES), bf16),
            pltpu.VMEM((FEATURES, QCOLS), bf16),
            pltpu.VMEM((2, FEATURES, HEAD), bf16),
            pltpu.VMEM((QCOLS, FEATURES), bf16),
            pltpu.VMEM((SEQS, 1, 128, HEAD), bf16),
            pltpu.VMEM((SEQS, 1, 128, HEAD), bf16),
            pltpu.VMEM((3, 64, RANK), bf16),
            pltpu.VMEM((RANK, 32), bf16),
            pltpu.VMEM((2, RANK, 8), bf16),
            pltpu.VMEM((32, RANK), bf16),
            pltpu.VMEM((RANK, 64), bf16),
            pltpu.VMEM((2, CHIPS, DROWS, 128), bf16),
            pltpu.VMEM((2 * CHIPS, 128, 256), bf16),
            pltpu.VMEM((CHIPS, UROWS, 128), bf16),
            pltpu.VMEM((2, TP, UROWS, 128), bf16),
            pltpu.VMEM((TP, DROWS, 128), bf16),
            pltpu.VMEM((RANK, OUTC), bf16),
            pltpu.VMEM((TP, 32, 128), f32),
            pltpu.VMEM((TP, SEQS, OUTC), bf16),
            pltpu.VMEM((TP, SEQS, OUTC), bf16),
            pltpu.VMEM((SEQS, QCOLS), f32),
            pltpu.VMEM((SEQS, HEAD), f32),
            pltpu.VMEM((SEQS, HEAD), f32),
            pltpu.VMEM((SEQS * 8, HEAD), f32),
            pltpu.VMEM((SEQS * 8, HEAD), f32),
            pltpu.VMEM((SEQS * 8, HEAD), f32),
            pltpu.VMEM((SEQS * 8, HEAD), f32),
            pltpu.VMEM((SEQS, QCOLS), bf16),
            pltpu.VMEM((SEQS, OUTC), f32),
            dma((4,)), dma((CHUNKS,)), dma((CHUNKS,)), dma((5,)),
            dma((CHIPS,)), dma((CHIPS,)), dma((2,)), dma((CHIPS,)), dma((CHIPS,)),
            dma((TP,)), dma((TP,)), dma((2,)),
            dma((TP,)), dma((TP,)), dma((TP,)), dma((TP,)), dma((TP,)), dma((TP,)),
        ],
        compiler_params=pltpu.CompilerParams(
            collective_id=0, has_side_effects=True, vmem_limit_bytes=60 * 1024 * 1024),
        cost_estimate=pl.CostEstimate(
            flops=3 * 10**9, bytes_accessed=26 * 2**20, transcendentals=0),
    )(
        hidden, norm_gain.reshape(1, FEATURES), query_weight_matrix, key_value_weight,
        output_weight_matrix, input_down_factors, query_up_factor, key_value_up_factors,
        output_down_factor, output_up_factor, cache_keys, cache_values, lengths,
    )


def solution(mesh):
    placed = (
        P("rep", None),
        P(),
        P(None, "tp"),
        P(None, None, "tp"),
        P("tp", None),
        P(None, ("rep", "tp"), None),
        P(None, ("rep", "tp")),
        P(None, None, ("rep", "tp")),
        P(("rep", "tp"), None),
        P(None, ("rep", "tp")),
        P("rep", "tp", None, None),
        P("rep", "tp", None, None),
        P("rep"),
    )
    return jax.shard_map(
        local, mesh=mesh, in_specs=placed, out_specs=P("rep", "tp"), check_vma=False
    )
```

```python
import math

import jax
import jax.numpy as jnp
from jax import lax
from jax.experimental import pallas as pl
from jax.experimental.pallas import tpu as pltpu
from jax.sharding import PartitionSpec as P

MESH = pl.DeviceIdType.MESH
bf16, f32 = jnp.bfloat16, jnp.float32

epsilon = 1e-06
rope_base = 1000000.0
adapter_scale = 0.5

FEATURES = 8192
SEQS = 64
RANK = 64
HEAD = 128
QCOLS = 512
OUTC = 1024
TP = 8
CHIPS = 8
CHUNKS = 8
CHUNK = FEATURES // CHUNKS
DROWS = 96
UROWS = 80
GROUP = 16
PART = 512


def dot(a, b):
    return jnp.dot(a, b, preferred_element_type=f32)


def dot_nt(a, b):
    return lax.dot_general(a, b, (((1,), (1,)), ((), ())), preferred_element_type=f32)


def at_lanes(offset, rows):
    row = lax.broadcasted_iota(jnp.int32, (rows, 128), 0)
    lane = lax.broadcasted_iota(jnp.int32, (rows, 128), 1)
    return jnp.where(lane == row + offset, 1.0, 0.0).astype(bf16)


def kernel(
    hidden, gain, wq, wkv, wo, down, qup, kvup, odown, oup, keys, values, lengths,
    out,
    hid_v, nrm_v, wq_v, wkv_v, wo_v, k_v, v_v,
    down_v, qup_v, kvup_v, odown_v, oup_v, gain_v, len_v,
    dg, w2, ug, ute, utl, inner_p, inner_v, ou_v, od_v, mid_p,
    xs0, xr0, z1s, z1r, o1s, o1r, y1s, y1r, xs1, xr1, z0s, z0r, o0s, o0r, y0s, y0r,
    own1, own0, qacc, kacc, vacc, q_s, own_s, ctx_s, len_s, ctx_b,
    load_sem, wq_sem, wkv_sem, small_sem,
    d_send, d_recv, dd_sem, u_send, u_recv, t_send, t_recv, tt_sem, l_send, l_recv, ll_sem,
    i_send, i_recv, v_send, v_recv, m_send, m_recv,
    x0_send, x0_recv, x1_sem, z_send, z_recv,
):
    rep = lax.axis_index("rep")
    t = lax.axis_index("tp")
    chip = rep // 2
    core = rep % 2
    partner = chip * 2 + (1 - core)
    a, k = t // 4, t % 4
    other = 1 - a

    def chip_at(j):
        return lax.rem(chip + j, CHIPS)

    def tp_at(j):
        return lax.rem(t + j, TP)

    def z_at(d):
        return lax.rem(k + d, 4)

    def remote(src, dst, send_sem, recv_sem, rep_to, tp_to):
        return pltpu.make_async_remote_copy(
            src_ref=src, dst_ref=dst, send_sem=send_sem, recv_sem=recv_sem,
            device_id=(rep_to, tp_to), device_id_type=MESH)

    barrier = pltpu.get_barrier_semaphore()
    small = [
        pltpu.make_async_copy(src, dst, small_sem.at[i])
        for i, (src, dst) in enumerate(
            ((down, down_v), (qup, qup_v), (kvup, kvup_v), (odown, odown_v), (oup, oup_v),
             (gain, gain_v), (lengths, len_v))
        )
    ]
    small[0].start()
    pl.semaphore_signal(barrier, inc=1, device_id=(partner, t), device_id_type=MESH)
    for j in range(1, CHIPS):
        pl.semaphore_signal(barrier, inc=1, device_id=(chip_at(j) * 2 + core, t), device_id_type=MESH)
    for j in range(1, TP):
        pl.semaphore_signal(barrier, inc=1, device_id=(rep, tp_at(j)), device_id_type=MESH)
    for copy in small[1:]:
        copy.start()
    hid_copy = pltpu.make_async_copy(hidden, hid_v, load_sem.at[0])
    hid_copy.start()

    def wq_copy(i):
        rows = pl.ds(pl.multiple_of(i * CHUNK, CHUNK), CHUNK)
        return pltpu.make_async_copy(wq.at[rows, :], wq_v.at[rows, :], wq_sem.at[i])

    def wkv_copy(i):
        rows = pl.ds(pl.multiple_of(i * CHUNK, CHUNK), CHUNK)
        return pltpu.make_async_copy(wkv.at[:, rows, :], wkv_v.at[:, rows, :], wkv_sem.at[i])

    def start_chunk(i, carry):
        wq_copy(i).start()
        wkv_copy(i).start()
        return carry

    lax.fori_loop(0, CHUNKS, start_chunk, 0)
    key_copy = pltpu.make_async_copy(keys, k_v, load_sem.at[1])
    value_copy = pltpu.make_async_copy(values, v_v, load_sem.at[2])
    wo_copy = pltpu.make_async_copy(wo, wo_v, load_sem.at[3])
    key_copy.start()
    value_copy.start()
    wo_copy.start()

    low, high = at_lanes(0, RANK), at_lanes(64, RANK)
    with jax.named_scope("pack"):
        small[0].wait()
        dg[core, chip, 0:64, :] = (dot(down_v[0], low) + dot(down_v[1], high)).astype(bf16)
        dg[core, chip, 64:96, :] = (dot(down_v[2, 0:32, :], low) + dot(down_v[2, 32:64, :], high)).astype(bf16)
        for copy in small[1:]:
            copy.wait()
        ug[chip, 0:16, :] = (dot(qup_v[0:16, :], low) + dot(qup_v[16:32, :], high)).astype(bf16)
        last = dot(kvup_v[1], low) + dot(kvup_v[0], high)
        ug[chip, 16:32, :] = jnp.concatenate([last, jnp.zeros_like(last)], axis=0).astype(bf16)
        ug[chip, 32:48, :] = (dot(odown_v[0:16, :], low) + dot(odown_v[16:32, :], high)).astype(bf16)
        ug[chip, 48:80, :] = (dot(oup_v[0:32, :], low) + dot(oup_v[32:64, :], high)).astype(bf16)

    with jax.named_scope("barrier_wait"):
        pl.semaphore_wait(barrier, CHIPS + TP - 1)

    def d_copy(j):
        return remote(dg.at[core, chip], dg.at[core, chip], d_send.at[j], d_recv.at[j],
                      chip_at(j) * 2 + core, t)

    def u_copy(j):
        return remote(ug.at[chip], ug.at[chip], u_send.at[j], u_recv.at[j],
                      chip_at(j) * 2 + core, t)

    for j in range(1, CHIPS):
        d_copy(j).start()
    for j in range(1, CHIPS):
        u_copy(j).start()

    with jax.named_scope("hid_wait"):
        hid_copy.wait()

    def squares(i, total):
        cols = pl.ds(pl.multiple_of(i * CHUNK, CHUNK), CHUNK)
        x = hid_v[:, cols].astype(f32)
        x = x * x
        for n in range(CHUNK // 128):
            total = total + x[:, n * 128 : (n + 1) * 128]
        return total

    with jax.named_scope("norm"):
        total = lax.fori_loop(0, CHUNKS, squares, jnp.zeros((SEQS, 128), f32))
        square = jnp.sum(total, axis=-1, keepdims=True) * (1.0 / FEATURES)
        scale = lax.rsqrt(square + epsilon)

        def normalise(i, carry):
            cols = pl.ds(pl.multiple_of(i * CHUNK, CHUNK), CHUNK)
            x = hid_v[:, cols].astype(f32)
            nrm_v[:, cols] = (x * scale * gain_v[cols].astype(f32).reshape(1, CHUNK)).astype(bf16)
            return carry

        lax.fori_loop(0, CHUNKS, normalise, 0)

    w2[...] = jnp.zeros_like(w2)
    qacc[...] = jnp.zeros_like(qacc)
    kacc[...] = jnp.zeros_like(kacc)
    vacc[...] = jnp.zeros_like(vacc)

    def project(i, carry):
        wq_copy(i).wait()
        wkv_copy(i).wait()
        cols = pl.ds(pl.multiple_of(i * CHUNK, CHUNK), CHUNK)
        x = nrm_v[:, cols]
        qacc[...] += dot(x, wq_v[cols, :])
        kacc[...] += dot(x, wkv_v[0, cols, :])
        vacc[...] += dot(x, wkv_v[1, cols, :])
        return carry

    with jax.named_scope("project"):
        lax.fori_loop(0, CHUNKS, project, 0)

    lane = lax.broadcasted_iota(jnp.int32, (SEQS, 128), 1)
    left = lane < 64
    with jax.named_scope("angles"):
        lens = len_v[...].reshape(1, SEQS)
        square_rows = lax.broadcasted_iota(jnp.int32, (SEQS, SEQS), 0)
        square_lanes = lax.broadcasted_iota(jnp.int32, (SEQS, SEQS), 1)
        len_col = jnp.sum(
            jnp.where(square_rows == square_lanes, jnp.broadcast_to(lens, (SEQS, SEQS)), 0).astype(f32),
            axis=-1, keepdims=True)
        len_b = jnp.broadcast_to(len_col, (SEQS, 128))
        for h in range(8):
            len_s[pl.ds(h, SEQS, stride=8), :] = len_b
        index = (lane % 64).astype(f32)
        frequency = jnp.exp(index * (-2.0 / HEAD * math.log(rope_base)))
        angles = len_b * frequency
        cosine = jnp.cos(angles)
        sine = jnp.where(left, -jnp.sin(angles), jnp.sin(angles))

    def rotate(x):
        return x * cosine + pltpu.roll(x, 64, axis=1) * sine

    with jax.named_scope("d_wait"):
        for j in range(1, CHIPS):
            d_copy(j).wait_recv()
    across = remote(dg.at[core], dg.at[core], dd_sem.at[0], dd_sem.at[1], partner, t)
    across.start()

    half = pl.multiple_of((t % 2) * 64, 64)

    def spread(c):
        for q in range(CHIPS):
            w2[c, q, pl.ds(half, 64), 0:128] = dg[c, q, 0:64, :]
            tail = dg[c, q, 64:96, :].astype(f32)
            both = jnp.concatenate([tail, pltpu.roll(tail, 64, axis=1)], axis=0)
            w2[c, q, pl.ds(half, 64), 128:256] = both.astype(bf16)

    def features(c):
        total = jnp.zeros((SEQS, 256), f32)
        for q in range(CHIPS):
            at = (q * 2 + c) * QCOLS + (t // 2) * 128
            total = total + dot(nrm_v[:, pl.ds(pl.multiple_of(at, 128), 128)], w2[c, q])
        return total

    with jax.named_scope("inner_own"):
        spread(core)
        partial = features(core)

    with jax.named_scope("u_wait"):
        for j in range(1, CHIPS):
            u_copy(j).wait_recv()

    def t_copy(j):
        return remote(ug.at[tp_at(j), 0:32], ute.at[core, t], t_send.at[j], t_recv.at[j], rep, tp_at(j))

    def l_copy(j):
        return remote(ug.at[tp_at(j), 32:80], utl.at[core, t], l_send.at[j], l_recv.at[j], rep, tp_at(j))

    for j in range(1, TP):
        t_copy(j).start()
    ute[core, t] = ug[t, 0:32]
    utl[core, t] = ug[t, 32:80]

    with jax.named_scope("across_wait"):
        across.wait_recv()
    with jax.named_scope("inner_other"):
        spread(1 - core)
        partial = partial + features(1 - core)
        inner_p[t] = partial[:, 0:128].astype(bf16)
        tail = partial[:, 128:256]
        tail = jnp.where(left[0:32], tail[0:32], pltpu.roll(tail[32:64], 64, axis=1))
        inner_v[t] = tail.astype(bf16)

    def i_copy(j):
        return remote(inner_p.at[t], inner_p.at[t], i_send.at[j], i_recv.at[j], rep, tp_at(j))

    def v_copy(j):
        return remote(inner_v.at[t], inner_v.at[t], v_send.at[j], v_recv.at[j], rep, tp_at(j))

    for j in range(1, TP):
        i_copy(j).start()
    for j in range(1, TP):
        v_copy(j).start()
    for j in range(1, TP):
        l_copy(j).start()

    with jax.named_scope("t_wait"):
        for j in range(1, TP):
            t_copy(j).wait_recv()
    t_across = remote(ute.at[core], ute.at[core], tt_sem.at[0], tt_sem.at[1], partner, t)
    t_across.start()
    with jax.named_scope("up_wait"):
        t_across.wait_recv()
    with jax.named_scope("unpack"):
        rows = []
        for n in range(2 * TP):
            e = ute[n // TP, n % TP, 0:16, :].astype(f32)
            rows += [e, pltpu.roll(e, 64, axis=1)]
        up_rows = jnp.concatenate(rows, axis=0).astype(bf16)
        kv_rows = jnp.concatenate(
            [ute[n // TP, n % TP, 16:32, :].astype(f32)[0:8] for n in range(2 * TP)], axis=0).astype(bf16)

    with jax.named_scope("i_wait"):
        for j in range(1, TP):
            i_copy(j).wait_recv()
    score_scale = 1.0 / math.sqrt(HEAD)
    with jax.named_scope("queries"):
        inner = inner_p[0].astype(f32)
        for n in range(1, TP):
            inner = inner + inner_p[n].astype(f32)
        inner_q = jnp.where(left, inner, 0.0).astype(bf16)
        inner_k = jnp.where(left, 0.0, inner).astype(bf16)
        new_key = rotate(kacc[...] + adapter_scale * dot_nt(inner_k, kv_rows)).astype(bf16).astype(f32)
        query = qacc[...] + adapter_scale * dot_nt(inner_q, up_rows)
        for h in range(4):
            x = rotate(query[:, h * HEAD : (h + 1) * HEAD])
            main = x.astype(bf16).astype(f32)
            own = jnp.sum(x * new_key, axis=-1, keepdims=True) * score_scale
            own = jnp.broadcast_to(own, (SEQS, 128))
            q_s[pl.ds(h, SEQS, stride=8), :] = main
            q_s[pl.ds(h + 4, SEQS, stride=8), :] = x - main
            own_s[pl.ds(h, SEQS, stride=8), :] = own
            own_s[pl.ds(h + 4, SEQS, stride=8), :] = own

    with jax.named_scope("late_wait"):
        for j in range(1, TP):
            v_copy(j).wait_recv()
        for j in range(1, TP):
            l_copy(j).wait_recv()
    l_across = remote(utl.at[core], utl.at[core], ll_sem.at[0], ll_sem.at[1], partner, t)
    l_across.start()

    with jax.named_scope("cache_wait"):
        key_copy.wait()
        value_copy.wait()
    wide = 8 * GROUP
    position = lax.broadcasted_iota(jnp.int32, (wide, 128), 1).astype(f32)

    def attend(g, carry):
        rows = pl.ds(pl.multiple_of(g * wide, wide), wide)
        q_rows = q_s[rows, :].astype(bf16)
        scores = []
        for s in range(GROUP):
            sc = dot_nt(q_rows[s * 8 : (s + 1) * 8], k_v[g * GROUP + s, 0])
            scores.append(sc + pltpu.roll(sc, 4, axis=0))
        scores = jnp.concatenate(scores, axis=0) * score_scale
        own = own_s[rows, :]
        live = position < len_s[rows, :]
        row_max = jnp.maximum(
            jnp.max(jnp.where(live, scores, -1e30), axis=-1, keepdims=True), own)
        weights = jnp.where(live, jnp.exp(scores - row_max), 0.0)
        own_weight = jnp.exp(own - row_max)
        denom = jnp.sum(weights, axis=-1, keepdims=True) + own_weight
        probs = (weights / denom).astype(bf16)
        own_s[rows, :] = (own_weight / denom).astype(bf16).astype(f32)
        parts = [
            dot(probs[s * 8 : (s + 1) * 8], v_v[g * GROUP + s, 0]) for s in range(GROUP)
        ]
        ctx_s[rows, :] = jnp.concatenate(parts, axis=0)
        return carry

    with jax.named_scope("attend"):
        lax.fori_loop(0, SEQS // GROUP, attend, 0)

    with jax.named_scope("context"):
        l_across.wait_recv()
        inner = inner_v[0].astype(f32)
        for n in range(1, TP):
            inner = inner + inner_v[n].astype(f32)
        inner = jnp.concatenate([inner, pltpu.roll(inner, 64, axis=1)], axis=0)
        inner = jnp.where(left, inner, 0.0).astype(bf16)
        new_value = (vacc[...] + adapter_scale * dot_nt(inner, kv_rows)).astype(bf16).astype(f32)
        for h in range(4):
            x = ctx_s[pl.ds(h, SEQS, stride=8), :] + own_s[pl.ds(h, SEQS, stride=8), :] * new_value
            ctx_b[:, h * HEAD : (h + 1) * HEAD] = x.astype(bf16)

    def m_copy(j):
        return remote(mid_p.at[t], mid_p.at[t], m_send.at[j], m_recv.at[j], rep, tp_at(j))

    with jax.named_scope("middle"):
        for n in range(2 * TP):
            e = utl[n // TP, n % TP, 0:16, :].astype(f32)
            e = jnp.concatenate([e, pltpu.roll(e, 64, axis=1)], axis=0)
            od_v[n * 32 : (n + 1) * 32, :] = e.astype(bf16)
        middle = dot(ctx_b[...], od_v[...])
        middle = jnp.where(left[0:32], middle[0:32], pltpu.roll(middle[32:64], 64, axis=1))
        mid_p[t] = middle.astype(bf16)
        for j in range(1, TP):
            m_copy(j).start()

    with jax.named_scope("wo_wait"):
        wo_copy.wait()

    z_minus, z_plus = a * 4 + z_at(3), a * 4 + z_at(1)
    across_x = other * 4 + k

    def block(a_to, d, part):
        at = (a_to * 4 + z_at(d)) * OUTC + part * PART
        return dot(ctx_b[...], wo_v[:, pl.ds(pl.multiple_of(at, PART), PART)])

    def x0_copy(d):
        return remote(xs0.at[d], xr0.at[d], x0_send.at[d], x0_recv.at[d], rep, across_x)

    x1_copy = remote(xs1, xr1, x1_sem.at[0], x1_sem.at[1], rep, across_x)

    def z_copy(src, dst, n, way):
        return remote(src.at[way], dst.at[way], z_send.at[n, way], z_recv.at[n, way],
                      rep, z_minus if way == 0 else z_plus)

    with jax.named_scope("send1"):
        for a_to in range(2):
            x = block(a_to, 2, 1).astype(bf16)
            z1s[0, :, a_to * PART : (a_to + 1) * PART] = x[0:32]
            z1s[1, :, a_to * PART : (a_to + 1) * PART] = x[32:64]
        for way in range(2):
            z_copy(z1s, z1r, 0, way).start()
    with jax.named_scope("send2"):
        for d in (2, 3, 1, 0):
            xs0[d] = block(other, d, 0).astype(bf16)
            x0_copy(d).start()
    with jax.named_scope("send3"):
        for way, d in ((0, 3), (1, 1)):
            for a_to in range(2):
                cols = slice(a_to * PART, (a_to + 1) * PART)
                x = block(a_to, d, 1)
                sent, kept = (x[32:64], x[0:32]) if way == 0 else (x[0:32], x[32:64])
                o1s[way, :, cols] = sent.astype(bf16)
                own1[way, :, cols] = kept
            z_copy(o1s, o1r, 1, way).start()
    with jax.named_scope("own"):
        for d in (2, 3, 1, 0):
            own0[d] = block(a, d, 0)
    with jax.named_scope("relay1"):
        for way in range(2):
            z_copy(z1s, z1r, 0, way).wait_recv()
            y1s[way] = (own1[way] + z1r[way].astype(f32)).astype(bf16)
            z_copy(y1s, y1r, 2, way).start()
    with jax.named_scope("xfirst"):
        x0_copy(2).wait_recv()
        x = (own0[2] + xr0[2].astype(f32)).astype(bf16)
        z0s[0], z0s[1] = x[0:32], x[32:64]
        for way in range(2):
            z_copy(z0s, z0r, 3, way).start()
        for way, d in ((0, 3), (1, 1)):
            x0_copy(d).wait_recv()
            x = own0[d] + xr0[d].astype(f32)
            sent, kept = (x[32:64], x[0:32]) if way == 0 else (x[0:32], x[32:64])
            o0s[way] = sent.astype(bf16)
            own0[d, 0:32] = kept
            z_copy(o0s, o0r, 4, way).start()
    with jax.named_scope("relay0"):
        for way, d in ((0, 3), (1, 1)):
            z_copy(z0s, z0r, 3, way).wait_recv()
            y0s[way] = (own0[d, 0:32] + z0r[way].astype(f32)).astype(bf16)
            z_copy(y0s, y0r, 5, way).start()
    with jax.named_scope("own1"):
        mine = [block(other, 0, 1), block(a, 0, 1)]
    with jax.named_scope("ou"):
        for n in range(TP):
            e = utl[(2 * n) // TP, (2 * n) % TP, 16:48, :].astype(f32)
            g = utl[(2 * n) // TP, (2 * n + 1) % TP, 16:48, :].astype(f32)
            e_r, g_r = pltpu.roll(e, 64, axis=1), pltpu.roll(g, 64, axis=1)
            ou_v[0:32, n * 128 : (n + 1) * 128] = jnp.where(left[0:32], e, g_r).astype(bf16)
            ou_v[32:64, n * 128 : (n + 1) * 128] = jnp.where(left[0:32], e_r, g).astype(bf16)
    with jax.named_scope("m_wait"):
        for j in range(1, TP):
            m_copy(j).wait_recv()
    with jax.named_scope("delta"):
        middle = mid_p[0].astype(f32)
        for n in range(1, TP):
            middle = middle + mid_p[n].astype(f32)
        middle = jnp.concatenate([middle, pltpu.roll(middle, 64, axis=1)], axis=0)[:, 0:64].astype(bf16)
        delta = adapter_scale * dot(middle, ou_v[...])
    with jax.named_scope("z1_wait"):
        for way in range(2):
            z_copy(o1s, o1r, 1, way).wait_recv()
        for way in range(2):
            z_copy(y1s, y1r, 2, way).wait_recv()
    with jax.named_scope("sum1"):

        def arrived(a_to):
            cols = pl.ds(pl.multiple_of(a_to * PART, PART), PART)
            top = y1r[0, :, cols].astype(f32) + o1r[1, :, cols].astype(f32)
            bottom = y1r[1, :, cols].astype(f32) + o1r[0, :, cols].astype(f32)
            return jnp.concatenate([top, bottom], axis=0)

        xs1[...] = (mine[0] + arrived(other)).astype(bf16)
        x1_copy.start()
        high_half = mine[1] + arrived(a) + delta[:, PART:]
    with jax.named_scope("z0_wait"):
        x0_copy(0).wait_recv()
        for way in range(2):
            z_copy(o0s, o0r, 4, way).wait_recv()
        for way in range(2):
            z_copy(y0s, y0r, 5, way).wait_recv()
    with jax.named_scope("sum0"):
        top = y0r[0].astype(f32) + o0r[1].astype(f32)
        bottom = y0r[1].astype(f32) + o0r[0].astype(f32)
        x = own0[0] + xr0[0].astype(f32) + jnp.concatenate([top, bottom], axis=0)
        out[:, 0:PART] = (x + delta[:, 0:PART]).astype(bf16)
    with jax.named_scope("x1_wait"):
        x1_copy.wait_recv()
    out[:, PART:] = (high_half + xr1[...].astype(f32)).astype(bf16)

    with jax.named_scope("drain"):
        for j in range(1, CHIPS):
            d_copy(j).wait_send()
            u_copy(j).wait_send()
        across.wait_send()
        t_across.wait_send()
        l_across.wait_send()
        for j in range(1, TP):
            i_copy(j).wait_send()
            v_copy(j).wait_send()
            t_copy(j).wait_send()
            l_copy(j).wait_send()
            m_copy(j).wait_send()
        for d in range(4):
            x0_copy(d).wait_send()
        x1_copy.wait_send()
        for way in range(2):
            for n, (src, dst) in enumerate(
                ((z1s, z1r), (o1s, o1r), (y1s, y1r), (z0s, z0r), (o0s, o0r), (y0s, y0r))
            ):
                z_copy(src, dst, n, way).wait_send()


def local(
    hidden, norm_gain, query_weight_matrix, key_value_weight, output_weight_matrix,
    input_down_factors, query_up_factor, key_value_up_factors, output_down_factor,
    output_up_factor, cache_keys, cache_values, lengths,
):
    hbm = pl.BlockSpec(memory_space=pltpu.HBM)
    dma = pltpu.SemaphoreType.DMA
    vmem = pltpu.VMEM
    half_block = vmem((2, 32, OUTC), bf16)
    half_part = vmem((2, 32, PART), bf16)
    return pl.pallas_call(
        kernel,
        out_shape=jax.ShapeDtypeStruct((SEQS, OUTC), bf16),
        in_specs=[hbm] * 13,
        out_specs=pl.BlockSpec(memory_space=pltpu.VMEM),
        scratch_shapes=[
            vmem((SEQS, FEATURES), bf16),
            vmem((SEQS, FEATURES), bf16),
            vmem((FEATURES, QCOLS), bf16),
            vmem((2, FEATURES, HEAD), bf16),
            vmem((QCOLS, FEATURES), bf16),
            vmem((SEQS, 1, 128, HEAD), bf16),
            vmem((SEQS, 1, 128, HEAD), bf16),
            vmem((3, 64, RANK), bf16),
            vmem((32, RANK), bf16),
            vmem((2, 8, RANK), bf16),
            vmem((32, RANK), bf16),
            vmem((RANK, 64), bf16),
            vmem((FEATURES,), bf16),
            vmem((SEQS,), jnp.int32),
            vmem((2, CHIPS, DROWS, 128), bf16),
            vmem((2, CHIPS, 128, 256), bf16),
            vmem((CHIPS, UROWS, 128), bf16),
            vmem((2, TP, 32, 128), bf16),
            vmem((2, TP, 48, 128), bf16),
            vmem((TP, SEQS, 128), bf16),
            vmem((TP, 32, 128), bf16),
            vmem((RANK, OUTC), bf16),
            vmem((QCOLS, 128), bf16),
            vmem((TP, 32, 128), bf16),
            vmem((4, SEQS, PART), bf16),
            vmem((4, SEQS, PART), bf16),
            half_block, half_block, half_block, half_block, half_block, half_block,
            vmem((SEQS, PART), bf16),
            vmem((SEQS, PART), bf16),
            half_part, half_part, half_part, half_part, half_part, half_part,
            vmem((2, 32, OUTC), f32),
            vmem((4, SEQS, PART), f32),
            vmem((SEQS, QCOLS), f32),
            vmem((SEQS, HEAD), f32),
            vmem((SEQS, HEAD), f32),
            vmem((SEQS * 8, HEAD), f32),
            vmem((SEQS * 8, HEAD), f32),
            vmem((SEQS * 8, HEAD), f32),
            vmem((SEQS * 8, HEAD), f32),
            vmem((SEQS, QCOLS), bf16),
            dma((4,)), dma((CHUNKS,)), dma((CHUNKS,)), dma((7,)),
            dma((CHIPS,)), dma((CHIPS,)), dma((2,)), dma((CHIPS,)), dma((CHIPS,)),
            dma((TP,)), dma((TP,)), dma((2,)), dma((TP,)), dma((TP,)), dma((2,)),
            dma((TP,)), dma((TP,)), dma((TP,)), dma((TP,)), dma((TP,)), dma((TP,)),
            dma((4,)), dma((4,)), dma((2,)), dma((6, 2)), dma((6, 2)),
        ],
        compiler_params=pltpu.CompilerParams(
            collective_id=0, has_side_effects=True, vmem_limit_bytes=48 * 1024 * 1024),
        cost_estimate=pl.CostEstimate(
            flops=3 * 10**9, bytes_accessed=26 * 2**20, transcendentals=0),
    )(*[pltpu.with_memory_space_constraint(x, pltpu.HBM) for x in (
        hidden, norm_gain, query_weight_matrix, key_value_weight,
        output_weight_matrix, input_down_factors, jnp.swapaxes(query_up_factor, 0, 1),
        jnp.swapaxes(key_value_up_factors, 1, 2), output_down_factor, output_up_factor,
        cache_keys, cache_values, lengths,
    )])


def solution(mesh):
    placed = (
        P("rep", None),
        P(),
        P(None, "tp"),
        P(None, None, "tp"),
        P("tp", None),
        P(None, ("rep", "tp"), None),
        P(None, ("rep", "tp")),
        P(None, None, ("rep", "tp")),
        P(("rep", "tp"), None),
        P(None, ("rep", "tp")),
        P("rep", "tp", None, None),
        P("rep", "tp", None, None),
        P("rep"),
    )
    return jax.shard_map(
        local, mesh=mesh, in_specs=placed, out_specs=P("rep", "tp"), check_vma=False
    )
```

```python
import math

import jax
import jax.numpy as jnp
from jax import lax
from jax.experimental import pallas as pl
from jax.experimental.pallas import tpu as pltpu
from jax.sharding import PartitionSpec as P

MESH = pl.DeviceIdType.MESH
bf16, f32 = jnp.bfloat16, jnp.float32

epsilon = 1e-06
rope_base = 1000000.0
adapter_scale = 0.5

FEATURES = 8192
SEQS = 64
RANK = 64
HEAD = 128
QCOLS = 512
OUTC = 1024
TP = 8
CHIPS = 8
CHUNKS = 8
CHUNK = FEATURES // CHUNKS
DROWS = 96
UROWS = 80
GROUP = 32
PART = 512


def dot(a, b):
    return jnp.dot(a, b, preferred_element_type=f32)


def dot_nt(a, b):
    return lax.dot_general(a, b, (((1,), (1,)), ((), ())), preferred_element_type=f32)


def at_lanes(offset, rows):
    row = lax.broadcasted_iota(jnp.int32, (rows, 128), 0)
    lane = lax.broadcasted_iota(jnp.int32, (rows, 128), 1)
    return jnp.where(lane == row + offset, 1.0, 0.0).astype(bf16)


def kernel(
    hidden, gain, wq, wkv, wo, down, qup, kvup, odown, oup, keys, values, lengths,
    out,
    hid_v, nrm_v, wq_v, wkv_v, wo_v, k_v, v_v,
    down_v, qup_v, kvup_v, odown_v, oup_v, gain_v, len_v,
    dg, w2, ug, ute, utl, inner_p, inner_v, ou_v, od_v, mid_p,
    xs0, xr0, zs, zr, xs1, xr1, kept, own0, mine, qacc, kacc, vacc, q_s, own_s, ctx_s, len_s, ctx_b,
    load_sem, wq_sem, wkv_sem, small_sem,
    d_send, d_recv, dd_send, dd_recv, u_send, u_recv, t_send, t_recv, tt_sem, l_send, l_recv, ll_sem,
    i_send, i_recv, v_send, v_recv, m_send, m_recv,
    x0_send, x0_recv, x1_sem, z_send, z_recv,
):
    rep = lax.axis_index("rep")
    t = lax.axis_index("tp")
    chip = rep // 2
    core = rep % 2
    partner = chip * 2 + (1 - core)
    a, k = t // 4, t % 4
    other = 1 - a

    def chip_at(j):
        return lax.rem(chip + j, CHIPS)

    def tp_of(j):
        return t if j % 2 == 0 else lax.rem(t + 4, TP)

    def gather_peer(j):
        return chip_at(j) * 2 + core, tp_of(j)

    far_first = (4, 3, 5, 1, 7, 2, 6)

    def tp_at(j):
        return lax.rem(t + j, TP)

    def z_at(d):
        return lax.rem(k + d, 4)

    def remote(src, dst, send_sem, recv_sem, rep_to, tp_to):
        return pltpu.make_async_remote_copy(
            src_ref=src, dst_ref=dst, send_sem=send_sem, recv_sem=recv_sem,
            device_id=(rep_to, tp_to), device_id_type=MESH)

    barrier = pltpu.get_barrier_semaphore()
    small = [
        pltpu.make_async_copy(src, dst, small_sem.at[i])
        for i, (src, dst) in enumerate(
            ((down, down_v), (qup, qup_v), (kvup, kvup_v), (odown, odown_v), (oup, oup_v),
             (gain, gain_v), (lengths, len_v))
        )
    ]
    small[0].start()
    pl.semaphore_signal(barrier, inc=1, device_id=(partner, t), device_id_type=MESH)
    for j in range(1, CHIPS):
        pl.semaphore_signal(barrier, inc=1, device_id=gather_peer(j), device_id_type=MESH)
    for j in range(1, TP):
        pl.semaphore_signal(barrier, inc=1, device_id=(rep, tp_at(j)), device_id_type=MESH)
    for copy in small[1:]:
        copy.start()
    hid_copy = pltpu.make_async_copy(hidden, hid_v, load_sem.at[0])
    hid_copy.start()

    def wq_copy(i):
        rows = pl.ds(pl.multiple_of(i * CHUNK, CHUNK), CHUNK)
        return pltpu.make_async_copy(wq.at[rows, :], wq_v.at[rows, :], wq_sem.at[i])

    def wkv_copy(i):
        rows = pl.ds(pl.multiple_of(i * CHUNK, CHUNK), CHUNK)
        return pltpu.make_async_copy(wkv.at[:, rows, :], wkv_v.at[:, rows, :], wkv_sem.at[i])

    def start_chunk(i, carry):
        wq_copy(i).start()
        wkv_copy(i).start()
        return carry

    lax.fori_loop(0, CHUNKS, start_chunk, 0)
    key_copy = pltpu.make_async_copy(keys, k_v, load_sem.at[1])
    value_copy = pltpu.make_async_copy(values, v_v, load_sem.at[2])
    wo_copy = pltpu.make_async_copy(wo, wo_v, load_sem.at[3])
    key_copy.start()
    value_copy.start()
    wo_copy.start()

    low, high = at_lanes(0, RANK), at_lanes(64, RANK)
    with jax.named_scope("pack"):
        small[0].wait()
        dg[core, chip, 0:64, :] = (dot(down_v[0], low) + dot(down_v[1], high)).astype(bf16)
        dg[core, chip, 64:96, :] = (dot(down_v[2, 0:32, :], low) + dot(down_v[2, 32:64, :], high)).astype(bf16)
        for copy in small[1:]:
            copy.wait()
        ug[chip, 0:16, :] = (dot(qup_v[0:16, :], low) + dot(qup_v[16:32, :], high)).astype(bf16)
        last = dot(kvup_v[1], low) + dot(kvup_v[0], high)
        ug[chip, 16:32, :] = jnp.concatenate([last, jnp.zeros_like(last)], axis=0).astype(bf16)
        ug[chip, 32:48, :] = (dot(odown_v[0:16, :], low) + dot(odown_v[16:32, :], high)).astype(bf16)
        ug[chip, 48:80, :] = (dot(oup_v[0:32, :], low) + dot(oup_v[32:64, :], high)).astype(bf16)

    with jax.named_scope("barrier_wait"):
        pl.semaphore_wait(barrier, CHIPS + TP - 1)

    def d_copy(j):
        return remote(dg.at[core, chip], dg.at[core, chip], d_send.at[j], d_recv.at[j],
                      *gather_peer(j))

    def u_copy(j):
        return remote(ug.at[chip], ug.at[chip], u_send.at[j], u_recv.at[j],
                      *gather_peer(j))

    def across(j):
        q = lax.rem(chip + CHIPS - j, CHIPS)
        return remote(dg.at[core, q], dg.at[core, q], dd_send.at[j], dd_recv.at[j], partner, t)

    for j in far_first:
        d_copy(j).start()
    across(0).start()
    for j in far_first:
        u_copy(j).start()

    with jax.named_scope("hid_wait"):
        hid_copy.wait()

    def squares(i, total):
        cols = pl.ds(pl.multiple_of(i * CHUNK, CHUNK), CHUNK)
        x = hid_v[:, cols].astype(f32)
        x = x * x
        for n in range(CHUNK // 128):
            total = total + x[:, n * 128 : (n + 1) * 128]
        return total

    with jax.named_scope("norm"):
        total = lax.fori_loop(0, CHUNKS, squares, jnp.zeros((SEQS, 128), f32))
        square = jnp.sum(total, axis=-1, keepdims=True) * (1.0 / FEATURES)
        scale = lax.rsqrt(square + epsilon)

        def normalise(i, carry):
            cols = pl.ds(pl.multiple_of(i * CHUNK, CHUNK), CHUNK)
            x = hid_v[:, cols].astype(f32)
            nrm_v[:, cols] = (x * scale * gain_v[cols].astype(f32).reshape(1, CHUNK)).astype(bf16)
            return carry

        lax.fori_loop(0, CHUNKS, normalise, 0)

    w2[...] = jnp.zeros_like(w2)
    qacc[...] = jnp.zeros_like(qacc)
    kacc[...] = jnp.zeros_like(kacc)
    vacc[...] = jnp.zeros_like(vacc)

    def project(i, carry):
        wq_copy(i).wait()
        wkv_copy(i).wait()
        cols = pl.ds(pl.multiple_of(i * CHUNK, CHUNK), CHUNK)
        x = nrm_v[:, cols]
        qacc[...] += dot(x, wq_v[cols, :])
        kacc[...] += dot(x, wkv_v[0, cols, :])
        vacc[...] += dot(x, wkv_v[1, cols, :])
        return carry

    with jax.named_scope("project"):
        lax.fori_loop(0, CHUNKS, project, 0)

    lane = lax.broadcasted_iota(jnp.int32, (SEQS, 128), 1)
    left = lane < 64
    with jax.named_scope("angles"):
        lens = len_v[...].reshape(1, SEQS)
        square_rows = lax.broadcasted_iota(jnp.int32, (SEQS, SEQS), 0)
        square_lanes = lax.broadcasted_iota(jnp.int32, (SEQS, SEQS), 1)
        len_col = jnp.sum(
            jnp.where(square_rows == square_lanes, jnp.broadcast_to(lens, (SEQS, SEQS)), 0).astype(f32),
            axis=-1, keepdims=True)
        len_b = jnp.broadcast_to(len_col, (SEQS, 128))
        for h in range(8):
            len_s[pl.ds(h, SEQS, stride=8), :] = len_b
        index = (lane % 64).astype(f32)
        frequency = jnp.exp(index * (-2.0 / HEAD * math.log(rope_base)))
        angles = len_b * frequency
        cosine = jnp.cos(angles)
        sine = jnp.where(left, -jnp.sin(angles), jnp.sin(angles))

    def rotate(x):
        return x * cosine + pltpu.roll(x, 64, axis=1) * sine

    with jax.named_scope("d_wait"):
        for j in range(1, CHIPS):
            d_copy(j).wait_recv()
            across(j).start()

    half = pl.multiple_of((t % 2) * 64, 64)

    def spread(c):
        for q in range(CHIPS):
            w2[c, q, pl.ds(half, 64), 0:128] = dg[c, q, 0:64, :]
            tail = dg[c, q, 64:96, :].astype(f32)
            both = jnp.concatenate([tail, pltpu.roll(tail, 64, axis=1)], axis=0)
            w2[c, q, pl.ds(half, 64), 128:256] = both.astype(bf16)

    def features(c):
        total = jnp.zeros((SEQS, 256), f32)
        for j in range(CHIPS):
            at = (chip_at(j) * 2 + c) * QCOLS + (tp_of(j) // 2) * 128
            total = total + dot(nrm_v[:, pl.ds(pl.multiple_of(at, 128), 128)], w2[c, chip_at(j)])
        return total

    with jax.named_scope("inner_own"):
        spread(core)
        partial = features(core)

    with jax.named_scope("u_wait"):
        for j in range(1, CHIPS):
            u_copy(j).wait_recv()

    def slot_for(to):
        return lax.rem(t + 4 * lax.rem(to + chip, 2), TP)

    def t_copy(j):
        to = tp_at(j)
        return remote(ug.at[to, 0:32], ute.at[core, slot_for(to)], t_send.at[j], t_recv.at[j], rep, to)

    def l_copy(j):
        to = tp_at(j)
        return remote(ug.at[to, 32:80], utl.at[core, slot_for(to)], l_send.at[j], l_recv.at[j], rep, to)

    for j in range(1, TP):
        t_copy(j).start()
    ute[core, slot_for(t)] = ug[t, 0:32]
    utl[core, slot_for(t)] = ug[t, 32:80]

    with jax.named_scope("across_wait"):
        for j in range(CHIPS):
            across(j).wait_recv()
    with jax.named_scope("inner_other"):
        spread(1 - core)
        partial = partial + features(1 - core)
        inner_p[t] = partial[:, 0:128].astype(bf16)
        tail = partial[:, 128:256]
        tail = jnp.where(left[0:32], tail[0:32], pltpu.roll(tail[32:64], 64, axis=1))
        inner_v[t] = tail.astype(bf16)

    def i_copy(j):
        return remote(inner_p.at[t], inner_p.at[t], i_send.at[j], i_recv.at[j], rep, tp_at(j))

    def v_copy(j):
        return remote(inner_v.at[t], inner_v.at[t], v_send.at[j], v_recv.at[j], rep, tp_at(j))

    for j in range(1, TP):
        i_copy(j).start()
    for j in range(1, TP):
        v_copy(j).start()
    for j in range(1, TP):
        l_copy(j).start()

    with jax.named_scope("t_wait"):
        for j in range(1, TP):
            t_copy(j).wait_recv()
    t_across = remote(ute.at[core], ute.at[core], tt_sem.at[0], tt_sem.at[1], partner, t)
    t_across.start()
    with jax.named_scope("up_wait"):
        t_across.wait_recv()
    with jax.named_scope("unpack"):
        rows = []
        for n in range(2 * TP):
            e = ute[n // TP, n % TP, 0:16, :].astype(f32)
            rows += [e, pltpu.roll(e, 64, axis=1)]
        up_rows = jnp.concatenate(rows, axis=0).astype(bf16)
        kv_rows = jnp.concatenate(
            [ute[n // TP, n % TP, 16:32, :].astype(f32)[0:8] for n in range(2 * TP)], axis=0).astype(bf16)

    with jax.named_scope("i_wait"):
        for j in range(1, TP):
            i_copy(j).wait_recv()
    score_scale = 1.0 / math.sqrt(HEAD)
    with jax.named_scope("queries"):
        inner = inner_p[0].astype(f32)
        for n in range(1, TP):
            inner = inner + inner_p[n].astype(f32)
        inner_q = jnp.where(left, inner, 0.0).astype(bf16)
        inner_k = jnp.where(left, 0.0, inner).astype(bf16)
        new_key = rotate(kacc[...] + adapter_scale * dot_nt(inner_k, kv_rows)).astype(bf16).astype(f32)
        query = qacc[...] + adapter_scale * dot_nt(inner_q, up_rows)
        for h in range(4):
            x = rotate(query[:, h * HEAD : (h + 1) * HEAD])
            main = x.astype(bf16).astype(f32)
            own = jnp.sum(x * new_key, axis=-1, keepdims=True) * score_scale
            own = jnp.broadcast_to(own, (SEQS, 128))
            q_s[pl.ds(h, SEQS, stride=8), :] = main
            q_s[pl.ds(h + 4, SEQS, stride=8), :] = x - main
            own_s[pl.ds(h, SEQS, stride=8), :] = own
            own_s[pl.ds(h + 4, SEQS, stride=8), :] = own

    with jax.named_scope("cache_wait"):
        key_copy.wait()
        value_copy.wait()
    wide = 8 * GROUP
    position = lax.broadcasted_iota(jnp.int32, (wide, 128), 1).astype(f32)

    def attend(g, carry):
        rows = pl.ds(pl.multiple_of(g * wide, wide), wide)
        q_rows = q_s[rows, :].astype(bf16)
        scores = []
        for s in range(GROUP):
            sc = dot_nt(q_rows[s * 8 : (s + 1) * 8], k_v[g * GROUP + s, 0])
            scores.append(sc + pltpu.roll(sc, 4, axis=0))
        scores = jnp.concatenate(scores, axis=0) * score_scale
        own = own_s[rows, :]
        live = position < len_s[rows, :]
        row_max = jnp.maximum(
            jnp.max(jnp.where(live, scores, -1e30), axis=-1, keepdims=True), own)
        weights = jnp.where(live, jnp.exp(scores - row_max), 0.0)
        own_weight = jnp.exp(own - row_max)
        denom = jnp.sum(weights, axis=-1, keepdims=True) + own_weight
        probs = (weights / denom).astype(bf16)
        own_s[rows, :] = (own_weight / denom).astype(bf16).astype(f32)
        parts = [
            dot(probs[s * 8 : (s + 1) * 8], v_v[g * GROUP + s, 0]) for s in range(GROUP)
        ]
        ctx_s[rows, :] = jnp.concatenate(parts, axis=0)
        return carry

    with jax.named_scope("attend"):
        lax.fori_loop(0, SEQS // GROUP // 2, attend, 0)
    with jax.named_scope("late_wait"):
        for j in range(1, TP):
            v_copy(j).wait_recv()
        for j in range(1, TP):
            l_copy(j).wait_recv()
    l_across = remote(utl.at[core], utl.at[core], ll_sem.at[0], ll_sem.at[1], partner, t)
    l_across.start()
    with jax.named_scope("attend2"):
        lax.fori_loop(SEQS // GROUP // 2, SEQS // GROUP, attend, 0)

    with jax.named_scope("context"):
        l_across.wait_recv()
        for n in range(2 * TP):
            e = utl[n // TP, n % TP, 0:16, :].astype(f32)
            e = jnp.concatenate([e, pltpu.roll(e, 64, axis=1)], axis=0)
            od_v[n * 32 : (n + 1) * 32, :] = e.astype(bf16)
        inner = inner_v[0].astype(f32)
        for n in range(1, TP):
            inner = inner + inner_v[n].astype(f32)
        inner = jnp.concatenate([inner, pltpu.roll(inner, 64, axis=1)], axis=0)
        inner = jnp.where(left, inner, 0.0).astype(bf16)
        new_value = (vacc[...] + adapter_scale * dot_nt(inner, kv_rows)).astype(bf16).astype(f32)
        for h in range(4):
            x = ctx_s[pl.ds(h, SEQS, stride=8), :] + own_s[pl.ds(h, SEQS, stride=8), :] * new_value
            ctx_b[:, h * HEAD : (h + 1) * HEAD] = x.astype(bf16)

    with jax.named_scope("wo_wait"):
        wo_copy.wait()

    z_minus, z_plus = a * 4 + z_at(3), a * 4 + z_at(1)
    across_x = other * 4 + k
    top, bottom = slice(0, 32), slice(32, 64)

    def block(a_to, d, part):
        at = (a_to * 4 + z_at(d)) * OUTC + part * PART
        return dot(ctx_b[...], wo_v[:, pl.ds(pl.multiple_of(at, PART), PART)])

    def field(f, d):
        return block(other, d, 1) if f == 1 else block(a, d, 1 if f == 2 else 0)

    def x0_copy(d):
        return remote(xs0.at[d], xr0.at[d], x0_send.at[d], x0_recv.at[d], rep, across_x)

    x1_copy = remote(xs1, xr1, x1_sem.at[0], x1_sem.at[1], rep, across_x)

    def z_copy(f, kind, way):
        return remote(zs.at[f, kind, way], zr.at[f, kind, way], z_send.at[f, kind, way],
                      z_recv.at[f, kind, way], rep, z_minus if way == 0 else z_plus)

    def far(f, x):
        zs[f, 0, 0] = x[top].astype(bf16)
        zs[f, 0, 1] = x[bottom].astype(bf16)
        for way in range(2):
            z_copy(f, 0, way).start()

    def near(f, way, x):
        zs[f, 1, way] = (x[bottom] if way == 0 else x[top]).astype(bf16)
        kept[f, way] = x[top] if way == 0 else x[bottom]
        z_copy(f, 1, way).start()

    def relay(f, way):
        z_copy(f, 0, way).wait_recv()
        zs[f, 2, way] = (kept[f, way] + zr[f, 0, way].astype(f32)).astype(bf16)
        z_copy(f, 2, way).start()

    def arrived(f):
        for kind in (1, 2):
            for way in range(2):
                z_copy(f, kind, way).wait_recv()
        first = zr[f, 2, 0].astype(f32) + zr[f, 1, 1].astype(f32)
        last = zr[f, 2, 1].astype(f32) + zr[f, 1, 0].astype(f32)
        return jnp.concatenate([first, last], axis=0)

    def x_first(d):
        xs0[d] = block(other, d, 0).astype(bf16)
        x0_copy(d).start()

    def m_copy(src, dst, n, to):
        return remote(mid_p.at[src], mid_p.at[dst], m_send.at[n], m_recv.at[n], rep, to)

    m_x = m_copy(0, 1, 0, across_x)
    m_minus = m_copy(2, 3, 1, z_minus)
    m_plus = m_copy(2, 4, 2, z_plus)
    m_two = m_copy(2, 5, 3, a * 4 + z_at(2))

    with jax.named_scope("send0"):
        far(1, field(1, 2))
    with jax.named_scope("middle"):
        middle = dot(ctx_b[...], od_v[...])
        middle = jnp.where(left[0:32], middle[0:32], pltpu.roll(middle[32:64], 64, axis=1))
        mid_p[0] = middle.astype(bf16)
        m_x.start()
    with jax.named_scope("send1"):
        x_first(2)
        far(2, field(2, 2))
        x_first(3)
        near(1, 0, field(1, 3))
        near(1, 1, field(1, 1))
        x_first(1)
        near(2, 0, field(2, 3))
        near(2, 1, field(2, 1))
    with jax.named_scope("send2"):
        x_first(0)
        own0[0] = field(0, 2)
        own0[1] = field(0, 3)
        own0[2] = field(0, 1)
    with jax.named_scope("relay1"):
        for way in range(2):
            relay(1, way)
    with jax.named_scope("own"):
        mine[1] = field(1, 0)
        mine[0] = field(0, 0)
        mine[2] = field(2, 0)
    with jax.named_scope("mid_x"):
        m_x.wait_recv()
        mid_p[2] = (mid_p[0].astype(f32) + mid_p[1].astype(f32)).astype(bf16)
        m_two.start()
        m_minus.start()
        m_plus.start()
    with jax.named_scope("x_far"):
        x0_copy(2).wait_recv()
        far(0, own0[0] + xr0[2].astype(f32))
    with jax.named_scope("relay2"):
        for way in range(2):
            relay(2, way)
    with jax.named_scope("x_near0"):
        x0_copy(3).wait_recv()
        near(0, 0, own0[1] + xr0[3].astype(f32))
    with jax.named_scope("ou"):
        for n in range(TP):
            e = utl[(2 * n) // TP, (2 * n) % TP, 16:48, :].astype(f32)
            g = utl[(2 * n) // TP, (2 * n + 1) % TP, 16:48, :].astype(f32)
            e_r, g_r = pltpu.roll(e, 64, axis=1), pltpu.roll(g, 64, axis=1)
            ou_v[0:32, n * 128 : (n + 1) * 128] = jnp.where(left[0:32], e, g_r).astype(bf16)
            ou_v[32:64, n * 128 : (n + 1) * 128] = jnp.where(left[0:32], e_r, g).astype(bf16)
    with jax.named_scope("done1"):
        xs1[...] = (mine[1] + arrived(1)).astype(bf16)
        x1_copy.start()
    with jax.named_scope("x_near1"):
        x0_copy(1).wait_recv()
        near(0, 1, own0[2] + xr0[1].astype(f32))
    with jax.named_scope("relay0"):
        for way in range(2):
            relay(0, way)
    with jax.named_scope("done2"):
        mine[2] = mine[2] + arrived(2)
    with jax.named_scope("delta"):
        for copy in (m_minus, m_plus, m_two):
            copy.wait_recv()
        middle = mid_p[2].astype(f32)
        for n in range(3, 6):
            middle = middle + mid_p[n].astype(f32)
        middle = jnp.concatenate([middle, pltpu.roll(middle, 64, axis=1)], axis=0)[:, 0:64].astype(bf16)
        delta = adapter_scale * dot(middle, ou_v[...])
    with jax.named_scope("done0"):
        x0_copy(0).wait_recv()
        x = mine[0] + xr0[0].astype(f32) + delta[:, 0:PART]
        out[:, 0:PART] = (x + arrived(0)).astype(bf16)
    with jax.named_scope("x1_wait"):
        x1_copy.wait_recv()
    out[:, PART:] = (mine[2] + delta[:, PART:] + xr1[...].astype(f32)).astype(bf16)

    with jax.named_scope("drain"):
        for j in range(1, CHIPS):
            d_copy(j).wait_send()
            u_copy(j).wait_send()
        for j in range(CHIPS):
            across(j).wait_send()
        t_across.wait_send()
        l_across.wait_send()
        for j in range(1, TP):
            i_copy(j).wait_send()
            v_copy(j).wait_send()
            t_copy(j).wait_send()
            l_copy(j).wait_send()
        for copy in (m_x, m_minus, m_plus, m_two):
            copy.wait_send()
        for d in range(4):
            x0_copy(d).wait_send()
        x1_copy.wait_send()
        for f in range(3):
            for kind in range(3):
                for way in range(2):
                    z_copy(f, kind, way).wait_send()


def local(
    hidden, norm_gain, query_weight_matrix, key_value_weight, output_weight_matrix,
    input_down_factors, query_up_factor, key_value_up_factors, output_down_factor,
    output_up_factor, cache_keys, cache_values, lengths,
):
    hbm = pl.BlockSpec(memory_space=pltpu.HBM)
    dma = pltpu.SemaphoreType.DMA
    vmem = pltpu.VMEM
    return pl.pallas_call(
        kernel,
        out_shape=jax.ShapeDtypeStruct((SEQS, OUTC), bf16),
        in_specs=[hbm] * 13,
        out_specs=pl.BlockSpec(memory_space=pltpu.VMEM),
        scratch_shapes=[
            vmem((SEQS, FEATURES), bf16),
            vmem((SEQS, FEATURES), bf16),
            vmem((FEATURES, QCOLS), bf16),
            vmem((2, FEATURES, HEAD), bf16),
            vmem((QCOLS, FEATURES), bf16),
            vmem((SEQS, 1, 128, HEAD), bf16),
            vmem((SEQS, 1, 128, HEAD), bf16),
            vmem((3, 64, RANK), bf16),
            vmem((32, RANK), bf16),
            vmem((2, 8, RANK), bf16),
            vmem((32, RANK), bf16),
            vmem((RANK, 64), bf16),
            vmem((FEATURES,), bf16),
            vmem((SEQS,), jnp.int32),
            vmem((2, CHIPS, DROWS, 128), bf16),
            vmem((2, CHIPS, 128, 256), bf16),
            vmem((CHIPS, UROWS, 128), bf16),
            vmem((2, TP, 32, 128), bf16),
            vmem((2, TP, 48, 128), bf16),
            vmem((TP, SEQS, 128), bf16),
            vmem((TP, 32, 128), bf16),
            vmem((RANK, OUTC), bf16),
            vmem((QCOLS, 128), bf16),
            vmem((6, 32, 128), bf16),
            vmem((4, SEQS, PART), bf16),
            vmem((4, SEQS, PART), bf16),
            vmem((3, 3, 2, 32, PART), bf16),
            vmem((3, 3, 2, 32, PART), bf16),
            vmem((SEQS, PART), bf16),
            vmem((SEQS, PART), bf16),
            vmem((3, 2, 32, PART), f32),
            vmem((3, SEQS, PART), f32),
            vmem((3, SEQS, PART), f32),
            vmem((SEQS, QCOLS), f32),
            vmem((SEQS, HEAD), f32),
            vmem((SEQS, HEAD), f32),
            vmem((SEQS * 8, HEAD), f32),
            vmem((SEQS * 8, HEAD), f32),
            vmem((SEQS * 8, HEAD), f32),
            vmem((SEQS * 8, HEAD), f32),
            vmem((SEQS, QCOLS), bf16),
            dma((4,)), dma((CHUNKS,)), dma((CHUNKS,)), dma((7,)),
            dma((CHIPS,)), dma((CHIPS,)), dma((CHIPS,)), dma((CHIPS,)), dma((CHIPS,)), dma((CHIPS,)),
            dma((TP,)), dma((TP,)), dma((2,)), dma((TP,)), dma((TP,)), dma((2,)),
            dma((TP,)), dma((TP,)), dma((TP,)), dma((TP,)), dma((4,)), dma((4,)),
            dma((4,)), dma((4,)), dma((2,)), dma((3, 3, 2)), dma((3, 3, 2)),
        ],
        compiler_params=pltpu.CompilerParams(
            collective_id=0, has_side_effects=True, vmem_limit_bytes=48 * 1024 * 1024),
        cost_estimate=pl.CostEstimate(
            flops=3 * 10**9, bytes_accessed=26 * 2**20, transcendentals=0),
    )(*[pltpu.with_memory_space_constraint(x, pltpu.HBM) for x in (
        hidden, norm_gain, query_weight_matrix, key_value_weight,
        output_weight_matrix, input_down_factors, jnp.swapaxes(query_up_factor, 0, 1),
        jnp.swapaxes(key_value_up_factors, 1, 2), output_down_factor, output_up_factor,
        cache_keys, cache_values, lengths,
    )])


def solution(mesh):
    placed = (
        P("rep", None),
        P(),
        P(None, "tp"),
        P(None, None, "tp"),
        P("tp", None),
        P(None, ("rep", "tp"), None),
        P(None, ("rep", "tp")),
        P(None, None, ("rep", "tp")),
        P(("rep", "tp"), None),
        P(None, ("rep", "tp")),
        P("rep", "tp", None, None),
        P("rep", "tp", None, None),
        P("rep"),
    )
    return jax.shard_map(
        local, mesh=mesh, in_specs=placed, out_specs=P("rep", "tp"), check_vma=False
    )
```

```python
import math

import jax
import jax.numpy as jnp
from jax import lax
from jax.experimental import pallas as pl
from jax.experimental.pallas import tpu as pltpu
from jax.sharding import PartitionSpec as P

MESH = pl.DeviceIdType.MESH
bf16, f32 = jnp.bfloat16, jnp.float32

epsilon = 1e-06
rope_base = 1000000.0
adapter_scale = 0.5

FEATURES = 8192
SEQS = 64
RANK = 64
HEAD = 128
QCOLS = 512
OUTC = 1024
TP = 8
CHIPS = 8
CHUNKS = 8
CHUNK = FEATURES // CHUNKS
DROWS = 96
UROWS = 80
GROUP = 32
PART = 512
SLIM = 256


def dot(a, b):
    return jnp.dot(a, b, preferred_element_type=f32)


def dot_nt(a, b):
    return lax.dot_general(a, b, (((1,), (1,)), ((), ())), preferred_element_type=f32)


def at_lanes(offset, rows):
    row = lax.broadcasted_iota(jnp.int32, (rows, 128), 0)
    lane = lax.broadcasted_iota(jnp.int32, (rows, 128), 1)
    return jnp.where(lane == row + offset, 1.0, 0.0).astype(bf16)


def kernel(
    hidden, gain, wq, wkv, wo, down, qup, kvup, odown, oup, keys, values, lengths,
    out,
    hid_v, nrm_v, wq_v, wkv_v, wo_v, k_v, v_v,
    down_v, qup_v, kvup_v, odown_v, oup_v, gain_v, len_v,
    dg, w2, ug, ute, utl, uto, inner_p, inner_v, ou_v, od_v, mid_p,
    xs0, xr0, zs, zr, hs, hr, xs1, xr1, kept, kept_h, own0, mine, qacc, kacc, vacc, q_s, max_s, sum_s, ctx_s, len_s, ctx_b,
    load_sem, wq_sem, small_sem,
    d_recv, x0_recv, x1_recv, far_recv, near_recv, sems,
):
    names = ("d_send across_send across_recv u_send u_recv e_send e_recv w_send w_recv t_send t_recv "
             "tt_send tt_recv l_send l_recv ll_send ll_recv o_send o_recv oo_send oo_recv i_send i_recv "
             "v_send v_recv m_send m_x m_z x0_send x1_send slim_send wide_send").split()
    sem = {name: sems.at[n] for n, name in enumerate(names)}

    def wait(ref, name):
        pltpu.make_async_copy(ref, ref, sem[name]).wait()

    rep = lax.axis_index("rep")
    t = lax.axis_index("tp")
    chip = rep // 2
    core = rep % 2
    partner = chip * 2 + (1 - core)
    a, k = t // 4, t % 4
    other = 1 - a

    def chip_at(j):
        return lax.rem(chip + j, CHIPS)

    def tp_of(j):
        return t if j % 2 == 0 else lax.rem(t + 4, TP)

    def gather_peer(j):
        return chip_at(j) * 2 + core, tp_of(j)

    far_first = (4, 3, 5, 1, 7, 2, 6)

    def tp_at(j):
        return lax.rem(t + j, TP)

    def z_at(d):
        return lax.rem(k + d, 4)

    def remote(src, dst, send_sem, recv_sem, rep_to, tp_to):
        return pltpu.make_async_remote_copy(
            src_ref=src, dst_ref=dst, send_sem=send_sem, recv_sem=recv_sem,
            device_id=(rep_to, tp_to), device_id_type=MESH)

    barrier = pltpu.get_barrier_semaphore()
    small = [
        pltpu.make_async_copy(src, dst, small_sem.at[i])
        for i, (src, dst) in enumerate(
            ((down, down_v), (qup, qup_v), (kvup, kvup_v), (odown, odown_v), (oup, oup_v),
             (gain, gain_v), (lengths, len_v))
        )
    ]
    small[0].start()
    pl.semaphore_signal(barrier, inc=1, device_id=(partner, t), device_id_type=MESH)
    for j in range(1, CHIPS):
        pl.semaphore_signal(barrier, inc=1, device_id=gather_peer(j), device_id_type=MESH)
    for j in range(1, TP):
        pl.semaphore_signal(barrier, inc=1, device_id=(rep, tp_at(j)), device_id_type=MESH)
    for copy in small[1:]:
        copy.start()
    hid_copy = pltpu.make_async_copy(hidden, hid_v, load_sem.at[0])
    hid_copy.start()

    def wq_copy(i):
        rows = pl.ds(pl.multiple_of(i * CHUNK, CHUNK), CHUNK)
        return pltpu.make_async_copy(wq.at[rows, :], wq_v.at[rows, :], wq_sem.at[i])

    def wkv_copy(i):
        rows = pl.ds(pl.multiple_of(i * CHUNK, CHUNK), CHUNK)
        return pltpu.make_async_copy(wkv.at[:, rows, :], wkv_v.at[:, rows, :], wq_sem.at[i])

    def start_chunk(i, carry):
        wq_copy(i).start()
        wkv_copy(i).start()
        return carry

    lax.fori_loop(0, CHUNKS, start_chunk, 0)
    key_copy = pltpu.make_async_copy(keys, k_v, load_sem.at[1])
    value_copy = pltpu.make_async_copy(values, v_v, load_sem.at[2])
    wo_copy = pltpu.make_async_copy(wo, wo_v, load_sem.at[3])
    key_copy.start()
    value_copy.start()
    wo_copy.start()

    low, high = at_lanes(0, RANK), at_lanes(64, RANK)
    with jax.named_scope("pack"):
        small[0].wait()
        dg[core, chip, 0:64, :] = (dot(down_v[0], low) + dot(down_v[1], high)).astype(bf16)
        dg[core, chip, 64:96, :] = (dot(down_v[2, 0:32, :], low) + dot(down_v[2, 32:64, :], high)).astype(bf16)
        for copy in small[1:]:
            copy.wait()
        ug[chip, 0:16, :] = (dot(qup_v[0:16, :], low) + dot(qup_v[16:32, :], high)).astype(bf16)
        last = dot(kvup_v[1], low) + dot(kvup_v[0], high)
        ug[chip, 16:32, :] = jnp.concatenate([last, jnp.zeros_like(last)], axis=0).astype(bf16)
        ug[chip, 32:48, :] = (dot(odown_v[0:16, :], low) + dot(odown_v[16:32, :], high)).astype(bf16)
        ug[chip, 48:80, :] = (dot(oup_v[0:32, :], low) + dot(oup_v[32:64, :], high)).astype(bf16)

    with jax.named_scope("barrier_wait"):
        pl.semaphore_wait(barrier, CHIPS + TP - 1)

    def d_copy(j):
        return remote(dg.at[core, chip], dg.at[core, chip], sem["d_send"], d_recv.at[j],
                      *gather_peer(j))

    def u_copy(j):
        piece = ug.at[chip, 0:32]
        return remote(piece, piece, sem["u_send"], sem["u_recv"], *gather_peer(j))

    def e_copy(j):
        piece = ug.at[chip, 32:48]
        return remote(piece, piece, sem["e_send"], sem["e_recv"], *gather_peer(j))

    def w_copy(j):
        piece = ug.at[chip, 48:80]
        return remote(piece, piece, sem["w_send"], sem["w_recv"], *gather_peer(j))

    def across(j):
        q = lax.rem(chip + CHIPS - j, CHIPS)
        return remote(dg.at[core, q], dg.at[core, q], sem["across_send"], sem["across_recv"], partner, t)

    for j in far_first:
        u_copy(j).start()
    for j in far_first:
        d_copy(j).start()
    across(0).start()
    for j in far_first:
        e_copy(j).start()

    with jax.named_scope("hid_wait"):
        hid_copy.wait()

    def squares(i, total):
        cols = pl.ds(pl.multiple_of(i * CHUNK, CHUNK), CHUNK)
        x = hid_v[:, cols].astype(f32)
        x = x * x
        for n in range(CHUNK // 128):
            total = total + x[:, n * 128 : (n + 1) * 128]
        return total

    with jax.named_scope("norm"):
        total = lax.fori_loop(0, CHUNKS, squares, jnp.zeros((SEQS, 128), f32))
        square = jnp.sum(total, axis=-1, keepdims=True) * (1.0 / FEATURES)
        scale = lax.rsqrt(square + epsilon)

        def normalise(i, carry):
            cols = pl.ds(pl.multiple_of(i * CHUNK, CHUNK), CHUNK)
            x = hid_v[:, cols].astype(f32)
            nrm_v[:, cols] = (x * scale * gain_v[cols].astype(f32).reshape(1, CHUNK)).astype(bf16)
            return carry

        lax.fori_loop(0, CHUNKS, normalise, 0)

    w2[...] = jnp.zeros_like(w2)
    qacc[...] = jnp.zeros_like(qacc)
    kacc[...] = jnp.zeros_like(kacc)
    vacc[...] = jnp.zeros_like(vacc)

    def project(i, carry):
        chunk = wq_v.at[0 : CHUNK * 3 // 2]
        pltpu.make_async_copy(chunk, chunk, wq_sem.at[i]).wait()
        cols = pl.ds(pl.multiple_of(i * CHUNK, CHUNK), CHUNK)
        x = nrm_v[:, cols]
        qacc[...] += dot(x, wq_v[cols, :])
        kacc[...] += dot(x, wkv_v[0, cols, :])
        vacc[...] += dot(x, wkv_v[1, cols, :])
        return carry

    with jax.named_scope("project"):
        lax.fori_loop(0, CHUNKS, project, 0)

    lane = lax.broadcasted_iota(jnp.int32, (SEQS, 128), 1)
    left = lane < 64
    with jax.named_scope("angles"):
        lens = len_v[...].reshape(1, SEQS)
        square_rows = lax.broadcasted_iota(jnp.int32, (SEQS, SEQS), 0)
        square_lanes = lax.broadcasted_iota(jnp.int32, (SEQS, SEQS), 1)
        len_col = jnp.sum(
            jnp.where(square_rows == square_lanes, jnp.broadcast_to(lens, (SEQS, SEQS)), 0).astype(f32),
            axis=-1, keepdims=True)
        len_b = jnp.broadcast_to(len_col, (SEQS, 128))
        for h in range(8):
            len_s[pl.ds(h, SEQS, stride=8), :] = len_b
        index = (lane % 64).astype(f32)
        frequency = jnp.exp(index * (-2.0 / HEAD * math.log(rope_base)))
        angles = len_b * frequency
        cosine = jnp.cos(angles)
        sine = jnp.where(left, -jnp.sin(angles), jnp.sin(angles))

    def rotate(x):
        return x * cosine + pltpu.roll(x, 64, axis=1) * sine

    def slot_for(to):
        return lax.rem(t + 4 * lax.rem(to + chip, 2), TP)

    def t_copy(j):
        to = tp_at(j)
        return remote(ug.at[to, 0:32], ute.at[core, slot_for(to)], sem["t_send"], sem["t_recv"], rep, to)

    def l_copy(j):
        to = tp_at(j)
        return remote(ug.at[to, 32:48], utl.at[core, slot_for(to)], sem["l_send"], sem["l_recv"], rep, to)

    def o_copy(j):
        to = tp_at(j)
        return remote(ug.at[to, 48:80], uto.at[core, slot_for(to)], sem["o_send"], sem["o_recv"], rep, to)

    with jax.named_scope("u_wait"):
        wait(ug.at[0:7, 0:32], "u_recv")
        for j in range(1, TP):
            t_copy(j).start()
    with jax.named_scope("d_wait"):
        for j in range(1, CHIPS):
            d_copy(j).wait_recv()
            across(j).start()
    for j in far_first:
        w_copy(j).start()

    half = pl.multiple_of((t % 2) * 64, 64)

    def spread(c):
        for q in range(CHIPS):
            w2[c, q, pl.ds(half, 64), 0:128] = dg[c, q, 0:64, :]
            tail = dg[c, q, 64:96, :].astype(f32)
            both = jnp.concatenate([tail, pltpu.roll(tail, 64, axis=1)], axis=0)
            w2[c, q, pl.ds(half, 64), 128:256] = both.astype(bf16)

    def features(c):
        total = jnp.zeros((SEQS, 256), f32)
        for j in range(CHIPS):
            at = (chip_at(j) * 2 + c) * QCOLS + (tp_of(j) // 2) * 128
            total = total + dot(nrm_v[:, pl.ds(pl.multiple_of(at, 128), 128)], w2[c, chip_at(j)])
        return total

    with jax.named_scope("inner_own"):
        spread(core)
        partial = features(core)

    with jax.named_scope("across_wait"):
        wait(dg.at[1 - core], "across_recv")
    with jax.named_scope("inner_other"):
        spread(1 - core)
        partial = partial + features(1 - core)
        first, tail = partial[:, 0:128], partial[:, 128:256]
        packed = jnp.where(left[0:32], first[0:32], pltpu.roll(first[32:64], 64, axis=1))
        inner_p[t] = packed.astype(bf16)
        inner_v[t] = jnp.where(left, tail, first).astype(bf16)

    def i_copy(j):
        return remote(inner_p.at[t], inner_p.at[t], sem["i_send"], sem["i_recv"], rep, tp_at(j))

    def v_copy(j):
        return remote(inner_v.at[t], inner_v.at[t], sem["v_send"], sem["v_recv"], rep, tp_at(j))

    for j in range(1, TP):
        i_copy(j).start()
    for j in range(1, TP):
        v_copy(j).start()
    with jax.named_scope("w_wait"):
        wait(ug.at[0:7, 32:48], "e_recv")
    for j in range(1, TP):
        l_copy(j).start()
    ute[core, slot_for(t)] = ug[t, 0:32]
    utl[core, slot_for(t)] = ug[t, 32:48]

    with jax.named_scope("t_wait"):
        wait(ute.at[core, 0:7], "t_recv")
    t_across = remote(ute.at[core], ute.at[core], sem["tt_send"], sem["tt_recv"], partner, t)
    t_across.start()
    with jax.named_scope("up_wait"):
        wait(ute.at[1 - core], "tt_recv")
    with jax.named_scope("unpack"):
        rows = []
        for n in range(2 * TP):
            e = ute[n // TP, n % TP, 0:16, :].astype(f32)
            rows += [e, pltpu.roll(e, 64, axis=1)]
        up_rows = jnp.concatenate(rows, axis=0).astype(bf16)
        kv_rows = jnp.concatenate(
            [ute[n // TP, n % TP, 16:32, :].astype(f32)[0:8] for n in range(2 * TP)], axis=0).astype(bf16)

    with jax.named_scope("i_wait"):
        wait(inner_p.at[0:7], "i_recv")
    score_scale = 1.0 / math.sqrt(HEAD)
    with jax.named_scope("queries"):
        inner = inner_p[0].astype(f32)
        for n in range(1, TP):
            inner = inner + inner_p[n].astype(f32)
        inner = jnp.concatenate([inner, pltpu.roll(inner, 64, axis=1)], axis=0)
        inner_q = jnp.where(left, inner, 0.0).astype(bf16)
        query = qacc[...] + adapter_scale * dot_nt(inner_q, up_rows)
        for h in range(4):
            x = rotate(query[:, h * HEAD : (h + 1) * HEAD])
            main = x.astype(bf16).astype(f32)
            q_s[pl.ds(h, SEQS, stride=8), :] = main
            q_s[pl.ds(h + 4, SEQS, stride=8), :] = x - main
            qacc[:, h * HEAD : (h + 1) * HEAD] = x

    with jax.named_scope("cache_wait"):
        key_copy.wait()
        value_copy.wait()
    wide = 8 * GROUP
    position = lax.broadcasted_iota(jnp.int32, (wide, 128), 1).astype(f32)

    def attend(g, carry):
        rows = pl.ds(pl.multiple_of(g * wide, wide), wide)
        q_rows = q_s[rows, :].astype(bf16)
        scores = []
        for s in range(GROUP):
            sc = dot_nt(q_rows[s * 8 : (s + 1) * 8], k_v[g * GROUP + s, 0])
            scores.append(sc + pltpu.roll(sc, 4, axis=0))
        scores = jnp.concatenate(scores, axis=0) * score_scale
        live = position < len_s[rows, :]
        row_max = jnp.max(jnp.where(live, scores, -1e30), axis=-1, keepdims=True)
        weights = jnp.where(live, jnp.exp(scores - row_max), 0.0)
        denom = jnp.sum(weights, axis=-1, keepdims=True)
        probs = (weights / denom).astype(bf16)
        max_s[rows, :] = jnp.broadcast_to(row_max, (wide, 128))
        sum_s[rows, :] = jnp.broadcast_to(denom, (wide, 128))
        parts = [
            dot(probs[s * 8 : (s + 1) * 8], v_v[g * GROUP + s, 0]) for s in range(GROUP)
        ]
        ctx_s[rows, :] = jnp.concatenate(parts, axis=0)
        return carry

    with jax.named_scope("attend"):
        lax.fori_loop(0, SEQS // GROUP // 2, attend, 0)
    with jax.named_scope("late_wait"):
        wait(inner_v.at[0:7], "v_recv")
        wait(utl.at[core, 0:7], "l_recv")
    l_across = remote(utl.at[core], utl.at[core], sem["ll_send"], sem["ll_recv"], partner, t)
    l_across.start()
    with jax.named_scope("o_start"):
        wait(ug.at[0:7, 48:80], "w_recv")
        for j in range(1, TP):
            o_copy(j).start()
    with jax.named_scope("attend2"):
        lax.fori_loop(SEQS // GROUP // 2, SEQS // GROUP, attend, 0)

    with jax.named_scope("context"):
        wait(utl.at[1 - core], "ll_recv")
        for n in range(2 * TP):
            e = utl[n // TP, n % TP].astype(f32)
            e = jnp.concatenate([e, pltpu.roll(e, 64, axis=1)], axis=0)
            od_v[n * 32 : (n + 1) * 32, :] = e.astype(bf16)
        inner = inner_v[0].astype(f32)
        for n in range(1, TP):
            inner = inner + inner_v[n].astype(f32)
        inner_k = jnp.where(left, 0.0, inner).astype(bf16)
        new_key = rotate(kacc[...] + adapter_scale * dot_nt(inner_k, kv_rows)).astype(bf16).astype(f32)
        inner_k = jnp.where(left, inner, 0.0).astype(bf16)
        new_value = (vacc[...] + adapter_scale * dot_nt(inner_k, kv_rows)).astype(bf16).astype(f32)
        for h in range(4):
            at = pl.ds(h, SEQS, stride=8)
            own = jnp.sum(qacc[:, h * HEAD : (h + 1) * HEAD] * new_key, axis=-1, keepdims=True)
            own = jnp.broadcast_to(own * score_scale, (SEQS, 128))
            row_max = jnp.maximum(max_s[at, :], own)
            cached = sum_s[at, :] * jnp.exp(max_s[at, :] - row_max)
            own = jnp.exp(own - row_max)
            x = (ctx_s[at, :] * cached + own * new_value) / (cached + own)
            ctx_b[:, h * HEAD : (h + 1) * HEAD] = x.astype(bf16)

    with jax.named_scope("wo_wait"):
        wo_copy.wait()
    o_across = remote(uto.at[core], uto.at[core], sem["oo_send"], sem["oo_recv"], partner, t)

    z_minus, z_plus = a * 4 + z_at(3), a * 4 + z_at(1)
    across_x = other * 4 + k
    top, bottom = slice(0, 32), slice(32, 64)

    def block(a_to, d, part):
        at = (a_to * 4 + z_at(d)) * OUTC + part * PART
        return dot(ctx_b[...], wo_v[:, pl.ds(pl.multiple_of(at, PART), PART)])

    def x0_copy(n, d):
        return remote(xs0.at[n, d], xr0.at[n, d], sem["x0_send"], x0_recv.at[n, d], rep, across_x)

    def x1_copy(n):
        return remote(xs1.at[n], xr1.at[n], sem["x1_send"], x1_recv.at[n], rep, across_x)

    fields = [(hs.at[f], hr.at[f], kept_h.at[f]) for f in range(4)] + [(zs, zr, kept)]

    def z_copy(f, kind, way):
        sent, got, _ = fields[f]
        return remote(sent.at[kind, way], got.at[kind, way], sem["wide_send" if f == 4 else "slim_send"],
                      far_recv.at[f, way] if kind == 0 else near_recv.at[f],
                      rep, z_minus if way == 0 else z_plus)

    def far(f, x):
        for way in range(2):
            fields[f][0][0, way] = x[top if way == 0 else bottom].astype(bf16)
            z_copy(f, 0, way).start()

    def near(f, way, x):
        fields[f][0][1, way] = x[bottom if way == 0 else top].astype(bf16)
        fields[f][2][way] = x[top if way == 0 else bottom]
        z_copy(f, 1, way).start()

    def relay(f):
        sent, got, mid = fields[f]
        for way in range(2):
            z_copy(f, 0, way).wait_recv()
            sent[2, way] = (mid[way] + got[0, way].astype(f32)).astype(bf16)
            z_copy(f, 2, way).start()

    def arrived(f):
        got = fields[f][1]
        both = got.at[1:3]
        pltpu.make_async_copy(both, both, near_recv.at[f]).wait()
        first = got[2, 0].astype(f32) + got[1, 1].astype(f32)
        last = got[2, 1].astype(f32) + got[1, 0].astype(f32)
        return jnp.concatenate([first, last], axis=0)

    def x_first(d):
        x = block(other, d, 0).astype(bf16)
        for n in range(2):
            xs0[n, d] = x[:, n * SLIM : (n + 1) * SLIM]
            x0_copy(n, d).start()

    def x_sum(n, d):
        x0_copy(n, d).wait_recv()
        return own0[d, :, n * SLIM : (n + 1) * SLIM] + xr0[n, d].astype(f32)

    def m_copy(src, dst, n, to):
        return remote(mid_p.at[src], mid_p.at[dst], sem["m_send"], sem["m_x" if n == 0 else "m_z"], rep, to)

    m_x = m_copy(0, 1, 0, across_x)
    m_minus = m_copy(2, 3, 1, z_minus)
    m_plus = m_copy(2, 4, 2, z_plus)
    m_two = m_copy(2, 5, 3, a * 4 + z_at(2))

    with jax.named_scope("send0"):
        x_first(2)
        x = block(other, 2, 1)
        far(2, x[:, :SLIM])
        far(3, x[:, SLIM:])
    with jax.named_scope("middle"):
        middle = dot(ctx_b[...], od_v[...])
        middle = jnp.where(left[0:32], middle[0:32], pltpu.roll(middle[32:64], 64, axis=1))
        mid_p[0] = middle.astype(bf16)
        m_x.start()
    with jax.named_scope("send1"):
        x_first(3)
        for way, d in ((0, 3), (1, 1)):
            x = block(other, d, 1)
            near(2, way, x[:, :SLIM])
            near(3, way, x[:, SLIM:])
        x_first(1)
        far(4, block(a, 2, 1))
        near(4, 0, block(a, 3, 1))
        near(4, 1, block(a, 1, 1))
    with jax.named_scope("send2"):
        x_first(0)
        own0[2] = block(a, 2, 0)
        own0[3] = block(a, 3, 0)
    with jax.named_scope("own"):
        own0[1] = block(a, 1, 0)
        mine[1] = block(other, 0, 1)
    with jax.named_scope("relay2"):
        relay(2)
    with jax.named_scope("x_far0"):
        far(0, x_sum(0, 2))
    with jax.named_scope("relay3"):
        relay(3)
    with jax.named_scope("x_far"):
        far(1, x_sum(1, 2))
    with jax.named_scope("mid_x"):
        wait(mid_p.at[1], "m_x")
        mid_p[2] = (mid_p[0].astype(f32) + mid_p[1].astype(f32)).astype(bf16)
        m_two.start()
        m_minus.start()
        m_plus.start()
    with jax.named_scope("own2"):
        wait(uto.at[core, 0:7], "o_recv")
        uto[core, slot_for(t)] = ug[t, 48:80]
        o_across.start()
        mine[0] = block(a, 0, 0)
        mine[2] = block(a, 0, 1)
    with jax.named_scope("relay4"):
        relay(4)
    with jax.named_scope("ou"):
        wait(uto.at[1 - core], "oo_recv")
        for n in range(TP):
            e = uto[(2 * n) // TP, (2 * n) % TP].astype(f32)
            g = uto[(2 * n) // TP, (2 * n + 1) % TP].astype(f32)
            e_r, g_r = pltpu.roll(e, 64, axis=1), pltpu.roll(g, 64, axis=1)
            ou_v[0:32, n * 128 : (n + 1) * 128] = jnp.where(left[0:32], e, g_r).astype(bf16)
            ou_v[32:64, n * 128 : (n + 1) * 128] = jnp.where(left[0:32], e_r, g).astype(bf16)
    with jax.named_scope("x_near0"):
        for n in range(2):
            near(n, 0, x_sum(n, 3))
    with jax.named_scope("done2"):
        xs1[0] = (mine[1, :, :SLIM] + arrived(2)).astype(bf16)
        x1_copy(0).start()
    with jax.named_scope("done3"):
        xs1[1] = (mine[1, :, SLIM:] + arrived(3)).astype(bf16)
        x1_copy(1).start()
    with jax.named_scope("x_near1"):
        for n in range(2):
            near(n, 1, x_sum(n, 1))
    with jax.named_scope("relay0"):
        relay(0)
        relay(1)
    with jax.named_scope("delta"):
        wait(mid_p.at[3:6], "m_z")
        middle = mid_p[2].astype(f32)
        for n in range(3, 6):
            middle = middle + mid_p[n].astype(f32)
        middle = jnp.concatenate([middle, pltpu.roll(middle, 64, axis=1)], axis=0)[:, 0:64].astype(bf16)
        delta = adapter_scale * dot(middle, ou_v[...])
        mine[0] = mine[0] + delta[:, 0:PART]
        mine[2] = mine[2] + delta[:, PART:]
    with jax.named_scope("done4"):
        mine[2] = mine[2] + arrived(4)
    with jax.named_scope("x0_wait"):
        for n in range(2):
            cols = slice(n * SLIM, (n + 1) * SLIM)
            x0_copy(n, 0).wait_recv()
            mine[0, :, cols] = mine[0, :, cols] + xr0[n, 0].astype(f32)
    with jax.named_scope("x1_wait"):
        for n in range(2):
            x1_copy(n).wait_recv()
            cols = slice(n * SLIM, (n + 1) * SLIM)
            out[:, PART + n * SLIM : PART + (n + 1) * SLIM] = (mine[2, :, cols] + xr1[n].astype(f32)).astype(bf16)
    with jax.named_scope("done0"):
        for n in range(2):
            cols = slice(n * SLIM, (n + 1) * SLIM)
            out[:, cols] = (mine[0, :, cols] + arrived(n)).astype(bf16)

    with jax.named_scope("drain"):
        for ref, name in (
            (dg.at[core, 0:7], "d_send"), (dg.at[core], "across_send"), (ug.at[0:7, 0:32], "u_send"),
            (ug.at[0:7, 32:48], "e_send"), (ug.at[0:7, 48:80], "w_send"), (ug.at[0:7, 0:32], "t_send"),
            (ug.at[0:7, 32:48], "l_send"), (ug.at[0:7, 48:80], "o_send"), (ute.at[core], "tt_send"),
            (utl.at[core], "ll_send"), (uto.at[core], "oo_send"), (inner_p.at[0:7], "i_send"),
            (inner_v.at[0:7], "v_send"), (mid_p.at[0:4], "m_send"), (xs0, "x0_send"), (xs1, "x1_send"),
            (hs, "slim_send"), (zs, "wide_send"),
        ):
            wait(ref, name)


def local(
    hidden, norm_gain, query_weight_matrix, key_value_weight, output_weight_matrix,
    input_down_factors, query_up_factor, key_value_up_factors, output_down_factor,
    output_up_factor, cache_keys, cache_values, lengths,
):
    hbm = pl.BlockSpec(memory_space=pltpu.HBM)
    dma = pltpu.SemaphoreType.DMA
    vmem = pltpu.VMEM
    return pl.pallas_call(
        kernel,
        out_shape=jax.ShapeDtypeStruct((SEQS, OUTC), bf16),
        in_specs=[hbm] * 13,
        out_specs=pl.BlockSpec(memory_space=pltpu.VMEM),
        scratch_shapes=[
            vmem((SEQS, FEATURES), bf16),
            vmem((SEQS, FEATURES), bf16),
            vmem((FEATURES, QCOLS), bf16),
            vmem((2, FEATURES, HEAD), bf16),
            vmem((QCOLS, FEATURES), bf16),
            vmem((SEQS, 1, 128, HEAD), bf16),
            vmem((SEQS, 1, 128, HEAD), bf16),
            vmem((3, 64, RANK), bf16),
            vmem((32, RANK), bf16),
            vmem((2, 8, RANK), bf16),
            vmem((32, RANK), bf16),
            vmem((RANK, 64), bf16),
            vmem((FEATURES,), bf16),
            vmem((SEQS,), jnp.int32),
            vmem((2, CHIPS, DROWS, 128), bf16),
            vmem((2, CHIPS, 128, 256), bf16),
            vmem((CHIPS, UROWS, 128), bf16),
            vmem((2, TP, 32, 128), bf16),
            vmem((2, TP, 16, 128), bf16),
            vmem((2, TP, 32, 128), bf16),
            vmem((TP, 32, 128), bf16),
            vmem((TP, SEQS, 128), bf16),
            vmem((RANK, OUTC), bf16),
            vmem((QCOLS, 128), bf16),
            vmem((6, 32, 128), bf16),
            vmem((2, 4, SEQS, SLIM), bf16),
            vmem((2, 4, SEQS, SLIM), bf16),
            vmem((3, 2, 32, PART), bf16),
            vmem((3, 2, 32, PART), bf16),
            vmem((4, 3, 2, 32, SLIM), bf16),
            vmem((4, 3, 2, 32, SLIM), bf16),
            vmem((2, SEQS, SLIM), bf16),
            vmem((2, SEQS, SLIM), bf16),
            vmem((2, 32, PART), f32),
            vmem((4, 2, 32, SLIM), f32),
            vmem((4, SEQS, PART), f32),
            vmem((3, SEQS, PART), f32),
            vmem((SEQS, QCOLS), f32),
            vmem((SEQS, HEAD), f32),
            vmem((SEQS, HEAD), f32),
            vmem((SEQS * 8, HEAD), f32),
            vmem((SEQS * 8, HEAD), f32),
            vmem((SEQS * 8, HEAD), f32),
            vmem((SEQS * 8, HEAD), f32),
            vmem((SEQS * 8, HEAD), f32),
            vmem((SEQS, QCOLS), bf16),
            dma((4,)), dma((CHUNKS,)), dma((7,)),
            dma((CHIPS,)), dma((2, 4)), dma((2,)), dma((5, 2)), dma((5,)), dma((32,)),
        ],
        compiler_params=pltpu.CompilerParams(
            collective_id=0, has_side_effects=True, vmem_limit_bytes=48 * 1024 * 1024),
        cost_estimate=pl.CostEstimate(
            flops=3 * 10**9, bytes_accessed=26 * 2**20, transcendentals=0),
    )(*[pltpu.with_memory_space_constraint(x, pltpu.HBM) for x in (
        hidden, norm_gain, query_weight_matrix, key_value_weight,
        output_weight_matrix, input_down_factors, jnp.swapaxes(query_up_factor, 0, 1),
        jnp.swapaxes(key_value_up_factors, 1, 2), output_down_factor, output_up_factor,
        cache_keys, cache_values, lengths,
    )])


def solution(mesh):
    placed = (
        P("rep", None),
        P(),
        P(None, "tp"),
        P(None, None, "tp"),
        P("tp", None),
        P(None, ("rep", "tp"), None),
        P(None, ("rep", "tp")),
        P(None, None, ("rep", "tp")),
        P(("rep", "tp"), None),
        P(None, ("rep", "tp")),
        P("rep", "tp", None, None),
        P("rep", "tp", None, None),
        P("rep"),
    )
    return jax.shard_map(
        local, mesh=mesh, in_specs=placed, out_specs=P("rep", "tp"), check_vma=False
    )
```

```python
import math

import jax
import jax.numpy as jnp
from jax import lax
from jax.experimental import pallas as pl
from jax.experimental.pallas import tpu as pltpu
from jax.sharding import PartitionSpec as P

MESH = pl.DeviceIdType.MESH
bf16, f32 = jnp.bfloat16, jnp.float32

epsilon = 1e-06
rope_base = 1000000.0
adapter_scale = 0.5

FEATURES = 8192
SEQS = 64
RANK = 64
HEAD = 128
QCOLS = 512
OUTC = 1024
TP = 8
CHIPS = 8
CHUNKS = 8
CHUNK = FEATURES // CHUNKS
DROWS = 96
UROWS = 80
GROUP = 32
SENT_ROWS = (
    7 * DROWS + 8 * DROWS + 2 * 7 * UROWS + 8 * UROWS + 7 * 32 + 7 * 64 + 4 * 32
    + 1024 + 256 + 1536 + 768
)
SENT_BYTES = SENT_ROWS * 256
PART = 512
SLIM = 256


def dot(a, b):
    return jnp.dot(a, b, preferred_element_type=f32)


def dot_nt(a, b):
    return lax.dot_general(a, b, (((1,), (1,)), ((), ())), preferred_element_type=f32)


def at_lanes(offset, rows):
    row = lax.broadcasted_iota(jnp.int32, (rows, 128), 0)
    lane = lax.broadcasted_iota(jnp.int32, (rows, 128), 1)
    return jnp.where(lane == row + offset, 1.0, 0.0).astype(bf16)


def kernel(
    hidden, gain, wq, wkv, wo, down, qup, kvup, odown, oup, keys, values, lengths,
    out,
    hid_v, nrm_v, wq_v, wkv_v, wo_v, k_v, v_v,
    down_v, qup_v, kvup_v, odown_v, oup_v, gain_v, len_v,
    dg, d2, own_x, own_y, ug, ute, utl, uto, inner_p, inner_v, ou_v, od_v, mid_p,
    xs0, xr0, zs, zr, hs, hr, xs1, xr1, kept, kept_h, own0, mine, qacc, kacc, vacc, q_s, max_s, sum_s, ctx_s, len_s, ctx_b,
    load_sem, wq_sem, small_sem,
    d_recv, x0_recv, x1_recv, far_recv, near_recv, sems,
):
    names = ("send", "across", "d2", "across2", "u", "e", "w", "t", "tt", "l", "ll", "o", "oo", "i", "v", "m_x", "m_z")
    sem = {name: sems.at[n] for n, name in enumerate(names)}

    def wait(ref, name):
        pltpu.make_async_copy(ref, ref, sem[name]).wait()

    rep = lax.axis_index("rep")
    t = lax.axis_index("tp")
    chip = rep // 2
    core = rep % 2
    partner = chip * 2 + (1 - core)
    a, k = t // 4, t % 4
    other = 1 - a

    def chip_at(j):
        return lax.rem(chip + j, CHIPS)

    def tp_of(j):
        return t if j % 2 == 0 else lax.rem(t + 4, TP)

    def gather_peer(j):
        return chip_at(j) * 2 + core, tp_of(j)

    far_first = (4, 3, 5, 1, 7, 2, 6)

    farthest = ((1, 2), (0, 2), (1, 1), (1, 3), (0, 1), (0, 3), (1, 0))

    def tp_at(j):
        da, dk = farthest[j - 1]
        return lax.rem(a + da, 2) * 4 + lax.rem(k + dk, 4)

    def z_at(d):
        return lax.rem(k + d, 4)

    def remote(src, dst, send_sem, recv_sem, rep_to, tp_to):
        return pltpu.make_async_remote_copy(
            src_ref=src, dst_ref=dst, send_sem=send_sem, recv_sem=recv_sem,
            device_id=(rep_to, tp_to), device_id_type=MESH)

    barrier = pltpu.get_barrier_semaphore()
    small = [
        pltpu.make_async_copy(src, dst, small_sem.at[i])
        for i, (src, dst) in enumerate(
            ((down, down_v), (qup, qup_v), (kvup, kvup_v), (odown, odown_v), (oup, oup_v),
             (gain, gain_v), (lengths, len_v))
        )
    ]
    small[0].start()
    pl.semaphore_signal(barrier, inc=1, device_id=(partner, t), device_id_type=MESH)
    for j in range(1, CHIPS):
        pl.semaphore_signal(barrier, inc=1, device_id=gather_peer(j), device_id_type=MESH)
    for j in range(1, TP):
        pl.semaphore_signal(barrier, inc=1, device_id=(rep, tp_at(j)), device_id_type=MESH)
    for copy in small[1:]:
        copy.start()
    hid_copy = pltpu.make_async_copy(hidden, hid_v, load_sem.at[0])
    hid_copy.start()

    def wq_copy(i):
        rows = pl.ds(pl.multiple_of(i * CHUNK, CHUNK), CHUNK)
        return pltpu.make_async_copy(wq.at[rows, :], wq_v.at[rows, :], wq_sem.at[i])

    def wkv_copy(i):
        rows = pl.ds(pl.multiple_of(i * CHUNK, CHUNK), CHUNK)
        return pltpu.make_async_copy(wkv.at[:, rows, :], wkv_v.at[:, rows, :], wq_sem.at[i])

    def start_chunk(i, carry):
        wq_copy(i).start()
        wkv_copy(i).start()
        return carry

    lax.fori_loop(0, CHUNKS, start_chunk, 0)
    key_copy = pltpu.make_async_copy(keys, k_v, load_sem.at[1])
    value_copy = pltpu.make_async_copy(values, v_v, load_sem.at[2])
    wo_copy = pltpu.make_async_copy(wo, wo_v, load_sem.at[3])
    key_copy.start()
    value_copy.start()
    wo_copy.start()

    low, high = at_lanes(0, RANK), at_lanes(64, RANK)
    with jax.named_scope("pack"):
        small[0].wait()
        dg[core, chip] = (dot(down_v[0], low) + dot(down_v[1], high)).astype(bf16)
        d2[core, chip] = (dot(down_v[2, 0:32, :], low) + dot(down_v[2, 32:64, :], high)).astype(bf16)
        for copy in small[1:]:
            copy.wait()
        ug[chip, 0:16, :] = (dot(qup_v[0:16, :], low) + dot(qup_v[16:32, :], high)).astype(bf16)
        last = dot(kvup_v[1], low) + dot(kvup_v[0], high)
        ug[chip, 16:32, :] = jnp.concatenate([last, jnp.zeros_like(last)], axis=0).astype(bf16)
        ug[chip, 32:48, :] = (dot(odown_v[0:16, :], low) + dot(odown_v[16:32, :], high)).astype(bf16)
        ug[chip, 48:80, :] = (dot(oup_v[0:32, :], low) + dot(oup_v[32:64, :], high)).astype(bf16)

    with jax.named_scope("hid_wait"):
        hid_copy.wait()

    def squares(i, total):
        cols = pl.ds(pl.multiple_of(i * CHUNK, CHUNK), CHUNK)
        x = hid_v[:, cols].astype(f32)
        x = x * x
        for n in range(CHUNK // 128):
            total = total + x[:, n * 128 : (n + 1) * 128]
        return total

    with jax.named_scope("norm"):
        total = lax.fori_loop(0, CHUNKS, squares, jnp.zeros((SEQS, 128), f32))
        square = jnp.sum(total, axis=-1, keepdims=True) * (1.0 / FEATURES)
        scale = lax.rsqrt(square + epsilon)

        def normalise(i, carry):
            cols = pl.ds(pl.multiple_of(i * CHUNK, CHUNK), CHUNK)
            x = hid_v[:, cols].astype(f32)
            nrm_v[:, cols] = (x * scale * gain_v[cols].astype(f32).reshape(1, CHUNK)).astype(bf16)
            return carry

        lax.fori_loop(0, CHUNKS, normalise, 0)

    with jax.named_scope("barrier_wait"):
        pl.semaphore_wait(barrier, CHIPS + TP - 1)

    def d_copy(j):
        return remote(dg.at[core, chip], dg.at[core, chip], sem["send"], d_recv.at[j],
                      *gather_peer(j))

    def u_copy(j):
        piece = ug.at[chip, 0:32]
        return remote(piece, piece, sem["send"], sem["u"], *gather_peer(j))

    def e_copy(j):
        piece = ug.at[chip, 32:48]
        return remote(piece, piece, sem["send"], sem["e"], *gather_peer(j))

    def w_copy(j):
        piece = ug.at[chip, 48:80]
        return remote(piece, piece, sem["send"], sem["w"], *gather_peer(j))

    def across(j):
        q = lax.rem(chip + CHIPS - j, CHIPS)
        return remote(dg.at[core, q], dg.at[core, q], sem["send"], sem["across"], partner, t)

    def d2_copy(j):
        return remote(d2.at[core, chip], d2.at[core, chip], sem["send"], sem["d2"], *gather_peer(j))

    for j in far_first:
        u_copy(j).start()
    for j in far_first:
        d_copy(j).start()
    across(0).start()
    for j in far_first:
        d2_copy(j).start()
    for j in far_first:
        e_copy(j).start()

    qacc[...] = jnp.zeros_like(qacc)
    kacc[...] = jnp.zeros_like(kacc)
    vacc[...] = jnp.zeros_like(vacc)

    def project(i, carry):
        chunk = wq_v.at[0 : CHUNK * 3 // 2]
        pltpu.make_async_copy(chunk, chunk, wq_sem.at[i]).wait()
        cols = pl.ds(pl.multiple_of(i * CHUNK, CHUNK), CHUNK)
        x = nrm_v[:, cols]
        qacc[...] += dot(x, wq_v[cols, :])
        kacc[...] += dot(x, wkv_v[0, cols, :])
        vacc[...] += dot(x, wkv_v[1, cols, :])
        return carry

    with jax.named_scope("project"):
        lax.fori_loop(0, CHUNKS, project, 0)

    lane = lax.broadcasted_iota(jnp.int32, (SEQS, 128), 1)
    left = lane < 64
    with jax.named_scope("angles"):
        lens = len_v[...].reshape(1, SEQS)
        square_rows = lax.broadcasted_iota(jnp.int32, (SEQS, SEQS), 0)
        square_lanes = lax.broadcasted_iota(jnp.int32, (SEQS, SEQS), 1)
        len_col = jnp.sum(
            jnp.where(square_rows == square_lanes, jnp.broadcast_to(lens, (SEQS, SEQS)), 0).astype(f32),
            axis=-1, keepdims=True)
        len_b = jnp.broadcast_to(len_col, (SEQS, 128))
        for h in range(8):
            len_s[pl.ds(h, SEQS, stride=8), :] = len_b
        index = (lane % 64).astype(f32)
        frequency = jnp.exp(index * (-2.0 / HEAD * math.log(rope_base)))
        angles = len_b * frequency
        cosine = jnp.cos(angles)
        sine = jnp.where(left, -jnp.sin(angles), jnp.sin(angles))

    with jax.named_scope("own_features"):
        for c in range(2):
            parts = []
            for q in range(CHIPS):
                owner = lax.rem(t + 4 * lax.rem(chip + q, 2), TP)
                at = pl.multiple_of((2 * q + c) * QCOLS + (owner // 2) * 128, 128)
                x = nrm_v[:, pl.ds(at, 128)].astype(f32)
                parts.append(jnp.where(left, jnp.where(t % 2 == 0, x, pltpu.roll(x, 64, axis=1)), 0.0))
            for n in range(CHIPS // 2):
                x = parts[2 * n] + pltpu.roll(parts[2 * n + 1], 64, axis=1)
                own_x[c, :, n * 128 : (n + 1) * 128] = x.astype(bf16)
            for n in range(CHIPS // 4):
                first, last = 0.0, 0.0
                for m in range(4):
                    x = parts[4 * n + m]
                    x1, x2 = jnp.where(lane < 32, x, 0.0), jnp.where(lane < 32, 0.0, x)
                    first = first + (pltpu.roll(x1, 32 * m, axis=1) if m else x1)
                    last = last + (pltpu.roll(x2, (32 * m + 96) % 128, axis=1) if m != 1 else x2)
                own_y[c, 0:64, n * 128 : (n + 1) * 128] = first.astype(bf16)
                own_y[c, 64:128, n * 128 : (n + 1) * 128] = last.astype(bf16)

    def rotate(x):
        return x * cosine + pltpu.roll(x, 64, axis=1) * sine

    def slot_for(to):
        return lax.rem(t + 4 * lax.rem(to + chip, 2), TP)

    def t_copy(j):
        to = tp_at(j)
        return remote(ug.at[to, 0:32], ute.at[core, slot_for(to)], sem["send"], sem["t"], rep, to)

    def l_copy(j):
        to = tp_at(j)
        return remote(ug.at[to, 32:48], utl.at[core, slot_for(to)], sem["send"], sem["l"], rep, to)

    def o_copy(j):
        to = tp_at(j)
        return remote(ug.at[to, 48:80], uto.at[core, slot_for(to)], sem["send"], sem["o"], rep, to)

    with jax.named_scope("u_wait"):
        wait(ug.at[0:7, 0:32], "u")
        for j in range(1, TP):
            t_copy(j).start()
    with jax.named_scope("d_wait"):
        for j in range(1, CHIPS):
            d_copy(j).wait_recv()
            across(j).start()
    for j in far_first:
        w_copy(j).start()

    def features(c):
        return dot(own_x[c], dg[c].reshape(CHIPS * 64, 128))

    def value_features(c):
        return dot(own_y[c], d2[c].reshape(CHIPS * 32, 128))

    def pass_values():
        wait(d2.at[core, 0:7], "d2")
        remote(d2.at[core], d2.at[core], sem["send"], sem["across2"], partner, t).start()

    @pl.when(core == 1)
    def _():
        pass_values()

    with jax.named_scope("inner_own"):
        partial = features(core)

    with jax.named_scope("across_wait"):
        wait(dg.at[1 - core], "across")
    with jax.named_scope("inner_other"):
        partial = partial + features(1 - core)
        packed = jnp.where(left[0:32], partial[0:32], pltpu.roll(partial[32:64], 64, axis=1))
        inner_p[t] = packed.astype(bf16)

    def i_copy(j):
        return remote(inner_p.at[t], inner_p.at[t], sem["send"], sem["i"], rep, tp_at(j))

    def v_copy(j):
        return remote(inner_v.at[t], inner_v.at[t], sem["send"], sem["v"], rep, tp_at(j))

    for j in range(1, TP):
        i_copy(j).start()
    with jax.named_scope("d2_wait"):

        @pl.when(core == 0)
        def _():
            pass_values()

    with jax.named_scope("w_wait"):
        wait(ug.at[0:7, 32:48], "e")
        for j in range(1, TP):
            l_copy(j).start()
        wait(d2.at[1 - core], "across2")
        x = value_features(core) + value_features(1 - core)
        inner_v[t] = jnp.where(left, x[0:64] + pltpu.roll(x[64:128], 64, axis=1), partial).astype(bf16)
    for j in range(1, TP):
        v_copy(j).start()
    ute[core, slot_for(t)] = ug[t, 0:32]
    utl[core, slot_for(t)] = ug[t, 32:48]

    with jax.named_scope("t_wait"):
        wait(ute.at[core, 0:7], "t")
    t_across = remote(ute.at[core], ute.at[core], sem["send"], sem["tt"], partner, t)
    t_across.start()
    with jax.named_scope("up_wait"):
        wait(ute.at[1 - core], "tt")
    with jax.named_scope("unpack"):
        rows = []
        for n in range(2 * TP):
            e = ute[n // TP, n % TP, 0:16, :].astype(f32)
            rows += [e, pltpu.roll(e, 64, axis=1)]
        up_rows = jnp.concatenate(rows, axis=0).astype(bf16)
        kv_rows = jnp.concatenate(
            [ute[n // TP, n % TP, 16:32, :].astype(f32)[0:8] for n in range(2 * TP)], axis=0).astype(bf16)

    with jax.named_scope("i_wait"):
        wait(inner_p.at[0:7], "i")
    score_scale = 1.0 / math.sqrt(HEAD)
    with jax.named_scope("queries"):
        inner = inner_p[0].astype(f32)
        for n in range(1, TP):
            inner = inner + inner_p[n].astype(f32)
        inner = jnp.concatenate([inner, pltpu.roll(inner, 64, axis=1)], axis=0)
        inner_q = jnp.where(left, inner, 0.0).astype(bf16)
        query = qacc[...] + adapter_scale * dot_nt(inner_q, up_rows)
        for h in range(4):
            x = rotate(query[:, h * HEAD : (h + 1) * HEAD])
            main = x.astype(bf16).astype(f32)
            q_s[pl.ds(h, SEQS, stride=8), :] = main
            q_s[pl.ds(h + 4, SEQS, stride=8), :] = x - main
            qacc[:, h * HEAD : (h + 1) * HEAD] = x

    with jax.named_scope("cache_wait"):
        key_copy.wait()
        value_copy.wait()
    wide = 8 * GROUP
    position = lax.broadcasted_iota(jnp.int32, (wide, 128), 1).astype(f32)

    def attend(g):
        rows = pl.ds(g * wide, wide)
        q_rows = q_s[rows, :].astype(bf16)
        scores = []
        for s in range(GROUP):
            sc = dot_nt(q_rows[s * 8 : (s + 1) * 8], k_v[g * GROUP + s, 0])
            scores.append(sc + pltpu.roll(sc, 4, axis=0))
        scores = jnp.concatenate(scores, axis=0) * score_scale
        live = position < len_s[rows, :]
        row_max = jnp.max(jnp.where(live, scores, -1e30), axis=-1, keepdims=True)
        weights = jnp.where(live, jnp.exp(scores - row_max), 0.0)
        denom = jnp.sum(weights, axis=-1, keepdims=True)
        probs = (weights / denom).astype(bf16)
        max_s[rows, :] = jnp.broadcast_to(row_max, (wide, 128))
        sum_s[rows, :] = jnp.broadcast_to(denom, (wide, 128))
        parts = [
            dot(probs[s * 8 : (s + 1) * 8], v_v[g * GROUP + s, 0]) for s in range(GROUP)
        ]
        ctx_s[rows, :] = jnp.concatenate(parts, axis=0)

    with jax.named_scope("attend"):
        attend(0)
    with jax.named_scope("late_wait"):
        wait(utl.at[core, 0:7], "l")
    l_across = remote(utl.at[core], utl.at[core], sem["send"], sem["ll"], partner, t)
    l_across.start()
    with jax.named_scope("o_start"):
        wait(ug.at[0:7, 48:80], "w")
        for j in range(1, TP):
            o_copy(j).start()
    with jax.named_scope("attend2"):
        attend(1)

    with jax.named_scope("v_wait"):
        wait(inner_v.at[0:7], "v")
    with jax.named_scope("context"):
        inner = inner_v[0].astype(f32)
        for n in range(1, TP):
            inner = inner + inner_v[n].astype(f32)
        inner_k = jnp.where(left, 0.0, inner).astype(bf16)
        new_key = rotate(kacc[...] + adapter_scale * dot_nt(inner_k, kv_rows)).astype(bf16).astype(f32)
        inner_k = jnp.where(left, inner, 0.0).astype(bf16)
        new_value = (vacc[...] + adapter_scale * dot_nt(inner_k, kv_rows)).astype(bf16).astype(f32)
        for h in range(4):
            at = pl.ds(h, SEQS, stride=8)
            own = jnp.sum(qacc[:, h * HEAD : (h + 1) * HEAD] * new_key, axis=-1, keepdims=True)
            own = jnp.broadcast_to(own * score_scale, (SEQS, 128))
            row_max = jnp.maximum(max_s[at, :], own)
            cached = sum_s[at, :] * jnp.exp(max_s[at, :] - row_max)
            own = jnp.exp(own - row_max)
            x = (ctx_s[at, :] * cached + own * new_value) / (cached + own)
            ctx_b[:, h * HEAD : (h + 1) * HEAD] = x.astype(bf16)

    with jax.named_scope("wo_wait"):
        wo_copy.wait()
    o_across = remote(uto.at[core], uto.at[core], sem["send"], sem["oo"], partner, t)

    z_minus, z_plus = a * 4 + z_at(3), a * 4 + z_at(1)
    across_x = other * 4 + k
    top, bottom = slice(0, 32), slice(32, 64)

    def block(a_to, d):
        at = (a_to * 4 + z_at(d)) * OUTC
        return dot(ctx_b[...], wo_v[:, pl.ds(pl.multiple_of(at, OUTC), OUTC)])

    def x0_copy(n, d):
        return remote(xs0.at[n, d], xr0.at[n, d], sem["send"], x0_recv.at[n, d], rep, across_x)

    def x1_copy(n):
        return remote(xs1.at[n], xr1.at[n], sem["send"], x1_recv.at[n], rep, across_x)

    fields = [(hs.at[f], hr.at[f], kept_h.at[f]) for f in range(4)] + [(zs, zr, kept)]

    def z_copy(f, kind, way):
        sent, got, _ = fields[f]
        return remote(sent.at[kind, way], got.at[kind, way], sem["send"],
                      far_recv.at[f, way] if kind == 0 else near_recv.at[f],
                      rep, z_minus if way == 0 else z_plus)

    def far(f, x):
        for way in range(2):
            fields[f][0][0, way] = x[top if way == 0 else bottom].astype(bf16)
            z_copy(f, 0, way).start()

    def near(f, way, x):
        fields[f][0][1, way] = x[bottom if way == 0 else top].astype(bf16)
        fields[f][2][way] = x[top if way == 0 else bottom]
        z_copy(f, 1, way).start()

    def relay(f):
        sent, got, mid = fields[f]
        for way in range(2):
            z_copy(f, 0, way).wait_recv()
            sent[2, way] = (mid[way] + got[0, way].astype(f32)).astype(bf16)
            z_copy(f, 2, way).start()

    def arrived(f):
        got = fields[f][1]
        both = got.at[1:3]
        pltpu.make_async_copy(both, both, near_recv.at[f]).wait()
        first = got[2, 0].astype(f32) + got[1, 1].astype(f32)
        last = got[2, 1].astype(f32) + got[1, 0].astype(f32)
        return jnp.concatenate([first, last], axis=0)

    def x_first(d, x):
        for n in range(2):
            xs0[n, d] = x[:, n * SLIM : (n + 1) * SLIM].astype(bf16)
            x0_copy(n, d).start()

    def other_far(x):
        x_first(2, x)
        far(2, x[:, PART : PART + SLIM])
        far(3, x[:, PART + SLIM :])

    def other_near(d, way, x):
        x_first(d, x)
        near(2, way, x[:, PART : PART + SLIM])
        near(3, way, x[:, PART + SLIM :])

    def x_sum(n, d):
        x0_copy(n, d).wait_recv()
        return own0[d, :, n * SLIM : (n + 1) * SLIM] + xr0[n, d].astype(f32)

    def m_copy(src, dst, n, to):
        return remote(mid_p.at[src], mid_p.at[dst], sem["send"], sem["m_x" if n == 0 else "m_z"], rep, to)

    m_x = m_copy(0, 1, 0, across_x)
    m_minus = m_copy(2, 3, 1, z_minus)
    m_plus = m_copy(2, 4, 2, z_plus)
    m_two = m_copy(2, 5, 3, a * 4 + z_at(2))

    with jax.named_scope("send0"):
        other_far(block(other, 2))
    with jax.named_scope("middle"):
        wait(utl.at[1 - core], "ll")
        for n in range(2 * TP):
            e = utl[n // TP, n % TP].astype(f32)
            e = jnp.concatenate([e, pltpu.roll(e, 64, axis=1)], axis=0)
            od_v[n * 32 : (n + 1) * 32, :] = e.astype(bf16)
        middle = dot(ctx_b[...], od_v[...])
        middle = jnp.where(left[0:32], middle[0:32], pltpu.roll(middle[32:64], 64, axis=1))
        mid_p[0] = middle.astype(bf16)
        m_x.start()
    with jax.named_scope("send1"):
        other_near(3, 0, block(other, 3))
        other_near(1, 1, block(other, 1))
        x = block(a, 2)
        far(4, x[:, PART:])
        own0[2] = x[:, :PART]
        for way, d in ((0, 3), (1, 1)):
            x = block(a, d)
            near(4, way, x[:, PART:])
            own0[d] = x[:, :PART]
    with jax.named_scope("send2"):
        x = block(other, 0)
        x_first(0, x)
        mine[1] = x[:, PART:]
    with jax.named_scope("relay2"):
        relay(2)
    with jax.named_scope("x_far0"):
        far(0, x_sum(0, 2))
    with jax.named_scope("relay3"):
        relay(3)
    with jax.named_scope("x_far"):
        far(1, x_sum(1, 2))
    with jax.named_scope("mid_x"):
        wait(mid_p.at[1], "m_x")
        mid_p[2] = (mid_p[0].astype(f32) + mid_p[1].astype(f32)).astype(bf16)
        m_two.start()
        m_minus.start()
        m_plus.start()
    with jax.named_scope("own2"):
        wait(uto.at[core, 0:7], "o")
        uto[core, slot_for(t)] = ug[t, 48:80]
        o_across.start()
        x = block(a, 0)
        mine[0] = x[:, :PART]
        mine[2] = x[:, PART:]
    with jax.named_scope("relay4"):
        relay(4)
    with jax.named_scope("ou"):
        wait(uto.at[1 - core], "oo")
        for n in range(TP):
            e = uto[(2 * n) // TP, (2 * n) % TP].astype(f32)
            g = uto[(2 * n) // TP, (2 * n + 1) % TP].astype(f32)
            e_r, g_r = pltpu.roll(e, 64, axis=1), pltpu.roll(g, 64, axis=1)
            ou_v[0:32, n * 128 : (n + 1) * 128] = jnp.where(left[0:32], e, g_r).astype(bf16)
            ou_v[32:64, n * 128 : (n + 1) * 128] = jnp.where(left[0:32], e_r, g).astype(bf16)
    with jax.named_scope("x_near0"):
        for n in range(2):
            near(n, 0, x_sum(n, 3))
    with jax.named_scope("done2"):
        xs1[0] = (mine[1, :, :SLIM] + arrived(2)).astype(bf16)
        x1_copy(0).start()
    with jax.named_scope("done3"):
        xs1[1] = (mine[1, :, SLIM:] + arrived(3)).astype(bf16)
        x1_copy(1).start()
    with jax.named_scope("x_near1"):
        for n in range(2):
            near(n, 1, x_sum(n, 1))
    with jax.named_scope("relay0"):
        relay(0)
        relay(1)
    with jax.named_scope("delta"):
        wait(mid_p.at[3:6], "m_z")
        middle = mid_p[2].astype(f32)
        for n in range(3, 6):
            middle = middle + mid_p[n].astype(f32)
        middle = jnp.concatenate([middle, pltpu.roll(middle, 64, axis=1)], axis=0)[:, 0:64].astype(bf16)
        delta = adapter_scale * dot(middle, ou_v[...])
        mine[0] = mine[0] + delta[:, 0:PART]
        mine[2] = mine[2] + delta[:, PART:]
    with jax.named_scope("done4"):
        mine[2] = mine[2] + arrived(4)
    with jax.named_scope("x0_wait"):
        for n in range(2):
            cols = slice(n * SLIM, (n + 1) * SLIM)
            x0_copy(n, 0).wait_recv()
            mine[0, :, cols] = mine[0, :, cols] + xr0[n, 0].astype(f32)
    with jax.named_scope("x1_wait"):
        for n in range(2):
            x1_copy(n).wait_recv()
            cols = slice(n * SLIM, (n + 1) * SLIM)
            out[:, PART + n * SLIM : PART + (n + 1) * SLIM] = (mine[2, :, cols] + xr1[n].astype(f32)).astype(bf16)
    with jax.named_scope("done0"):
        for n in range(2):
            cols = slice(n * SLIM, (n + 1) * SLIM)
            out[:, cols] = (mine[0, :, cols] + arrived(n)).astype(bf16)

    with jax.named_scope("drain"):
        wait(wq_v.at[0 : SENT_BYTES // 1024], "send")


def local(
    hidden, norm_gain, query_weight_matrix, key_value_weight, output_weight_matrix,
    input_down_factors, query_up_factor, key_value_up_factors, output_down_factor,
    output_up_factor, cache_keys, cache_values, lengths,
):
    hbm = pl.BlockSpec(memory_space=pltpu.HBM)
    dma = pltpu.SemaphoreType.DMA
    vmem = pltpu.VMEM
    return pl.pallas_call(
        kernel,
        out_shape=jax.ShapeDtypeStruct((SEQS, OUTC), bf16),
        in_specs=[hbm] * 13,
        out_specs=pl.BlockSpec(memory_space=pltpu.VMEM),
        scratch_shapes=[
            vmem((SEQS, FEATURES), bf16),
            vmem((SEQS, FEATURES), bf16),
            vmem((FEATURES, QCOLS), bf16),
            vmem((2, FEATURES, HEAD), bf16),
            vmem((QCOLS, FEATURES), bf16),
            vmem((SEQS, 1, 128, HEAD), bf16),
            vmem((SEQS, 1, 128, HEAD), bf16),
            vmem((3, 64, RANK), bf16),
            vmem((32, RANK), bf16),
            vmem((2, 8, RANK), bf16),
            vmem((32, RANK), bf16),
            vmem((RANK, 64), bf16),
            vmem((FEATURES,), bf16),
            vmem((SEQS,), jnp.int32),
            vmem((2, CHIPS, 64, 128), bf16),
            vmem((2, CHIPS, 32, 128), bf16),
            vmem((2, SEQS, CHIPS * 64), bf16),
            vmem((2, 2 * SEQS, CHIPS * 32), bf16),
            vmem((CHIPS, UROWS, 128), bf16),
            vmem((2, TP, 32, 128), bf16),
            vmem((2, TP, 16, 128), bf16),
            vmem((2, TP, 32, 128), bf16),
            vmem((TP, 32, 128), bf16),
            vmem((TP, SEQS, 128), bf16),
            vmem((RANK, OUTC), bf16),
            vmem((QCOLS, 128), bf16),
            vmem((6, 32, 128), bf16),
            vmem((2, 4, SEQS, SLIM), bf16),
            vmem((2, 4, SEQS, SLIM), bf16),
            vmem((3, 2, 32, PART), bf16),
            vmem((3, 2, 32, PART), bf16),
            vmem((4, 3, 2, 32, SLIM), bf16),
            vmem((4, 3, 2, 32, SLIM), bf16),
            vmem((2, SEQS, SLIM), bf16),
            vmem((2, SEQS, SLIM), bf16),
            vmem((2, 32, PART), f32),
            vmem((4, 2, 32, SLIM), f32),
            vmem((4, SEQS, PART), f32),
            vmem((3, SEQS, PART), f32),
            vmem((SEQS, QCOLS), f32),
            vmem((SEQS, HEAD), f32),
            vmem((SEQS, HEAD), f32),
            vmem((SEQS * 8, HEAD), f32),
            vmem((SEQS * 8, HEAD), f32),
            vmem((SEQS * 8, HEAD), f32),
            vmem((SEQS * 8, HEAD), f32),
            vmem((SEQS * 8, HEAD), f32),
            vmem((SEQS, QCOLS), bf16),
            dma((4,)), dma((CHUNKS,)), dma((7,)),
            dma((CHIPS,)), dma((2, 4)), dma((2,)), dma((5, 2)), dma((5,)), dma((17,)),
        ],
        compiler_params=pltpu.CompilerParams(
            collective_id=0, has_side_effects=True, vmem_limit_bytes=48 * 1024 * 1024),
        cost_estimate=pl.CostEstimate(
            flops=3 * 10**9, bytes_accessed=26 * 2**20, transcendentals=0),
    )(*[pltpu.with_memory_space_constraint(x, pltpu.HBM) for x in (
        hidden, norm_gain, query_weight_matrix, key_value_weight,
        output_weight_matrix, input_down_factors, jnp.swapaxes(query_up_factor, 0, 1),
        jnp.swapaxes(key_value_up_factors, 1, 2), output_down_factor, output_up_factor,
        cache_keys, cache_values, lengths,
    )])


def solution(mesh):
    placed = (
        P("rep", None),
        P(),
        P(None, "tp"),
        P(None, None, "tp"),
        P("tp", None),
        P(None, ("rep", "tp"), None),
        P(None, ("rep", "tp")),
        P(None, None, ("rep", "tp")),
        P(("rep", "tp"), None),
        P(None, ("rep", "tp")),
        P("rep", "tp", None, None),
        P("rep", "tp", None, None),
        P("rep"),
    )
    return jax.shard_map(
        local, mesh=mesh, in_specs=placed, out_specs=P("rep", "tp"), check_vma=False
    )
```

```python
import math

import jax
import jax.numpy as jnp
from jax import lax
from jax.experimental import pallas as pl
from jax.experimental.pallas import tpu as pltpu
from jax.sharding import PartitionSpec as P

MESH = pl.DeviceIdType.MESH
bf16, f32 = jnp.bfloat16, jnp.float32

epsilon = 1e-06
rope_base = 1000000.0
adapter_scale = 0.5

FEATURES = 8192
SEQS = 64
RANK = 64
HEAD = 128
QCOLS = 512
OUTC = 1024
TP = 8
CHIPS = 8
CHUNKS = 8
CHUNK = FEATURES // CHUNKS
DROWS = 96
UROWS = 80
WIDTHS = (256, 256, 256, 256, 512)
STARTS = (0, 256, 512, 768, 512)
PART = 512
GROUP = 32
SENT_ROWS = (
    7 * DROWS + 8 * DROWS + 2 * 7 * UROWS + 8 * UROWS + 7 * 32 + 7 * 64 + 4 * 32
    + (4 * SEQS * PART + SEQS * (OUTC - PART) + 6 * 32 * sum(WIDTHS)) // 128
)
SENT_BYTES = SENT_ROWS * 256


def dot(a, b):
    return jnp.dot(a, b, preferred_element_type=f32)


def dot_nt(a, b):
    return lax.dot_general(a, b, (((1,), (1,)), ((), ())), preferred_element_type=f32)


def at_lanes(offset, rows):
    row = lax.broadcasted_iota(jnp.int32, (rows, 128), 0)
    lane = lax.broadcasted_iota(jnp.int32, (rows, 128), 1)
    return jnp.where(lane == row + offset, 1.0, 0.0).astype(bf16)


def kernel(
    hidden, gain, wq, wkv, wo, down, qup, kvup, odown, oup, keys, values, lengths,
    out,
    hid_v, nrm_v, wq_v, wkv_v, wo_v, k_v, v_v,
    down_v, qup_v, kvup_v, odown_v, oup_v, gain_v, len_v,
    dg, d2, own_x, own_y, ug, ute, utl, uto, inner_p, inner_v, ou_v, od_v, mid_p,
    xs0, xr0, zs, zr, xs1, xr1, kept, own0, mine_a, mine_b, qacc, kacc, vacc, q_s, max_s, sum_s, ctx_s, len_s, ctx_b,
    load_sem, wq_sem, small_sem,
    d_recv, x0_recv, x1_recv, far_recv, near_recv, sems,
):
    names = ("send", "across", "d2", "across2", "u", "e", "w", "t", "tt", "l", "ll", "o", "oo", "i", "v", "m_x", "m_z")
    sem = {name: sems.at[n] for n, name in enumerate(names)}

    def wait(ref, name):
        pltpu.make_async_copy(ref, ref, sem[name]).wait()

    rep = lax.axis_index("rep")
    t = lax.axis_index("tp")
    chip = rep // 2
    core = rep % 2
    partner = chip * 2 + (1 - core)
    a, k = t // 4, t % 4
    other = 1 - a

    def chip_at(j):
        return lax.rem(chip + j, CHIPS)

    def tp_of(j):
        return t if j % 2 == 0 else lax.rem(t + 4, TP)

    def gather_peer(j):
        return chip_at(j) * 2 + core, tp_of(j)

    far_first = (4, 3, 5, 1, 7, 2, 6)

    farthest = ((1, 2), (0, 2), (1, 1), (1, 3), (0, 1), (0, 3), (1, 0))

    def tp_at(j):
        da, dk = farthest[j - 1]
        return lax.rem(a + da, 2) * 4 + lax.rem(k + dk, 4)

    def z_at(d):
        return lax.rem(k + d, 4)

    def remote(src, dst, send_sem, recv_sem, rep_to, tp_to):
        return pltpu.make_async_remote_copy(
            src_ref=src, dst_ref=dst, send_sem=send_sem, recv_sem=recv_sem,
            device_id=(rep_to, tp_to), device_id_type=MESH)

    barrier = pltpu.get_barrier_semaphore()
    small = [
        pltpu.make_async_copy(src, dst, small_sem.at[i])
        for i, (src, dst) in enumerate(
            ((down, down_v), (qup, qup_v), (kvup, kvup_v), (odown, odown_v), (oup, oup_v),
             (gain, gain_v), (lengths, len_v))
        )
    ]
    small[0].start()
    pl.semaphore_signal(barrier, inc=1, device_id=(partner, t), device_id_type=MESH)
    for j in range(1, CHIPS):
        pl.semaphore_signal(barrier, inc=1, device_id=gather_peer(j), device_id_type=MESH)
    for j in range(1, TP):
        pl.semaphore_signal(barrier, inc=1, device_id=(rep, tp_at(j)), device_id_type=MESH)
    for copy in small[1:]:
        copy.start()
    hid_copy = pltpu.make_async_copy(hidden, hid_v, load_sem.at[0])
    hid_copy.start()

    def wq_copy(i):
        rows = pl.ds(pl.multiple_of(i * CHUNK, CHUNK), CHUNK)
        return pltpu.make_async_copy(wq.at[rows, :], wq_v.at[rows, :], wq_sem.at[i])

    def wkv_copy(i):
        rows = pl.ds(pl.multiple_of(i * CHUNK, CHUNK), CHUNK)
        return pltpu.make_async_copy(wkv.at[:, rows, :], wkv_v.at[:, rows, :], wq_sem.at[i])

    def start_chunk(i, carry):
        wq_copy(i).start()
        wkv_copy(i).start()
        return carry

    lax.fori_loop(0, CHUNKS, start_chunk, 0)
    key_copy = pltpu.make_async_copy(keys, k_v, load_sem.at[1])
    value_copy = pltpu.make_async_copy(values, v_v, load_sem.at[2])
    wo_copy = pltpu.make_async_copy(wo, wo_v, load_sem.at[3])
    key_copy.start()
    value_copy.start()
    wo_copy.start()

    low, high = at_lanes(0, RANK), at_lanes(64, RANK)
    with jax.named_scope("pack"):
        small[0].wait()
        dg[core, chip] = (dot(down_v[0], low) + dot(down_v[1], high)).astype(bf16)
        d2[core, chip] = (dot(down_v[2, 0:32, :], low) + dot(down_v[2, 32:64, :], high)).astype(bf16)
        for copy in small[1:]:
            copy.wait()
        ug[chip, 0:16, :] = (dot(qup_v[0:16, :], low) + dot(qup_v[16:32, :], high)).astype(bf16)
        last = dot(kvup_v[1], low) + dot(kvup_v[0], high)
        ug[chip, 16:32, :] = jnp.concatenate([last, jnp.zeros_like(last)], axis=0).astype(bf16)
        ug[chip, 32:48, :] = (dot(odown_v[0:16, :], low) + dot(odown_v[16:32, :], high)).astype(bf16)
        ug[chip, 48:80, :] = (dot(oup_v[0:32, :], low) + dot(oup_v[32:64, :], high)).astype(bf16)

    with jax.named_scope("hid_wait"):
        hid_copy.wait()

    def squares(i, total):
        cols = pl.ds(pl.multiple_of(i * CHUNK, CHUNK), CHUNK)
        x = hid_v[:, cols].astype(f32)
        x = x * x
        for n in range(CHUNK // 128):
            total = total + x[:, n * 128 : (n + 1) * 128]
        return total

    with jax.named_scope("norm"):
        total = lax.fori_loop(0, CHUNKS, squares, jnp.zeros((SEQS, 128), f32))
        square = jnp.sum(total, axis=-1, keepdims=True) * (1.0 / FEATURES)
        scale = lax.rsqrt(square + epsilon)

        def normalise(i, carry):
            cols = pl.ds(pl.multiple_of(i * CHUNK, CHUNK), CHUNK)
            x = hid_v[:, cols].astype(f32)
            nrm_v[:, cols] = (x * scale * gain_v[cols].astype(f32).reshape(1, CHUNK)).astype(bf16)
            return carry

        lax.fori_loop(0, CHUNKS, normalise, 0)

    with jax.named_scope("barrier_wait"):
        pl.semaphore_wait(barrier, CHIPS + TP - 1)

    def d_copy(j):
        return remote(dg.at[core, chip], dg.at[core, chip], sem["send"], d_recv.at[j],
                      *gather_peer(j))

    def u_copy(j):
        piece = ug.at[chip, 0:32]
        return remote(piece, piece, sem["send"], sem["u"], *gather_peer(j))

    def e_copy(j):
        piece = ug.at[chip, 32:48]
        return remote(piece, piece, sem["send"], sem["e"], *gather_peer(j))

    def w_copy(j):
        piece = ug.at[chip, 48:80]
        return remote(piece, piece, sem["send"], sem["w"], *gather_peer(j))

    def across(j):
        q = lax.rem(chip + CHIPS - j, CHIPS)
        return remote(dg.at[core, q], dg.at[core, q], sem["send"], sem["across"], partner, t)

    def d2_copy(j):
        return remote(d2.at[core, chip], d2.at[core, chip], sem["send"], sem["d2"], *gather_peer(j))

    for j in far_first:
        u_copy(j).start()
    for j in far_first:
        d_copy(j).start()
    across(0).start()
    for j in far_first:
        d2_copy(j).start()
    for j in far_first:
        e_copy(j).start()

    qacc[...] = jnp.zeros_like(qacc)
    kacc[...] = jnp.zeros_like(kacc)
    vacc[...] = jnp.zeros_like(vacc)

    def project(i, carry):
        chunk = wq_v.at[0 : CHUNK * 3 // 2]
        pltpu.make_async_copy(chunk, chunk, wq_sem.at[i]).wait()
        cols = pl.ds(pl.multiple_of(i * CHUNK, CHUNK), CHUNK)
        x = nrm_v[:, cols]
        qacc[...] += dot(x, wq_v[cols, :])
        kacc[...] += dot(x, wkv_v[0, cols, :])
        vacc[...] += dot(x, wkv_v[1, cols, :])
        return carry

    with jax.named_scope("project"):
        lax.fori_loop(0, CHUNKS, project, 0)

    lane = lax.broadcasted_iota(jnp.int32, (SEQS, 128), 1)
    left = lane < 64
    with jax.named_scope("angles"):
        lens = len_v[...].reshape(1, SEQS)
        square_rows = lax.broadcasted_iota(jnp.int32, (SEQS, SEQS), 0)
        square_lanes = lax.broadcasted_iota(jnp.int32, (SEQS, SEQS), 1)
        len_col = jnp.sum(
            jnp.where(square_rows == square_lanes, jnp.broadcast_to(lens, (SEQS, SEQS)), 0).astype(f32),
            axis=-1, keepdims=True)
        len_b = jnp.broadcast_to(len_col, (SEQS, 128))
        for h in range(8):
            len_s[pl.ds(h, SEQS, stride=8), :] = len_b
        index = (lane % 64).astype(f32)
        frequency = jnp.exp(index * (-2.0 / HEAD * math.log(rope_base)))
        angles = len_b * frequency
        cosine = jnp.cos(angles)
        sine = jnp.where(left, -jnp.sin(angles), jnp.sin(angles))

    with jax.named_scope("own_features"):
        for c in range(2):
            parts = []
            for q in range(CHIPS):
                owner = lax.rem(t + 4 * lax.rem(chip + q, 2), TP)
                at = pl.multiple_of((2 * q + c) * QCOLS + (owner // 2) * 128, 128)
                x = nrm_v[:, pl.ds(at, 128)].astype(f32)
                parts.append(jnp.where(left, jnp.where(t % 2 == 0, x, pltpu.roll(x, 64, axis=1)), 0.0))
            for n in range(CHIPS // 2):
                x = parts[2 * n] + pltpu.roll(parts[2 * n + 1], 64, axis=1)
                own_x[c, :, n * 128 : (n + 1) * 128] = x.astype(bf16)
            for n in range(CHIPS // 4):
                first, last = 0.0, 0.0
                for m in range(4):
                    x = parts[4 * n + m]
                    x1, x2 = jnp.where(lane < 32, x, 0.0), jnp.where(lane < 32, 0.0, x)
                    first = first + (pltpu.roll(x1, 32 * m, axis=1) if m else x1)
                    last = last + (pltpu.roll(x2, (32 * m + 96) % 128, axis=1) if m != 1 else x2)
                own_y[c, 0:64, n * 128 : (n + 1) * 128] = first.astype(bf16)
                own_y[c, 64:128, n * 128 : (n + 1) * 128] = last.astype(bf16)

    def rotate(x):
        return x * cosine + pltpu.roll(x, 64, axis=1) * sine

    def slot_for(to):
        return lax.rem(t + 4 * lax.rem(to + chip, 2), TP)

    def t_copy(j):
        to = tp_at(j)
        return remote(ug.at[to, 0:32], ute.at[core, slot_for(to)], sem["send"], sem["t"], rep, to)

    def l_copy(j):
        to = tp_at(j)
        return remote(ug.at[to, 32:48], utl.at[core, slot_for(to)], sem["send"], sem["l"], rep, to)

    def o_copy(j):
        to = tp_at(j)
        return remote(ug.at[to, 48:80], uto.at[core, slot_for(to)], sem["send"], sem["o"], rep, to)

    with jax.named_scope("u_wait"):
        wait(ug.at[0:7, 0:32], "u")
        for j in range(1, TP):
            t_copy(j).start()
    with jax.named_scope("d_wait"):
        for j in range(1, CHIPS):
            d_copy(j).wait_recv()
            across(j).start()
    for j in far_first:
        w_copy(j).start()

    def features(c):
        return dot(own_x[c], dg[c].reshape(CHIPS * 64, 128))

    def value_features(c):
        return dot(own_y[c], d2[c].reshape(CHIPS * 32, 128))

    def pass_values():
        wait(d2.at[core, 0:7], "d2")
        remote(d2.at[core], d2.at[core], sem["send"], sem["across2"], partner, t).start()

    @pl.when(core == 1)
    def _():
        pass_values()

    with jax.named_scope("inner_own"):
        partial = features(core)

    with jax.named_scope("across_wait"):
        wait(dg.at[1 - core], "across")
    with jax.named_scope("inner_other"):
        partial = partial + features(1 - core)
        packed = jnp.where(left[0:32], partial[0:32], pltpu.roll(partial[32:64], 64, axis=1))
        inner_p[t] = packed.astype(bf16)

    def i_copy(j):
        return remote(inner_p.at[t], inner_p.at[t], sem["send"], sem["i"], rep, tp_at(j))

    def v_copy(j):
        return remote(inner_v.at[t], inner_v.at[t], sem["send"], sem["v"], rep, tp_at(j))

    for j in range(1, TP):
        i_copy(j).start()
    with jax.named_scope("d2_wait"):

        @pl.when(core == 0)
        def _():
            pass_values()

    with jax.named_scope("w_wait"):
        wait(ug.at[0:7, 32:48], "e")
        for j in range(1, TP):
            l_copy(j).start()
        wait(d2.at[1 - core], "across2")
        x = value_features(core) + value_features(1 - core)
        inner_v[t] = jnp.where(left, x[0:64] + pltpu.roll(x[64:128], 64, axis=1), partial).astype(bf16)
    for j in range(1, TP):
        v_copy(j).start()
    ute[core, slot_for(t)] = ug[t, 0:32]
    utl[core, slot_for(t)] = ug[t, 32:48]

    with jax.named_scope("t_wait"):
        wait(ute.at[core, 0:7], "t")
    t_across = remote(ute.at[core], ute.at[core], sem["send"], sem["tt"], partner, t)
    t_across.start()
    with jax.named_scope("up_wait"):
        wait(ute.at[1 - core], "tt")
    with jax.named_scope("unpack"):
        rows = []
        for n in range(2 * TP):
            e = ute[n // TP, n % TP, 0:16, :].astype(f32)
            rows += [e, pltpu.roll(e, 64, axis=1)]
        up_rows = jnp.concatenate(rows, axis=0).astype(bf16)
        kv_rows = jnp.concatenate(
            [ute[n // TP, n % TP, 16:32, :].astype(f32)[0:8] for n in range(2 * TP)], axis=0).astype(bf16)

    with jax.named_scope("i_wait"):
        wait(inner_p.at[0:7], "i")
    score_scale = 1.0 / math.sqrt(HEAD)
    with jax.named_scope("queries"):
        inner = inner_p[0].astype(f32)
        for n in range(1, TP):
            inner = inner + inner_p[n].astype(f32)
        inner = jnp.concatenate([inner, pltpu.roll(inner, 64, axis=1)], axis=0)
        inner_q = jnp.where(left, inner, 0.0).astype(bf16)
        query = qacc[...] + adapter_scale * dot_nt(inner_q, up_rows)
        for h in range(4):
            x = rotate(query[:, h * HEAD : (h + 1) * HEAD])
            main = x.astype(bf16).astype(f32)
            q_s[pl.ds(h, SEQS, stride=8), :] = main
            q_s[pl.ds(h + 4, SEQS, stride=8), :] = x - main
            qacc[:, h * HEAD : (h + 1) * HEAD] = x

    with jax.named_scope("cache_wait"):
        key_copy.wait()
        value_copy.wait()
    wide = 8 * GROUP
    position = lax.broadcasted_iota(jnp.int32, (wide, 128), 1).astype(f32)

    def attend(g):
        rows = pl.ds(g * wide, wide)
        q_rows = q_s[rows, :].astype(bf16)
        scores = []
        for s in range(GROUP):
            sc = dot_nt(q_rows[s * 8 : (s + 1) * 8], k_v[g * GROUP + s, 0])
            scores.append(sc + pltpu.roll(sc, 4, axis=0))
        scores = jnp.concatenate(scores, axis=0) * score_scale
        live = position < len_s[rows, :]
        row_max = jnp.max(jnp.where(live, scores, -1e30), axis=-1, keepdims=True)
        weights = jnp.where(live, jnp.exp(scores - row_max), 0.0)
        denom = jnp.sum(weights, axis=-1, keepdims=True)
        probs = (weights / denom).astype(bf16)
        max_s[rows, :] = jnp.broadcast_to(row_max, (wide, 128))
        sum_s[rows, :] = jnp.broadcast_to(denom, (wide, 128))
        parts = [
            dot(probs[s * 8 : (s + 1) * 8], v_v[g * GROUP + s, 0]) for s in range(GROUP)
        ]
        ctx_s[rows, :] = jnp.concatenate(parts, axis=0)

    with jax.named_scope("attend"):
        attend(0)
    with jax.named_scope("late_wait"):
        wait(utl.at[core, 0:7], "l")
    l_across = remote(utl.at[core], utl.at[core], sem["send"], sem["ll"], partner, t)
    l_across.start()
    with jax.named_scope("o_start"):
        wait(ug.at[0:7, 48:80], "w")
        for j in range(1, TP):
            o_copy(j).start()
    with jax.named_scope("attend2"):
        attend(1)

    with jax.named_scope("v_wait"):
        wait(inner_v.at[0:7], "v")
    with jax.named_scope("context"):
        inner = inner_v[0].astype(f32)
        for n in range(1, TP):
            inner = inner + inner_v[n].astype(f32)
        inner_k = jnp.where(left, 0.0, inner).astype(bf16)
        new_key = rotate(kacc[...] + adapter_scale * dot_nt(inner_k, kv_rows)).astype(bf16).astype(f32)
        inner_k = jnp.where(left, inner, 0.0).astype(bf16)
        new_value = (vacc[...] + adapter_scale * dot_nt(inner_k, kv_rows)).astype(bf16).astype(f32)
        for h in range(4):
            at = pl.ds(h, SEQS, stride=8)
            own = jnp.sum(qacc[:, h * HEAD : (h + 1) * HEAD] * new_key, axis=-1, keepdims=True)
            own = jnp.broadcast_to(own * score_scale, (SEQS, 128))
            row_max = jnp.maximum(max_s[at, :], own)
            cached = sum_s[at, :] * jnp.exp(max_s[at, :] - row_max)
            own = jnp.exp(own - row_max)
            x = (ctx_s[at, :] * cached + own * new_value) / (cached + own)
            ctx_b[:, h * HEAD : (h + 1) * HEAD] = x.astype(bf16)

    with jax.named_scope("wo_wait"):
        wo_copy.wait()
    o_across = remote(uto.at[core], uto.at[core], sem["send"], sem["oo"], partner, t)

    z_minus, z_plus = a * 4 + z_at(3), a * 4 + z_at(1)
    across_x = other * 4 + k
    top, bottom = slice(0, 32), slice(32, 64)

    def block(a_to, d):
        at = (a_to * 4 + z_at(d)) * OUTC
        return dot(ctx_b[...], wo_v[:, pl.ds(pl.multiple_of(at, OUTC), OUTC)])

    def x0_copy(n, d):
        return remote(xs0[n].at[d], xr0[n].at[d], sem["send"], x0_recv.at[n, d], rep, across_x)

    def x1_copy(n):
        return remote(xs1[n], xr1[n], sem["send"], x1_recv.at[n], rep, across_x)

    def columns(f):
        return slice(STARTS[f], STARTS[f] + WIDTHS[f])

    def z_copy(f, kind, way):
        return remote(zs[f].at[kind, way], zr[f].at[kind, way], sem["send"],
                      far_recv.at[f, way] if kind == 0 else near_recv.at[f],
                      rep, z_minus if way == 0 else z_plus)

    def far(f, x):
        for way in range(2):
            zs[f][0, way] = x[top if way == 0 else bottom].astype(bf16)
            z_copy(f, 0, way).start()

    def near(f, way, x):
        zs[f][1, way] = x[bottom if way == 0 else top].astype(bf16)
        kept[f][way] = x[top if way == 0 else bottom]
        z_copy(f, 1, way).start()

    def relay(f):
        for way in range(2):
            z_copy(f, 0, way).wait_recv()
            zs[f][2, way] = (kept[f][way] + zr[f][0, way].astype(f32)).astype(bf16)
            z_copy(f, 2, way).start()

    def arrived(f):
        got = zr[f]
        both = got.at[1:3]
        pltpu.make_async_copy(both, both, near_recv.at[f]).wait()
        first = got[2, 0].astype(f32) + got[1, 1].astype(f32)
        last = got[2, 1].astype(f32) + got[1, 0].astype(f32)
        return jnp.concatenate([first, last], axis=0)

    def x_first(d, x):
        for n in range(2):
            xs0[n][d] = x[:, columns(n)].astype(bf16)
            x0_copy(n, d).start()

    def other_far(x):
        x_first(2, x)
        far(2, x[:, columns(2)])
        far(3, x[:, columns(3)])

    def other_near(d, way, x):
        x_first(d, x)
        near(2, way, x[:, columns(2)])
        near(3, way, x[:, columns(3)])

    def x_sum(n, d):
        x0_copy(n, d).wait_recv()
        return own0[d, :, columns(n)] + xr0[n][d].astype(f32)

    def m_copy(src, dst, n, to):
        return remote(mid_p.at[src], mid_p.at[dst], sem["send"], sem["m_x" if n == 0 else "m_z"], rep, to)

    m_x = m_copy(0, 1, 0, across_x)
    m_minus = m_copy(2, 3, 1, z_minus)
    m_plus = m_copy(2, 4, 2, z_plus)
    m_two = m_copy(2, 5, 3, a * 4 + z_at(2))

    with jax.named_scope("send0"):
        other_far(block(other, 2))
    with jax.named_scope("middle"):
        wait(utl.at[1 - core], "ll")
        for n in range(2 * TP):
            e = utl[n // TP, n % TP].astype(f32)
            e = jnp.concatenate([e, pltpu.roll(e, 64, axis=1)], axis=0)
            od_v[n * 32 : (n + 1) * 32, :] = e.astype(bf16)
        middle = dot(ctx_b[...], od_v[...])
        middle = jnp.where(left[0:32], middle[0:32], pltpu.roll(middle[32:64], 64, axis=1))
        mid_p[0] = middle.astype(bf16)
        m_x.start()
    with jax.named_scope("send1"):
        other_near(3, 0, block(other, 3))
        other_near(1, 1, block(other, 1))
        x = block(a, 2)
        far(4, x[:, PART:])
        own0[2] = x[:, :PART]
        for way, d in ((0, 3), (1, 1)):
            x = block(a, d)
            near(4, way, x[:, PART:])
            own0[d] = x[:, :PART]
    with jax.named_scope("send2"):
        x = block(other, 0)
        x_first(0, x)
        mine_b[0] = x[:, PART:]
    with jax.named_scope("x_far0"):
        far(0, x_sum(0, 2))
    with jax.named_scope("relay2"):
        relay(2)
    with jax.named_scope("x_far"):
        far(1, x_sum(1, 2))
    with jax.named_scope("relay3"):
        relay(3)
    with jax.named_scope("mid_x"):
        wait(mid_p.at[1], "m_x")
        mid_p[2] = (mid_p[0].astype(f32) + mid_p[1].astype(f32)).astype(bf16)
        m_two.start()
        m_minus.start()
        m_plus.start()
    with jax.named_scope("own2"):
        wait(uto.at[core, 0:7], "o")
        uto[core, slot_for(t)] = ug[t, 48:80]
        o_across.start()
        x = block(a, 0)
        mine_a[...] = x[:, :PART]
        mine_b[1] = x[:, PART:]
    with jax.named_scope("relay4"):
        relay(4)
    with jax.named_scope("ou"):
        wait(uto.at[1 - core], "oo")
        for n in range(TP):
            e = uto[(2 * n) // TP, (2 * n) % TP].astype(f32)
            g = uto[(2 * n) // TP, (2 * n + 1) % TP].astype(f32)
            e_r, g_r = pltpu.roll(e, 64, axis=1), pltpu.roll(g, 64, axis=1)
            ou_v[0:32, n * 128 : (n + 1) * 128] = jnp.where(left[0:32], e, g_r).astype(bf16)
            ou_v[32:64, n * 128 : (n + 1) * 128] = jnp.where(left[0:32], e_r, g).astype(bf16)
    with jax.named_scope("x_near0"):
        for n in range(2):
            near(n, 0, x_sum(n, 3))
    with jax.named_scope("done2"):
        xs1[0][...] = (mine_b[0, :, : WIDTHS[2]] + arrived(2)).astype(bf16)
        x1_copy(0).start()
    with jax.named_scope("x_near1"):
        for n in range(2):
            near(n, 1, x_sum(n, 1))
    with jax.named_scope("relay00"):
        relay(0)
    with jax.named_scope("done3"):
        xs1[1][...] = (mine_b[0, :, WIDTHS[2] :] + arrived(3)).astype(bf16)
        x1_copy(1).start()
    with jax.named_scope("relay0"):
        relay(1)
    with jax.named_scope("delta"):
        wait(mid_p.at[3:6], "m_z")
        middle = mid_p[2].astype(f32)
        for n in range(3, 6):
            middle = middle + mid_p[n].astype(f32)
        middle = jnp.concatenate([middle, pltpu.roll(middle, 64, axis=1)], axis=0)[:, 0:64].astype(bf16)
        delta = adapter_scale * dot(middle, ou_v[...])
        mine_a[...] = mine_a[...] + delta[:, 0:PART]
        mine_b[1] = mine_b[1] + delta[:, PART:]
    with jax.named_scope("done4"):
        mine_b[1] = mine_b[1] + arrived(4)
    with jax.named_scope("x0_wait"):
        for n in range(2):
            x0_copy(n, 0).wait_recv()
            mine_a[:, columns(n)] = mine_a[:, columns(n)] + xr0[n][0].astype(f32)
    with jax.named_scope("x1_wait"):
        for n in range(2):
            x1_copy(n).wait_recv()
            cols = columns(2 + n)
            own = mine_b[1, :, cols.start - PART : cols.stop - PART]
            out[:, cols] = (own + xr1[n][...].astype(f32)).astype(bf16)
    with jax.named_scope("done0"):
        for n in range(2):
            out[:, columns(n)] = (mine_a[:, columns(n)] + arrived(n)).astype(bf16)

    with jax.named_scope("drain"):
        wait(wq_v.at[0 : SENT_BYTES // 1024], "send")


def local(
    hidden, norm_gain, query_weight_matrix, key_value_weight, output_weight_matrix,
    input_down_factors, query_up_factor, key_value_up_factors, output_down_factor,
    output_up_factor, cache_keys, cache_values, lengths,
):
    hbm = pl.BlockSpec(memory_space=pltpu.HBM)
    dma = pltpu.SemaphoreType.DMA
    vmem = pltpu.VMEM
    return pl.pallas_call(
        kernel,
        out_shape=jax.ShapeDtypeStruct((SEQS, OUTC), bf16),
        in_specs=[hbm] * 13,
        out_specs=pl.BlockSpec(memory_space=pltpu.VMEM),
        scratch_shapes=[
            vmem((SEQS, FEATURES), bf16),
            vmem((SEQS, FEATURES), bf16),
            vmem((FEATURES, QCOLS), bf16),
            vmem((2, FEATURES, HEAD), bf16),
            vmem((QCOLS, FEATURES), bf16),
            vmem((SEQS, 1, 128, HEAD), bf16),
            vmem((SEQS, 1, 128, HEAD), bf16),
            vmem((3, 64, RANK), bf16),
            vmem((32, RANK), bf16),
            vmem((2, 8, RANK), bf16),
            vmem((32, RANK), bf16),
            vmem((RANK, 64), bf16),
            vmem((FEATURES,), bf16),
            vmem((SEQS,), jnp.int32),
            vmem((2, CHIPS, 64, 128), bf16),
            vmem((2, CHIPS, 32, 128), bf16),
            vmem((2, SEQS, CHIPS * 64), bf16),
            vmem((2, 2 * SEQS, CHIPS * 32), bf16),
            vmem((CHIPS, UROWS, 128), bf16),
            vmem((2, TP, 32, 128), bf16),
            vmem((2, TP, 16, 128), bf16),
            vmem((2, TP, 32, 128), bf16),
            vmem((TP, 32, 128), bf16),
            vmem((TP, SEQS, 128), bf16),
            vmem((RANK, OUTC), bf16),
            vmem((QCOLS, 128), bf16),
            vmem((6, 32, 128), bf16),
            [vmem((4, SEQS, w), bf16) for w in WIDTHS[:2]],
            [vmem((4, SEQS, w), bf16) for w in WIDTHS[:2]],
            [vmem((3, 2, 32, w), bf16) for w in WIDTHS],
            [vmem((3, 2, 32, w), bf16) for w in WIDTHS],
            [vmem((SEQS, w), bf16) for w in WIDTHS[2:4]],
            [vmem((SEQS, w), bf16) for w in WIDTHS[2:4]],
            [vmem((2, 32, w), f32) for w in WIDTHS],
            vmem((4, SEQS, PART), f32),
            vmem((SEQS, PART), f32),
            vmem((2, SEQS, OUTC - PART), f32),
            vmem((SEQS, QCOLS), f32),
            vmem((SEQS, HEAD), f32),
            vmem((SEQS, HEAD), f32),
            vmem((SEQS * 8, HEAD), f32),
            vmem((SEQS * 8, HEAD), f32),
            vmem((SEQS * 8, HEAD), f32),
            vmem((SEQS * 8, HEAD), f32),
            vmem((SEQS * 8, HEAD), f32),
            vmem((SEQS, QCOLS), bf16),
            dma((4,)), dma((CHUNKS,)), dma((7,)),
            dma((CHIPS,)), dma((2, 4)), dma((2,)), dma((5, 2)), dma((5,)), dma((17,)),
        ],
        compiler_params=pltpu.CompilerParams(
            collective_id=0, has_side_effects=True, vmem_limit_bytes=48 * 1024 * 1024),
        cost_estimate=pl.CostEstimate(
            flops=3 * 10**9, bytes_accessed=26 * 2**20, transcendentals=0),
    )(*[pltpu.with_memory_space_constraint(x, pltpu.HBM) for x in (
        hidden, norm_gain, query_weight_matrix, key_value_weight,
        output_weight_matrix, input_down_factors, jnp.swapaxes(query_up_factor, 0, 1),
        jnp.swapaxes(key_value_up_factors, 1, 2), output_down_factor, output_up_factor,
        cache_keys, cache_values, lengths,
    )])


def solution(mesh):
    placed = (
        P("rep", None),
        P(),
        P(None, "tp"),
        P(None, None, "tp"),
        P("tp", None),
        P(None, ("rep", "tp"), None),
        P(None, ("rep", "tp")),
        P(None, None, ("rep", "tp")),
        P(("rep", "tp"), None),
        P(None, ("rep", "tp")),
        P("rep", "tp", None, None),
        P("rep", "tp", None, None),
        P("rep"),
    )
    return jax.shard_map(
        local, mesh=mesh, in_specs=placed, out_specs=P("rep", "tp"), check_vma=False
    )
```

```python
import math

import jax
import jax.numpy as jnp
from jax import lax
from jax.experimental import pallas as pl
from jax.experimental.pallas import tpu as pltpu
from jax.sharding import PartitionSpec as P

MESH = pl.DeviceIdType.MESH
bf16, f32 = jnp.bfloat16, jnp.float32

epsilon = 1e-06
rope_base = 1000000.0
adapter_scale = 0.5

FEATURES = 8192
SEQS = 64
RANK = 64
HEAD = 128
QCOLS = 512
OUTC = 1024
TP = 8
CHIPS = 8
CHUNKS = 4
CHUNK = FEATURES // CHUNKS
DROWS = 96
UROWS = 80
WIDTHS = (256, 256, 256, 256, 512)
STARTS = (0, 256, 512, 768, 512)
PART = 512
GROUP = 32
SENT_ROWS = (
    7 * DROWS + 8 * DROWS + 2 * 7 * UROWS + 8 * UROWS + 7 * 32 + 7 * 64 + 4 * 32
    + (4 * SEQS * PART + SEQS * (OUTC - PART) + 6 * 32 * sum(WIDTHS)) // 128
)
SENT_BYTES = SENT_ROWS * 256


def dot(a, b):
    return jnp.dot(a, b, preferred_element_type=f32)


def dot_nt(a, b):
    return lax.dot_general(a, b, (((1,), (1,)), ((), ())), preferred_element_type=f32)


def at_lanes(offset, rows):
    row = lax.broadcasted_iota(jnp.int32, (rows, 128), 0)
    lane = lax.broadcasted_iota(jnp.int32, (rows, 128), 1)
    return jnp.where(lane == row + offset, 1.0, 0.0).astype(bf16)


def kernel(
    hidden, gain, wq, wkv, wo, down, qup, kvup, odown, oup, keys, values, lengths,
    out,
    hid_v, nrm_v, wq_v, wkv_v, wo_v, k_v, v_v,
    down_v, qup_v, kvup_v, odown_v, oup_v, gain_v, len_v,
    dg, d2, own_x, own_y, ug, ute, utl, uto, inner_p, inner_v, ou_v, od_v, mid_p,
    xs0, xr0, zs, zr, xs1, xr1, kept, own0, mine_a, mine_b, qacc, kacc, vacc, q_s, max_s, sum_s, ctx_s, len_s, ctx_b,
    load_sem, wq_sem, small_sem,
    d_recv, x0_recv, x1_recv, far_recv, near_recv, sems,
):
    names = ("send", "across", "d2", "across2", "u", "e", "w", "t", "tt", "l", "ll", "o", "oo", "i", "v", "m_x", "m_z")
    sem = {name: sems.at[n] for n, name in enumerate(names)}

    def wait(ref, name):
        pltpu.make_async_copy(ref, ref, sem[name]).wait()

    rep = lax.axis_index("rep")
    t = lax.axis_index("tp")
    chip = rep // 2
    core = rep % 2
    partner = chip * 2 + (1 - core)
    a, k = t // 4, t % 4
    other = 1 - a

    def chip_at(j):
        return lax.rem(chip + j, CHIPS)

    def tp_of(j):
        return t if j % 2 == 0 else lax.rem(t + 4, TP)

    def gather_peer(j):
        return chip_at(j) * 2 + core, tp_of(j)

    far_first = (4, 3, 5, 1, 7, 2, 6)

    farthest = ((1, 2), (0, 2), (1, 1), (1, 3), (0, 1), (0, 3), (1, 0))

    def tp_at(j):
        da, dk = farthest[j - 1]
        return lax.rem(a + da, 2) * 4 + lax.rem(k + dk, 4)

    def z_at(d):
        return lax.rem(k + d, 4)

    def remote(src, dst, send_sem, recv_sem, rep_to, tp_to):
        return pltpu.make_async_remote_copy(
            src_ref=src, dst_ref=dst, send_sem=send_sem, recv_sem=recv_sem,
            device_id=(rep_to, tp_to), device_id_type=MESH)

    barrier = pltpu.get_barrier_semaphore()
    small = [
        pltpu.make_async_copy(src, dst, small_sem.at[i])
        for i, (src, dst) in enumerate(
            ((down, down_v), (qup, qup_v), (kvup, kvup_v), (odown, odown_v), (oup, oup_v),
             (gain, gain_v), (lengths, len_v))
        )
    ]
    small[0].start()
    pl.semaphore_signal(barrier, inc=1, device_id=(partner, t), device_id_type=MESH)
    for j in range(1, CHIPS):
        pl.semaphore_signal(barrier, inc=1, device_id=gather_peer(j), device_id_type=MESH)
    for j in range(1, TP):
        pl.semaphore_signal(barrier, inc=1, device_id=(rep, tp_at(j)), device_id_type=MESH)
    for copy in small[1:]:
        copy.start()
    hid_copy = pltpu.make_async_copy(hidden, hid_v, load_sem.at[0])
    hid_copy.start()

    def wq_copy(i):
        rows = pl.ds(pl.multiple_of(i * CHUNK, CHUNK), CHUNK)
        return pltpu.make_async_copy(wq.at[rows, :], wq_v.at[rows, :], wq_sem.at[i])

    def wkv_copy(i):
        rows = pl.ds(pl.multiple_of(i * CHUNK, CHUNK), CHUNK)
        return pltpu.make_async_copy(wkv.at[:, rows, :], wkv_v.at[:, rows, :], wq_sem.at[i])

    def start_chunk(i, carry):
        wq_copy(i).start()
        wkv_copy(i).start()
        return carry

    lax.fori_loop(0, CHUNKS, start_chunk, 0)
    key_copy = pltpu.make_async_copy(keys, k_v, load_sem.at[1])
    value_copy = pltpu.make_async_copy(values, v_v, load_sem.at[2])
    wo_copy = pltpu.make_async_copy(wo, wo_v, load_sem.at[3])
    key_copy.start()
    value_copy.start()
    wo_copy.start()

    low, high = at_lanes(0, RANK), at_lanes(64, RANK)
    with jax.named_scope("pack"):
        small[0].wait()
        dg[core, chip] = (dot(down_v[0], low) + dot(down_v[1], high)).astype(bf16)
        d2[core, chip] = (dot(down_v[2, 0:32, :], low) + dot(down_v[2, 32:64, :], high)).astype(bf16)
        for copy in small[1:]:
            copy.wait()
        ug[chip, 0:16, :] = (dot(qup_v[0:16, :], low) + dot(qup_v[16:32, :], high)).astype(bf16)
        last = dot(kvup_v[1], low) + dot(kvup_v[0], high)
        ug[chip, 16:32, :] = jnp.concatenate([last, jnp.zeros_like(last)], axis=0).astype(bf16)
        ug[chip, 32:48, :] = (dot(odown_v[0:16, :], low) + dot(odown_v[16:32, :], high)).astype(bf16)
        ug[chip, 48:80, :] = (dot(oup_v[0:32, :], low) + dot(oup_v[32:64, :], high)).astype(bf16)

    with jax.named_scope("hid_wait"):
        hid_copy.wait()

    def squares(i, total):
        cols = pl.ds(pl.multiple_of(i * CHUNK, CHUNK), CHUNK)
        x = hid_v[:, cols].astype(f32)
        x = x * x
        for n in range(CHUNK // 128):
            total = total + x[:, n * 128 : (n + 1) * 128]
        return total

    with jax.named_scope("norm"):
        total = lax.fori_loop(0, CHUNKS, squares, jnp.zeros((SEQS, 128), f32))
        square = jnp.sum(total, axis=-1, keepdims=True) * (1.0 / FEATURES)
        scale = lax.rsqrt(square + epsilon)

        def normalise(i, carry):
            cols = pl.ds(pl.multiple_of(i * CHUNK, CHUNK), CHUNK)
            x = hid_v[:, cols].astype(f32)
            nrm_v[:, cols] = (x * scale * gain_v[cols].astype(f32).reshape(1, CHUNK)).astype(bf16)
            return carry

        lax.fori_loop(0, CHUNKS, normalise, 0)

    with jax.named_scope("barrier_wait"):
        pl.semaphore_wait(barrier, CHIPS + TP - 1)

    def d_copy(j):
        return remote(dg.at[core, chip], dg.at[core, chip], sem["send"], d_recv.at[j],
                      *gather_peer(j))

    def u_copy(j):
        piece = ug.at[chip, 0:32]
        return remote(piece, piece, sem["send"], sem["u"], *gather_peer(j))

    def e_copy(j):
        piece = ug.at[chip, 32:48]
        return remote(piece, piece, sem["send"], sem["e"], *gather_peer(j))

    def w_copy(j):
        piece = ug.at[chip, 48:80]
        return remote(piece, piece, sem["send"], sem["w"], *gather_peer(j))

    def across(j):
        q = lax.rem(chip + CHIPS - j, CHIPS)
        return remote(dg.at[core, q], dg.at[core, q], sem["send"], sem["across"], partner, t)

    def d2_copy(j):
        return remote(d2.at[core, chip], d2.at[core, chip], sem["send"], sem["d2"], *gather_peer(j))

    for j in far_first:
        u_copy(j).start()
    for j in far_first:
        d_copy(j).start()
    across(0).start()
    for j in far_first:
        d2_copy(j).start()
    for j in far_first:
        e_copy(j).start()

    qacc[...] = jnp.zeros_like(qacc)
    kacc[...] = jnp.zeros_like(kacc)
    vacc[...] = jnp.zeros_like(vacc)

    def project(i, carry):
        chunk = wq_v.at[0 : CHUNK * 3 // 2]
        pltpu.make_async_copy(chunk, chunk, wq_sem.at[i]).wait()
        cols = pl.ds(pl.multiple_of(i * CHUNK, CHUNK), CHUNK)
        x = nrm_v[:, cols]
        qacc[...] += dot(x, wq_v[cols, :])
        kacc[...] += dot(x, wkv_v[0, cols, :])
        vacc[...] += dot(x, wkv_v[1, cols, :])
        return carry

    with jax.named_scope("project"):
        lax.fori_loop(0, CHUNKS, project, 0)

    lane = lax.broadcasted_iota(jnp.int32, (SEQS, 128), 1)
    left = lane < 64
    with jax.named_scope("angles"):
        lens = len_v[...].reshape(1, SEQS)
        square_rows = lax.broadcasted_iota(jnp.int32, (SEQS, SEQS), 0)
        square_lanes = lax.broadcasted_iota(jnp.int32, (SEQS, SEQS), 1)
        len_col = jnp.sum(
            jnp.where(square_rows == square_lanes, jnp.broadcast_to(lens, (SEQS, SEQS)), 0).astype(f32),
            axis=-1, keepdims=True)
        len_b = jnp.broadcast_to(len_col, (SEQS, 128))
        for h in range(8):
            len_s[pl.ds(h, SEQS, stride=8), :] = len_b
        index = (lane % 64).astype(f32)
        frequency = jnp.exp(index * (-2.0 / HEAD * math.log(rope_base)))
        angles = len_b * frequency
        cosine = jnp.cos(angles)
        sine = jnp.where(left, -jnp.sin(angles), jnp.sin(angles))

    with jax.named_scope("own_features"):
        for c in range(2):
            parts = []
            for q in range(CHIPS):
                owner = lax.rem(t + 4 * lax.rem(chip + q, 2), TP)
                at = pl.multiple_of((2 * q + c) * QCOLS + (owner // 2) * 128, 128)
                x = nrm_v[:, pl.ds(at, 128)].astype(f32)
                parts.append(jnp.where(left, jnp.where(t % 2 == 0, x, pltpu.roll(x, 64, axis=1)), 0.0))
            for n in range(CHIPS // 2):
                x = parts[2 * n] + pltpu.roll(parts[2 * n + 1], 64, axis=1)
                own_x[c, :, n * 128 : (n + 1) * 128] = x.astype(bf16)
            for n in range(CHIPS // 4):
                first, last = 0.0, 0.0
                for m in range(4):
                    x = parts[4 * n + m]
                    x1, x2 = jnp.where(lane < 32, x, 0.0), jnp.where(lane < 32, 0.0, x)
                    first = first + (pltpu.roll(x1, 32 * m, axis=1) if m else x1)
                    last = last + (pltpu.roll(x2, (32 * m + 96) % 128, axis=1) if m != 1 else x2)
                own_y[c, 0:64, n * 128 : (n + 1) * 128] = first.astype(bf16)
                own_y[c, 64:128, n * 128 : (n + 1) * 128] = last.astype(bf16)

    def rotate(x):
        return x * cosine + pltpu.roll(x, 64, axis=1) * sine

    def slot_for(to):
        return lax.rem(t + 4 * lax.rem(to + chip, 2), TP)

    def t_copy(j):
        to = tp_at(j)
        return remote(ug.at[to, 0:32], ute.at[core, slot_for(to)], sem["send"], sem["t"], rep, to)

    def l_copy(j):
        to = tp_at(j)
        return remote(ug.at[to, 32:48], utl.at[core, slot_for(to)], sem["send"], sem["l"], rep, to)

    def o_copy(j):
        to = tp_at(j)
        return remote(ug.at[to, 48:80], uto.at[core, slot_for(to)], sem["send"], sem["o"], rep, to)

    with jax.named_scope("u_wait"):
        wait(ug.at[0:7, 0:32], "u")
        for j in range(1, TP):
            t_copy(j).start()
    with jax.named_scope("d_wait"):
        for j in range(1, CHIPS):
            d_copy(j).wait_recv()
            across(j).start()
    for j in far_first:
        w_copy(j).start()

    def features(c):
        return dot(own_x[c], dg[c].reshape(CHIPS * 64, 128))

    def value_features(c):
        return dot(own_y[c], d2[c].reshape(CHIPS * 32, 128))

    def pass_values():
        wait(d2.at[core, 0:7], "d2")
        remote(d2.at[core], d2.at[core], sem["send"], sem["across2"], partner, t).start()

    @pl.when(core == 1)
    def _():
        pass_values()

    with jax.named_scope("inner_own"):
        partial = features(core)

    with jax.named_scope("across_wait"):
        wait(dg.at[1 - core], "across")
    with jax.named_scope("inner_other"):
        partial = partial + features(1 - core)
        packed = jnp.where(left[0:32], partial[0:32], pltpu.roll(partial[32:64], 64, axis=1))
        inner_p[t] = packed.astype(bf16)

    def i_copy(j):
        return remote(inner_p.at[t], inner_p.at[t], sem["send"], sem["i"], rep, tp_at(j))

    def v_copy(j):
        return remote(inner_v.at[t], inner_v.at[t], sem["send"], sem["v"], rep, tp_at(j))

    for j in range(1, TP):
        i_copy(j).start()
    with jax.named_scope("d2_wait"):

        @pl.when(core == 0)
        def _():
            pass_values()

    with jax.named_scope("w_wait"):
        wait(ug.at[0:7, 32:48], "e")
        for j in range(1, TP):
            l_copy(j).start()
        wait(d2.at[1 - core], "across2")
        x = value_features(core) + value_features(1 - core)
        inner_v[t] = jnp.where(left, x[0:64] + pltpu.roll(x[64:128], 64, axis=1), partial).astype(bf16)
    for j in range(1, TP):
        v_copy(j).start()
    ute[core, slot_for(t)] = ug[t, 0:32]
    utl[core, slot_for(t)] = ug[t, 32:48]

    with jax.named_scope("t_wait"):
        wait(ute.at[core, 0:7], "t")
    t_across = remote(ute.at[core], ute.at[core], sem["send"], sem["tt"], partner, t)
    t_across.start()
    with jax.named_scope("up_wait"):
        wait(ute.at[1 - core], "tt")
    with jax.named_scope("unpack"):
        rows = []
        for n in range(2 * TP):
            e = ute[n // TP, n % TP, 0:16, :].astype(f32)
            rows += [e, pltpu.roll(e, 64, axis=1)]
        up_rows = jnp.concatenate(rows, axis=0).astype(bf16)
        kv_rows = jnp.concatenate(
            [ute[n // TP, n % TP, 16:32, :].astype(f32)[0:8] for n in range(2 * TP)], axis=0).astype(bf16)

    with jax.named_scope("i_wait"):
        wait(inner_p.at[0:7], "i")
    score_scale = 1.0 / math.sqrt(HEAD)
    with jax.named_scope("queries"):
        inner = inner_p[0].astype(f32)
        for n in range(1, TP):
            inner = inner + inner_p[n].astype(f32)
        inner = jnp.concatenate([inner, pltpu.roll(inner, 64, axis=1)], axis=0)
        inner_q = jnp.where(left, inner, 0.0).astype(bf16)
        query = qacc[...] + adapter_scale * dot_nt(inner_q, up_rows)
        for h in range(4):
            x = rotate(query[:, h * HEAD : (h + 1) * HEAD])
            main = x.astype(bf16).astype(f32)
            q_s[pl.ds(h, SEQS, stride=8), :] = main
            q_s[pl.ds(h + 4, SEQS, stride=8), :] = x - main
            qacc[:, h * HEAD : (h + 1) * HEAD] = x

    with jax.named_scope("cache_wait"):
        key_copy.wait()
        value_copy.wait()
    wide = 8 * GROUP
    position = lax.broadcasted_iota(jnp.int32, (wide, 128), 1).astype(f32)

    def attend(g):
        rows = pl.ds(g * wide, wide)
        q_rows = q_s[rows, :].astype(bf16)
        scores = []
        for s in range(GROUP):
            sc = dot_nt(q_rows[s * 8 : (s + 1) * 8], k_v[g * GROUP + s, 0])
            scores.append(sc + pltpu.roll(sc, 4, axis=0))
        scores = jnp.concatenate(scores, axis=0) * score_scale
        live = position < len_s[rows, :]
        row_max = jnp.max(jnp.where(live, scores, -1e30), axis=-1, keepdims=True)
        weights = jnp.where(live, jnp.exp(scores - row_max), 0.0)
        denom = jnp.sum(weights, axis=-1, keepdims=True)
        probs = (weights / denom).astype(bf16)
        max_s[rows, :] = jnp.broadcast_to(row_max, (wide, 128))
        sum_s[rows, :] = jnp.broadcast_to(denom, (wide, 128))
        parts = [
            dot(probs[s * 8 : (s + 1) * 8], v_v[g * GROUP + s, 0]) for s in range(GROUP)
        ]
        ctx_s[rows, :] = jnp.concatenate(parts, axis=0)

    with jax.named_scope("attend"):
        attend(0)
    with jax.named_scope("late_wait"):
        wait(utl.at[core, 0:7], "l")
    l_across = remote(utl.at[core], utl.at[core], sem["send"], sem["ll"], partner, t)
    l_across.start()
    with jax.named_scope("o_start"):
        wait(ug.at[0:7, 48:80], "w")
        for j in range(1, TP):
            o_copy(j).start()
    with jax.named_scope("attend2"):
        attend(1)

    with jax.named_scope("v_wait"):
        wait(inner_v.at[0:7], "v")
    with jax.named_scope("context"):
        inner = inner_v[0].astype(f32)
        for n in range(1, TP):
            inner = inner + inner_v[n].astype(f32)
        inner_k = jnp.where(left, 0.0, inner).astype(bf16)
        new_key = rotate(kacc[...] + adapter_scale * dot_nt(inner_k, kv_rows)).astype(bf16).astype(f32)
        inner_k = jnp.where(left, inner, 0.0).astype(bf16)
        new_value = (vacc[...] + adapter_scale * dot_nt(inner_k, kv_rows)).astype(bf16).astype(f32)
        for h in range(4):
            at = pl.ds(h, SEQS, stride=8)
            own = jnp.sum(qacc[:, h * HEAD : (h + 1) * HEAD] * new_key, axis=-1, keepdims=True)
            own = jnp.broadcast_to(own * score_scale, (SEQS, 128))
            row_max = jnp.maximum(max_s[at, :], own)
            cached = sum_s[at, :] * jnp.exp(max_s[at, :] - row_max)
            own = jnp.exp(own - row_max)
            x = (ctx_s[at, :] * cached + own * new_value) / (cached + own)
            ctx_b[:, h * HEAD : (h + 1) * HEAD] = x.astype(bf16)

    with jax.named_scope("wo_wait"):
        wo_copy.wait()
    o_across = remote(uto.at[core], uto.at[core], sem["send"], sem["oo"], partner, t)

    z_minus, z_plus = a * 4 + z_at(3), a * 4 + z_at(1)
    across_x = other * 4 + k
    top, bottom = slice(0, 32), slice(32, 64)

    def block(a_to, d):
        at = (a_to * 4 + z_at(d)) * OUTC
        return dot(ctx_b[...], wo_v[:, pl.ds(pl.multiple_of(at, OUTC), OUTC)])

    def x0_copy(n, d):
        return remote(xs0[n].at[d], xr0[n].at[d], sem["send"], x0_recv.at[n, d], rep, across_x)

    def x1_copy(n):
        return remote(xs1[n], xr1[n], sem["send"], x1_recv.at[n], rep, across_x)

    def columns(f):
        return slice(STARTS[f], STARTS[f] + WIDTHS[f])

    def z_copy(f, kind, way):
        return remote(zs[f].at[kind, way], zr[f].at[kind, way], sem["send"],
                      far_recv.at[f, way] if kind == 0 else near_recv.at[f],
                      rep, z_minus if way == 0 else z_plus)

    def far(f, x):
        for way in range(2):
            zs[f][0, way] = x[top if way == 0 else bottom].astype(bf16)
            z_copy(f, 0, way).start()

    def near(f, way, x):
        zs[f][1, way] = x[bottom if way == 0 else top].astype(bf16)
        kept[f][way] = x[top if way == 0 else bottom]
        z_copy(f, 1, way).start()

    def relay(f):
        for way in range(2):
            z_copy(f, 0, way).wait_recv()
            zs[f][2, way] = (kept[f][way] + zr[f][0, way].astype(f32)).astype(bf16)
            z_copy(f, 2, way).start()

    def arrived(f):
        got = zr[f]
        both = got.at[1:3]
        pltpu.make_async_copy(both, both, near_recv.at[f]).wait()
        first = got[2, 0].astype(f32) + got[1, 1].astype(f32)
        last = got[2, 1].astype(f32) + got[1, 0].astype(f32)
        return jnp.concatenate([first, last], axis=0)

    def x_first(d, x):
        for n in range(2):
            xs0[n][d] = x[:, columns(n)].astype(bf16)
            x0_copy(n, d).start()

    def other_far(x):
        x_first(2, x)
        far(2, x[:, columns(2)])
        far(3, x[:, columns(3)])

    def other_near(d, way, x):
        x_first(d, x)
        near(2, way, x[:, columns(2)])
        near(3, way, x[:, columns(3)])

    def x_sum(n, d):
        x0_copy(n, d).wait_recv()
        return own0[d, :, columns(n)] + xr0[n][d].astype(f32)

    def m_copy(src, dst, n, to):
        return remote(mid_p.at[src], mid_p.at[dst], sem["send"], sem["m_x" if n == 0 else "m_z"], rep, to)

    m_x = m_copy(0, 1, 0, across_x)
    m_minus = m_copy(2, 3, 1, z_minus)
    m_plus = m_copy(2, 4, 2, z_plus)
    m_two = m_copy(2, 5, 3, a * 4 + z_at(2))

    with jax.named_scope("send0"):
        other_far(block(other, 2))
    with jax.named_scope("middle"):
        wait(utl.at[1 - core], "ll")
        for n in range(2 * TP):
            e = utl[n // TP, n % TP].astype(f32)
            e = jnp.concatenate([e, pltpu.roll(e, 64, axis=1)], axis=0)
            od_v[n * 32 : (n + 1) * 32, :] = e.astype(bf16)
        middle = dot(ctx_b[...], od_v[...])
        middle = jnp.where(left[0:32], middle[0:32], pltpu.roll(middle[32:64], 64, axis=1))
        mid_p[0] = middle.astype(bf16)
        m_x.start()
    with jax.named_scope("send1"):
        other_near(3, 0, block(other, 3))
        other_near(1, 1, block(other, 1))
        x = block(a, 2)
        far(4, x[:, PART:])
        own0[2] = x[:, :PART]
        for way, d in ((0, 3), (1, 1)):
            x = block(a, d)
            near(4, way, x[:, PART:])
            own0[d] = x[:, :PART]
    with jax.named_scope("send2"):
        x = block(other, 0)
        x_first(0, x)
        mine_b[0] = x[:, PART:]
    with jax.named_scope("x_far0"):
        far(0, x_sum(0, 2))
    with jax.named_scope("relay2"):
        relay(2)
    with jax.named_scope("x_far"):
        far(1, x_sum(1, 2))
    with jax.named_scope("relay3"):
        relay(3)
    with jax.named_scope("mid_x"):
        wait(mid_p.at[1], "m_x")
        mid_p[2] = (mid_p[0].astype(f32) + mid_p[1].astype(f32)).astype(bf16)
        m_two.start()
        m_minus.start()
        m_plus.start()
    with jax.named_scope("own2"):
        wait(uto.at[core, 0:7], "o")
        uto[core, slot_for(t)] = ug[t, 48:80]
        o_across.start()
        x = block(a, 0)
        mine_a[...] = x[:, :PART]
        mine_b[1] = x[:, PART:]
    with jax.named_scope("relay4"):
        relay(4)
    with jax.named_scope("ou"):
        wait(uto.at[1 - core], "oo")
        for n in range(TP):
            e = uto[(2 * n) // TP, (2 * n) % TP].astype(f32)
            g = uto[(2 * n) // TP, (2 * n + 1) % TP].astype(f32)
            e_r, g_r = pltpu.roll(e, 64, axis=1), pltpu.roll(g, 64, axis=1)
            ou_v[0:32, n * 128 : (n + 1) * 128] = jnp.where(left[0:32], e, g_r).astype(bf16)
            ou_v[32:64, n * 128 : (n + 1) * 128] = jnp.where(left[0:32], e_r, g).astype(bf16)
    with jax.named_scope("x_near0"):
        for n in range(2):
            near(n, 0, x_sum(n, 3))
    with jax.named_scope("done2"):
        xs1[0][...] = (mine_b[0, :, : WIDTHS[2]] + arrived(2)).astype(bf16)
        x1_copy(0).start()
    with jax.named_scope("x_near1"):
        for n in range(2):
            near(n, 1, x_sum(n, 1))
    with jax.named_scope("relay00"):
        relay(0)
    with jax.named_scope("done3"):
        xs1[1][...] = (mine_b[0, :, WIDTHS[2] :] + arrived(3)).astype(bf16)
        x1_copy(1).start()
    with jax.named_scope("relay0"):
        relay(1)
    with jax.named_scope("delta"):
        wait(mid_p.at[3:6], "m_z")
        middle = mid_p[2].astype(f32)
        for n in range(3, 6):
            middle = middle + mid_p[n].astype(f32)
        middle = jnp.concatenate([middle, pltpu.roll(middle, 64, axis=1)], axis=0)[:, 0:64].astype(bf16)
        delta = adapter_scale * dot(middle, ou_v[...])
        mine_a[...] = mine_a[...] + delta[:, 0:PART]
        mine_b[1] = mine_b[1] + delta[:, PART:]
    with jax.named_scope("done4"):
        mine_b[1] = mine_b[1] + arrived(4)
    with jax.named_scope("x0_wait"):
        for n in range(2):
            x0_copy(n, 0).wait_recv()
            mine_a[:, columns(n)] = mine_a[:, columns(n)] + xr0[n][0].astype(f32)
    with jax.named_scope("x1_wait"):
        for n in range(2):
            x1_copy(n).wait_recv()
            cols = columns(2 + n)
            own = mine_b[1, :, cols.start - PART : cols.stop - PART]
            out[:, cols] = (own + xr1[n][...].astype(f32)).astype(bf16)
    with jax.named_scope("done0"):
        for n in range(2):
            out[:, columns(n)] = (mine_a[:, columns(n)] + arrived(n)).astype(bf16)

    with jax.named_scope("drain"):
        wait(wq_v.at[0 : SENT_BYTES // 1024], "send")


def local(
    hidden, norm_gain, query_weight_matrix, key_value_weight, output_weight_matrix,
    input_down_factors, query_up_factor, key_value_up_factors, output_down_factor,
    output_up_factor, cache_keys, cache_values, lengths,
):
    hbm = pl.BlockSpec(memory_space=pltpu.HBM)
    dma = pltpu.SemaphoreType.DMA
    vmem = pltpu.VMEM
    return pl.pallas_call(
        kernel,
        out_shape=jax.ShapeDtypeStruct((SEQS, OUTC), bf16),
        in_specs=[hbm] * 13,
        out_specs=pl.BlockSpec(memory_space=pltpu.VMEM),
        scratch_shapes=[
            vmem((SEQS, FEATURES), bf16),
            vmem((SEQS, FEATURES), bf16),
            vmem((FEATURES, QCOLS), bf16),
            vmem((2, FEATURES, HEAD), bf16),
            vmem((QCOLS, FEATURES), bf16),
            vmem((SEQS, 1, 128, HEAD), bf16),
            vmem((SEQS, 1, 128, HEAD), bf16),
            vmem((3, 64, RANK), bf16),
            vmem((32, RANK), bf16),
            vmem((2, 8, RANK), bf16),
            vmem((32, RANK), bf16),
            vmem((RANK, 64), bf16),
            vmem((FEATURES,), bf16),
            vmem((SEQS,), jnp.int32),
            vmem((2, CHIPS, 64, 128), bf16),
            vmem((2, CHIPS, 32, 128), bf16),
            vmem((2, SEQS, CHIPS * 64), bf16),
            vmem((2, 2 * SEQS, CHIPS * 32), bf16),
            vmem((CHIPS, UROWS, 128), bf16),
            vmem((2, TP, 32, 128), bf16),
            vmem((2, TP, 16, 128), bf16),
            vmem((2, TP, 32, 128), bf16),
            vmem((TP, 32, 128), bf16),
            vmem((TP, SEQS, 128), bf16),
            vmem((RANK, OUTC), bf16),
            vmem((QCOLS, 128), bf16),
            vmem((6, 32, 128), bf16),
            [vmem((4, SEQS, w), bf16) for w in WIDTHS[:2]],
            [vmem((4, SEQS, w), bf16) for w in WIDTHS[:2]],
            [vmem((3, 2, 32, w), bf16) for w in WIDTHS],
            [vmem((3, 2, 32, w), bf16) for w in WIDTHS],
            [vmem((SEQS, w), bf16) for w in WIDTHS[2:4]],
            [vmem((SEQS, w), bf16) for w in WIDTHS[2:4]],
            [vmem((2, 32, w), f32) for w in WIDTHS],
            vmem((4, SEQS, PART), f32),
            vmem((SEQS, PART), f32),
            vmem((2, SEQS, OUTC - PART), f32),
            vmem((SEQS, QCOLS), f32),
            vmem((SEQS, HEAD), f32),
            vmem((SEQS, HEAD), f32),
            vmem((SEQS * 8, HEAD), f32),
            vmem((SEQS * 8, HEAD), f32),
            vmem((SEQS * 8, HEAD), f32),
            vmem((SEQS * 8, HEAD), f32),
            vmem((SEQS * 8, HEAD), f32),
            vmem((SEQS, QCOLS), bf16),
            dma((4,)), dma((CHUNKS,)), dma((7,)),
            dma((CHIPS,)), dma((2, 4)), dma((2,)), dma((5, 2)), dma((5,)), dma((17,)),
        ],
        compiler_params=pltpu.CompilerParams(
            collective_id=0, has_side_effects=True, vmem_limit_bytes=48 * 1024 * 1024),
        cost_estimate=pl.CostEstimate(
            flops=3 * 10**9, bytes_accessed=26 * 2**20, transcendentals=0),
    )(*[pltpu.with_memory_space_constraint(x, pltpu.HBM) for x in (
        hidden, norm_gain, query_weight_matrix, key_value_weight,
        output_weight_matrix, input_down_factors, jnp.swapaxes(query_up_factor, 0, 1),
        jnp.swapaxes(key_value_up_factors, 1, 2), output_down_factor, output_up_factor,
        cache_keys, cache_values, lengths,
    )])


def solution(mesh):
    placed = (
        P("rep", None),
        P(),
        P(None, "tp"),
        P(None, None, "tp"),
        P("tp", None),
        P(None, ("rep", "tp"), None),
        P(None, ("rep", "tp")),
        P(None, None, ("rep", "tp")),
        P(("rep", "tp"), None),
        P(None, ("rep", "tp")),
        P("rep", "tp", None, None),
        P("rep", "tp", None, None),
        P("rep"),
    )
    return jax.shard_map(
        local, mesh=mesh, in_specs=placed, out_specs=P("rep", "tp"), check_vma=False
    )
```
